32 devices in a mesh: gx: 4 (over x, core), gy: 8 (over z, y).
Axes of the slice: x: 2, y: 2, z: 4, core: 2. Of those that a mesh axis runs over, the one named last changes fastest.
Arguments:
- east_velocity: float32 [48, 32, 2048], P(None, 'gx', 'gy'), may hold values from -3 to 3
- north_velocity: float32 [48, 32, 2048], P(None, 'gx', 'gy'), may hold values from -3 to 3
- salinity: float32 [48, 32, 2048], P(None, 'gx', 'gy'), may hold values from -6 to 6
- surface: float32 [32, 2048], P('gx', 'gy'), may hold values from -6 to 6
- column_depth: float32 [32, 2048], P('gx', 'gy'), may hold values from 0.5 to 4
- wet_column: int32 [32, 2048], P('gx', 'gy'), may hold values 0 or 1
- active_levels: int32 [32, 2048], P('gx', 'gy'), may hold values from 1 to 48
Outputs:
- east_flow: float32 [48, 32, 2048], P(None, 'gx', 'gy')
- north_flow: float32 [48, 32, 2048], P(None, 'gx', 'gy')
- salt_next: float32 [48, 32, 2048], P(None, 'gx', 'gy')
- surface_next: float32 [32, 2048], P('gx', 'gy')
The draws below stay inside these ranges and needn't reach their ends.
All inputs are finite; a program needn't handle non-finite values. No bound on the sum of `wet_column` on one device may be relied on, other than what follows from the above.
Results may differ from the reference program's by a relative error of at most 0.000024.
Values sent between devices are 32-bit elements; how exact they have to be, the bound alone decides.
A program may use at most 64 MiB of HBM per device.

```python
import math
import jax
import jax.numpy as jnp

LEV = 48
ITERS = 16
NX = 32
NY = 2048


def touch_ends(values, key, least, largest):
    spot = [jax.random.randint(jax.random.fold_in(key, axis), (), 0, length) for axis, length in enumerate(values.shape)]
    main_axis = values.shape.index(max(values.shape))
    neighbour = spot[:main_axis] + [(spot[main_axis] + 1) % values.shape[main_axis]] + spot[main_axis + 1:]
    return values.at[tuple(spot)].set(least).at[tuple(neighbour)].set(largest)


def level_of(own_key, shape, shards, low, high):
    gain = 1.0
    for position, blocks in shards:
        steps = jax.random.uniform(jax.random.fold_in(jax.random.fold_in(own_key, 6), position), (blocks,), jnp.float32, low / len(shards), high / len(shards))
        gain = gain * jnp.repeat(jnp.exp(steps), shape[position] // blocks).reshape((-1,) + (1,) * (len(shape) - 1 - position))
    return gain


def normal_values(own_key, shape, scale, reach, pieces=(), held_as=jnp.bfloat16):
    entries = jax.random.normal(own_key, shape, jnp.float32) * scale
    if len(pieces) > 0:
        entries = level_of(own_key, shape, pieces, -0.22, 0.18) * entries
    return jnp.clip(entries, min=-reach, max=reach).astype(held_as)


def setup_inputs(seed: int = 0) -> dict:
    arg_keys = jax.random.split(jax.random.key(seed), 8)
    east_velocity = normal_values(arg_keys[0], (LEV, NX, NY), 0.5, 3.0, ((1, 4), (2, 8)), jnp.float32)
    north_velocity = normal_values(arg_keys[1], (LEV, NX, NY), 0.5, 3.0, ((1, 4), (2, 8)), jnp.float32)
    salinity = normal_values(arg_keys[2], (LEV, NX, NY), 1.0, 6.0, ((1, 4), (2, 8)), jnp.float32)
    surface = normal_values(arg_keys[3], (NX, NY), 1.0, 6.0, ((0, 4), (1, 8)), jnp.float32)
    column_depth = jnp.clip(jnp.exp(math.log(4.0) - 2.0794415 * jax.random.uniform(arg_keys[4], (NX, NY), jnp.float32) ** level_of(arg_keys[4], (NX, NY), ((0, 4), (1, 8)), -0.2, 0.2)), 0.5, 4.0)
    wet_column = touch_ends((jax.random.randint(arg_keys[5], (NX, NY), 0, 8) < 7).astype(jnp.int32), jax.random.fold_in(arg_keys[5], 1), 0, 1)
    active_levels = touch_ends(jax.random.randint(arg_keys[6], (NX, NY), 1, LEV + 1), jax.random.fold_in(arg_keys[6], 1), 1, LEV).astype(jnp.int32)
    return {"east_velocity": east_velocity, "north_velocity": north_velocity, "salinity": salinity, "surface": surface, "column_depth": column_depth, "wet_column": wet_column, "active_levels": active_levels}


TIME_STEP = 0.2
CORIOLIS = 0.3
PRESS_COEF = 0.05
VISCOSITY = 0.1
DIFFUSIVITY = 0.1
SIGMA_SHIFT = 0.25
CHEB_CENTER = 3.625
CHEB_HALF = 3.375
DIVERGENCE_COEF = 8.0


def cheb_table(count):
    first = CHEB_CENTER / CHEB_HALF
    ratio = 1.0 / first
    keeps = []
    gains = []
    for index in range(count):
        ratio_next = 1.0 / (2.0 * first - ratio)
        keeps.append(ratio_next * ratio)
        gains.append(2.0 * ratio_next / CHEB_HALF)
        ratio = ratio_next
    return keeps, gains


def centre(field):
    return field[:, 2:-2, 2:-2]


def along_east(field):
    return (8.0 * (field[:, 3:-1, 2:-2] - field[:, 1:-3, 2:-2]) - (field[:, 4:, 2:-2] - field[:, :-4, 2:-2])) / 12.0


def along_north(field):
    return (8.0 * (field[:, 2:-2, 3:-1] - field[:, 2:-2, 1:-3]) - (field[:, 2:-2, 4:] - field[:, 2:-2, :-4])) / 12.0


def laplace(field):
    return field[:, 3:-1, 2:-2] + field[:, 1:-3, 2:-2] + field[:, 2:-2, 3:-1] + field[:, 2:-2, 1:-3] - 4.0 * centre(field)


def tendency(padded):
    east, north, tracer = padded[0], padded[1], padded[2]
    pressure = PRESS_COEF * jnp.cumsum(tracer, axis=0)
    east_mid = centre(east)
    north_mid = centre(north)

    def advect(field):
        return -(east_mid * along_east(field) + north_mid * along_north(field))

    east_rate = advect(east) + CORIOLIS * north_mid - along_east(pressure) + VISCOSITY * laplace(east)
    north_rate = advect(north) - CORIOLIS * east_mid - along_north(pressure) + VISCOSITY * laplace(north)
    salt_rate = advect(tracer) + DIFFUSIVITY * laplace(tracer)
    return jnp.stack([east_rate, north_rate, salt_rate])


def nine_point(field, wet):
    weighted = wet * field
    edges = weighted[2:, 1:-1] + weighted[:-2, 1:-1] + weighted[1:-1, 2:] + weighted[1:-1, :-2]
    corners = weighted[2:, 2:] + weighted[2:, :-2] + weighted[:-2, 2:] + weighted[:-2, :-2]
    stencil = (20.0 * weighted[1:-1, 1:-1] - 4.0 * edges - corners) / 6.0
    wet_mid = wet[1:-1, 1:-1]
    field_mid = field[1:-1, 1:-1]
    return wet_mid * (SIGMA_SHIFT * field_mid + stencil) + (1.0 - wet_mid) * field_mid


def reference(east_velocity, north_velocity, salinity, surface, column_depth, wet_column, active_levels):
    wet = wet_column.astype(jnp.float32)
    levels = jnp.arange(LEV, dtype=jnp.int32)
    mask3 = (levels[:, None, None] < active_levels[None]).astype(jnp.float32) * wet[None]
    state0 = jnp.stack([east_velocity, north_velocity, salinity]) * mask3

    def rate(state):
        padded = jnp.pad(state, ((0, 0), (0, 0), (2, 2), (2, 2)))
        return tendency(padded) * mask3

    state1 = state0 + TIME_STEP * rate(state0)
    state2 = 0.75 * state0 + 0.25 * (state1 + TIME_STEP * rate(state1))
    state3 = state0 / 3.0 + (2.0 / 3.0) * (state2 + TIME_STEP * rate(state2))
    flow_east = column_depth * (jnp.sum(state3[0], axis=0) / LEV)
    flow_north = column_depth * (jnp.sum(state3[1], axis=0) / LEV)
    east_pad = jnp.pad(flow_east, 1)
    north_pad = jnp.pad(flow_north, 1)
    divergence = (east_pad[2:, 1:-1] - east_pad[:-2, 1:-1]) * 0.5 + (north_pad[1:-1, 2:] - north_pad[1:-1, :-2]) * 0.5
    right_side = wet * (SIGMA_SHIFT * surface - DIVERGENCE_COEF * divergence)
    wet_pad = jnp.pad(wet, 1)

    def apply(field):
        return nine_point(jnp.pad(field, 1), wet_pad)

    solution = surface
    residual = right_side - apply(solution)
    direction = residual / CHEB_CENTER
    keeps, gains = cheb_table(ITERS)
    for index in range(ITERS):
        solution = solution + direction
        residual = residual - apply(direction)
        direction = keeps[index] * direction + gains[index] * residual
    surface_pad = jnp.pad(solution, 1)
    slope_east = (surface_pad[2:, 1:-1] - surface_pad[:-2, 1:-1]) * 0.5
    slope_north = (surface_pad[1:-1, 2:] - surface_pad[1:-1, :-2]) * 0.5
    east_flow = mask3 * (state3[0] - slope_east[None])
    north_flow = mask3 * (state3[1] - slope_north[None])
    return east_flow, north_flow, state3[2], solution
```

```python
import functools

import jax
import jax.numpy as jnp
from jax import lax
from jax.experimental import pallas as pl
from jax.experimental.pallas import tpu as pltpu
from jax.sharding import PartitionSpec as P

ITERS = 16

TIME_STEP = 0.2
CORIOLIS = 0.3
PRESS_COEF = 0.05
VISCOSITY = 0.1
DIFFUSIVITY = 0.1
SIGMA_SHIFT = 0.25
CHEB_CENTER = 3.625
CHEB_HALF = 3.375
DIVERGENCE_COEF = 8.0

ROWS = 8
LANES = 128
CHUNK = 8
RIM = LANES // 4
MESH = pl.DeviceIdType.MESH


def cheb_table(count):
    first = CHEB_CENTER / CHEB_HALF
    ratio = 1.0 / first
    keeps = []
    gains = []
    for index in range(count):
        ratio_next = 1.0 / (2.0 * first - ratio)
        keeps.append(ratio_next * ratio)
        gains.append(2.0 * ratio_next / CHEB_HALF)
        ratio = ratio_next
    return (keeps, gains)


def dry_factor(count):
    keeps, gains = cheb_table(count)
    x, r = 1.0, -1.0
    d = r / CHEB_CENTER
    for index in range(count):
        x = x + d
        r = r - d
        d = keeps[index] * d + gains[index] * r
    return x


def kernel(
    nx, ny, reach, slots,
    east_hbm, north_hbm, salt_hbm, surface_hbm, depth_hbm, wet_hbm, active_hbm,
    state_out, slope_out, surface_out,
    held, moved, shifts, ints, floats, zeros, halo, send_x, send_y, far_c, far_e, gath, xs,
    load_sem, small_sem, halo_sem, side_sem, far_send, far_recv,
):
    gx = lax.axis_index("gx")
    gy = lax.axis_index("gy")
    width = held.shape[4]
    tiles = width // LANES
    chunks = held.shape[0] // 3
    levels = chunks * CHUNK
    groups = 3 * CHUNK // 4
    n = groups * tiles
    relative = slots < nx
    row = lax.broadcasted_iota(jnp.int32, (ROWS, LANES), 0)
    lane = lax.broadcasted_iota(jnp.int32, (ROWS, LANES), 1)
    pair = row // 2
    zero = jnp.zeros((ROWS, LANES), jnp.float32)

    def lanes(t):
        return slice(t * LANES, (t + 1) * LANES)

    def inside(x, y):
        return jnp.logical_and(
            jnp.logical_and(x >= 0, x < nx), jnp.logical_and(y >= 0, y < ny)
        )

    def whole(ref, sem):
        return pltpu.make_async_copy(ref, ref, sem)

    pltpu.make_async_copy(active_hbm, ints.at[0], small_sem.at[0]).start()
    pltpu.make_async_copy(wet_hbm, ints.at[1], small_sem.at[0]).start()
    for c in range(chunks):
        part = pl.ds(c * CHUNK, CHUNK)
        for f, source in enumerate((east_hbm, north_hbm, salt_hbm)):
            pltpu.make_async_copy(source.at[part], held.at[c, f], load_sem.at[c]).start()
    pltpu.make_async_copy(surface_hbm, floats.at[0], small_sem.at[1]).start()
    pltpu.make_async_copy(depth_hbm, floats.at[1], small_sem.at[1]).start()

    own = reach if relative else gx
    partners = [
        (o, side)
        for o in range(-reach, reach + 1)
        for side in (-1, 0, 1)
        if (o, side) != (0, 0)
    ]

    def far(action):
        for o, side in partners:
            @pl.when(inside(gx + o, gy + side))
            def _(o=o, side=side):
                action(o, side)

    barrier = pltpu.get_barrier_semaphore()
    count = jnp.int32(0)
    for o, side in partners:
        there = inside(gx + o, gy + side)

        @pl.when(there)
        def _(o=o, side=side):
            pl.semaphore_signal(
                barrier, inc=1, device_id=(gx + o, gy + side), device_id_type=MESH
            )

        count = count + there.astype(jnp.int32)

    for i in range(n):
        zeros[i] = zero

    source = lax.broadcasted_iota(jnp.int32, (width, width), 0)
    target = lax.broadcasted_iota(jnp.int32, (width, width), 1)
    step = source - target
    one = jnp.abs(step) == 1
    sign = jnp.where(step > 0, 1.0, -1.0)
    slope = jnp.where(one, 8.0 * sign, jnp.where(jnp.abs(step) == 2, -sign, 0.0))
    shifts[:, :width] = slope.astype(jnp.bfloat16)
    shifts[:, width:] = jnp.where(one, 1.0, 0.0).astype(jnp.bfloat16)

    def move(index):
        value = held[index].reshape(3 * CHUNK * ROWS, width)
        high = value.astype(jnp.bfloat16)
        rest = value - high.astype(jnp.float32)
        middle = rest.astype(jnp.bfloat16)
        low = (rest - middle.astype(jnp.float32)).astype(jnp.bfloat16)
        total = jnp.dot(low, shifts[...], preferred_element_type=jnp.float32)
        total = total + jnp.dot(middle, shifts[...], preferred_element_type=jnp.float32)
        total = total + jnp.dot(high, shifts[...], preferred_element_type=jnp.float32)
        moved[index] = total.reshape(3, CHUNK, ROWS, 2 * width)

    def pack(stage, c):
        rim = zero
        for f in range(3):
            for half in range(CHUNK // 4):
                group = f * (CHUNK // 4) + half
                ups = [None] * tiles
                downs = [None] * tiles
                for m in range(4):
                    kk = half * 4 + m
                    position = group * 4 + m
                    parts = [
                        held[stage * chunks + c, f, kk, :, lanes(t)] for t in range(tiles)
                    ]
                    for t in range(tiles):
                        turned = parts[t] if m == 3 else pltpu.roll(parts[t], 2 * m + 2, 0)
                        if m == 0:
                            ups[t] = turned
                            downs[t] = turned
                        else:
                            ups[t] = jnp.where(pair == m, turned, ups[t])
                            downs[t] = jnp.where(pair == (m + 1) % 4, turned, downs[t])
                    ends = jnp.where(lane < LANES // 2, parts[0], parts[-1])
                    rim = jnp.where(
                        lane // 4 == position,
                        pltpu.roll(ends, (4 * position + 2) % LANES, 1),
                        rim,
                    )
                for t in range(tiles):
                    send_x[0, stage, c, group * tiles + t] = downs[t]
                    send_x[1, stage, c, group * tiles + t] = ups[t]
        send_y[stage, c, 0] = rim

    def x_copy(stage, c, side):
        return pltpu.make_async_remote_copy(
            src_ref=send_x.at[side, stage, c],
            dst_ref=halo.at[stage, c, pl.ds((1 - side) * n, n)],
            send_sem=side_sem.at[side],
            recv_sem=halo_sem.at[stage, c],
            device_id=(gx + 2 * side - 1, gy),
            device_id_type=MESH,
        )

    def y_copy(stage, c, side):
        return pltpu.make_async_remote_copy(
            src_ref=send_y.at[stage, c],
            dst_ref=halo.at[stage, c, pl.ds(2 * n + 1 - side, 1)],
            send_sem=side_sem.at[2 + side],
            recv_sem=halo_sem.at[stage, c],
            device_id=(gx, gy + 2 * side - 1),
            device_id_type=MESH,
        )

    near = [
        (x_copy, 0, gx > 0), (x_copy, 1, gx < nx - 1),
        (y_copy, 0, gy > 0), (y_copy, 1, gy < ny - 1),
    ]

    def launch(stage, c):
        for copy, side, there in near:
            @pl.when(there)
            def _(copy=copy, side=side):
                copy(stage, c, side).start()

    def far_start(kind):
        def action(o, side):
            slot = reach - o if relative else gx
            if side == 0:
                source, target = far_c.at[kind], gath.at[kind, slot, pl.ds(0, 2 * tiles)]
            else:
                at = 2 * tiles + (1 - side) // 2
                source, target = far_e.at[kind], gath.at[kind, slot, pl.ds(at, 1)]
            pltpu.make_async_remote_copy(
                src_ref=source, dst_ref=target,
                send_sem=far_send.at[side + 1, o + reach if relative else gx + o],
                recv_sem=far_recv.at[kind],
                device_id=(gx + o, gy + side), device_id_type=MESH,
            ).start()

        far(action)
        pltpu.make_async_copy(
            far_c.at[kind], gath.at[kind, own, pl.ds(0, 2 * tiles)], far_recv.at[kind]
        ).start()

    def far_drain(o, side):
        sem = far_send.at[side + 1, o + reach if relative else gx + o]
        whole(far_c if side == 0 else far_e, sem).wait()

    def fill_far(data):
        low, high = data
        first = jnp.where(lane < RIM, low[0], pltpu.roll(high[0], RIM, 1))
        second = jnp.where(
            lane < LANES - RIM, pltpu.roll(high[-1], LANES - RIM, 1), low[-1]
        )
        return jnp.where(lane < 2 * RIM, first, second)

    def put_far(kind, data):
        for f in range(2):
            for t in range(tiles):
                far_c[kind, f * tiles + t] = data[f][t]
        far_e[kind, 0] = fill_far(data)

    whole(ints, small_sem.at[0]).wait()
    active = [ints[0, :, lanes(t)] * ints[1, :, lanes(t)] for t in range(tiles)]

    def first(c):
        whole(held.at[c], load_sem.at[c]).wait()
        for kk in range(CHUNK):
            for t in range(tiles):
                live = active[t] > c * CHUNK + kk
                for f in range(3):
                    held[c, f, kk, :, lanes(t)] = jnp.where(
                        live, held[c, f, kk, :, lanes(t)], 0.0
                    )
        pack(0, c)

    first(0)
    pl.semaphore_wait(barrier, count)
    launch(0, 0)

    @pl.loop(1, chunks)
    def _(c):
        first(c)
        launch(0, c)
        move(c - 1)

    for side, missing in ((0, gx == 0), (1, gx == nx - 1)):
        @pl.when(missing)
        def _(side=side):
            for stage in range(3):
                @pl.loop(0, chunks)
                def _(c, stage=stage):
                    pltpu.make_async_copy(
                        zeros, halo.at[stage, c, pl.ds(side * n, n)], halo_sem.at[stage, c]
                    ).start()

    for side, missing in ((0, gy == 0), (1, gy == ny - 1)):
        @pl.when(missing)
        def _(side=side):
            for stage in range(3):
                @pl.loop(0, chunks)
                def _(c, stage=stage):
                    pltpu.make_async_copy(
                        zeros.at[pl.ds(0, 1)],
                        halo.at[stage, c, pl.ds(2 * n + side, 1)],
                        halo_sem.at[stage, c],
                    ).start()
            for j in range(slots):
                @pl.when(inside(gx + j - reach, gy) if relative else gy >= 0)
                def _(j=j):
                    for kind in range(2):
                        pltpu.make_async_copy(
                            zeros.at[pl.ds(0, 1)],
                            gath.at[kind, j, pl.ds(2 * tiles + side, 1)],
                            far_recv.at[kind],
                        ).start()

    if relative:
        for j in range(slots):
            @pl.when(jnp.logical_not(inside(gx + j - reach, gy)))
            def _(j=j):
                for kind in range(2):
                    pltpu.make_async_copy(
                        zeros.at[pl.ds(0, 2 * tiles + 2)], gath.at[kind, j], far_recv.at[kind]
                    ).start()

    whole(floats, small_sem.at[1]).wait()
    put_far(0, (
        [floats[0, :, lanes(t)] for t in range(tiles)],
        [ints[1, :, lanes(t)].astype(jnp.float32) for t in range(tiles)],
    ))

    quarter = lane % 4

    def run_stage(stage, weight0, weight1):
        gain = weight1 * TIME_STEP
        keep_flow = weight1 - 4.0 * gain * VISCOSITY
        keep_salt = weight1 - 4.0 * gain * DIFFUSIVITY
        drift = -gain / 12.0
        push = drift * PRESS_COEF

        def body(c, carry, behind=stage < 2):
            press_e, press_n = list(carry[0]), list(carry[1])
            sums = [list(x) for x in carry[2:]]
            index = stage * chunks + c
            whole(halo.at[stage, c], halo_sem.at[stage, c]).wait()
            if behind:
                move(index + chunks - 1)
            rims = jnp.where(quarter < 2, halo[stage, c, 2 * n], halo[stage, c, 2 * n + 1])
            r1, r2 = pltpu.roll(rims, LANES - 1, 1), pltpu.roll(rims, LANES - 2, 1)
            l1, l2 = pltpu.roll(rims, 1, 1), pltpu.roll(rims, 2, 1)
            rim_slope = jnp.where(
                quarter < 2,
                jnp.where(quarter == 0, -r2, 8.0 * r1 - r2),
                jnp.where(quarter == 2, l2 - 8.0 * l1, l2),
            )
            rim_sum = jnp.where(quarter == 1, r1, jnp.where(quarter == 2, l1, 0.0))
            for kk in range(CHUNK):
                fields = []
                for f in range(3):
                    position = f * CHUNK + kk
                    group, m = position // 4, position % 4
                    back = (-(4 * position + 2)) % LANES
                    extra_slope = pltpu.roll(rim_slope, back, 1)
                    extra_sum = pltpu.roll(rim_sum, back, 1)
                    per_tile = []
                    for t in range(tiles):
                        q = held[index, f, kk, :, lanes(t)]
                        ends = jnp.where(
                            pair == m,
                            halo[stage, c, group * tiles + t],
                            halo[stage, c, n + group * tiles + t],
                        )
                        if m != 3:
                            ends = pltpu.roll(ends, (-(2 * m + 2)) % ROWS, 0)
                        e1 = pltpu.roll(jnp.where(row < 1, ends, q), ROWS - 1, 0)
                        e2 = pltpu.roll(jnp.where(row < 2, ends, q), ROWS - 2, 0)
                        w1 = pltpu.roll(jnp.where(row >= ROWS - 1, ends, q), 1, 0)
                        w2 = pltpu.roll(jnp.where(row >= ROWS - 2, ends, q), 2, 0)
                        dy = moved[index, f, kk, :, lanes(t)]
                        sides = moved[index, f, kk, :, lanes(tiles + t)]
                        if t == 0:
                            dy = dy + jnp.where(lane < 2, extra_slope, 0.0)
                            sides = sides + jnp.where(lane < 1, extra_sum, 0.0)
                        if t == tiles - 1:
                            dy = dy + jnp.where(lane >= LANES - 2, extra_slope, 0.0)
                            sides = sides + jnp.where(lane >= LANES - 1, extra_sum, 0.0)
                        dx = 8.0 * (e1 - w1) - (e2 - w2)
                        per_tile.append((q, dx, dy, (e1 + w1) + sides))
                    fields.append(per_tile)
                for t in range(tiles):
                    live = active[t] > c * CHUNK + kk
                    (u, ux, uy, ul), (v, vx, vy, vl), (s, sx, sy, sl) = [
                        fields[f][t] for f in range(3)
                    ]
                    press_e[t] = press_e[t] + sx
                    press_n[t] = press_n[t] + sy
                    um = u * drift
                    vm = v * drift
                    news = [
                        (um * ux + vm * uy) + push * press_e[t] + (gain * CORIOLIS) * v
                        + (gain * VISCOSITY) * ul + keep_flow * u,
                        (um * vx + vm * vy) + push * press_n[t] - (gain * CORIOLIS) * u
                        + (gain * VISCOSITY) * vl + keep_flow * v,
                        (um * sx + vm * sy) + (gain * DIFFUSIVITY) * sl + keep_salt * s,
                    ]
                    for f in range(3):
                        new = news[f]
                        if weight0 is not None:
                            new = new + weight0 * held[c, f, kk, :, lanes(t)]
                        new = jnp.where(live, new, 0.0)
                        if stage < 2:
                            held[index + chunks, f, kk, :, lanes(t)] = new
                        else:
                            state_out[c, f, kk, :, lanes(t)] = new
                            if f < 2:
                                sums[f][t] = sums[f][t] + new
            if stage < 2:
                pack(stage + 1, c)
                launch(stage + 1, c)
            return (tuple(press_e), tuple(press_n)) + tuple(tuple(x) for x in sums)

        start = ((zero,) * tiles,) * (4 if stage == 2 else 2)
        if stage < 2:
            return lax.fori_loop(0, chunks, body, start)
        return lax.fori_loop(1, chunks, body, body(0, start, True))

    run_stage(0, None, 1.0)
    run_stage(1, 0.75, 0.25)
    far_start(0)
    carry = run_stage(2, 1.0 / 3.0, 2.0 / 3.0)

    put_far(1, [
        [floats[1, :, lanes(t)] * (carry[2 + f][t] / levels) for t in range(tiles)]
        for f in range(2)
    ])
    far_start(1)
    whole(gath.at[0], far_recv.at[0]).wait()

    wide = tiles + 1

    def window(kind, f):
        out = []
        for p in range(slots):
            line = [gath[kind, p, f * tiles + t] for t in range(tiles)]
            below = gath[kind, p, 2 * tiles]
            above = gath[kind, p, 2 * tiles + 1]
            if f == 1:
                above = pltpu.roll(above, LANES - RIM, 1)
                below = pltpu.roll(below, RIM, 1)
            line.append(
                jnp.where(lane < RIM, above, jnp.where(lane >= LANES - RIM, below, 0.0))
            )
            out.append(line)
        return out

    def up(z, p, t):
        after = z[p + 1][t] if p + 1 < slots else zero
        return pltpu.roll(jnp.where(row < 1, after, z[p][t]), ROWS - 1, 0)

    def down(z, p, t):
        before = z[p - 1][t] if p > 0 else zero
        return pltpu.roll(jnp.where(row >= ROWS - 1, before, z[p][t]), 1, 0)

    def right(z, p, t):
        return pltpu.roll(jnp.where(lane < 1, z[p][(t + 1) % wide], z[p][t]), LANES - 1, 1)

    def left(z, p, t):
        return pltpu.roll(jnp.where(lane >= LANES - 1, z[p][(t - 1) % wide], z[p][t]), 1, 1)

    def grid(make):
        return [[make(p, t) for t in range(wide)] for p in range(slots)]

    def box(w):
        b = grid(lambda p, t: 4.0 * w[p][t] + (up(w, p, t) + down(w, p, t)))
        return grid(lambda p, t: 4.0 * b[p][t] + (right(b, p, t) + left(b, p, t)))

    x = window(0, 0)
    wet = window(0, 1)
    wet6 = grid(lambda p, t: wet[p][t] * (1.0 / 6.0))
    w = grid(lambda p, t: wet[p][t] * x[p][t])
    image = box(w)
    start = grid(lambda p, t: wet6[p][t] * image[p][t] - 6.0 * w[p][t])

    whole(gath.at[1], far_recv.at[1]).wait()
    fe = window(1, 0)
    fn = window(1, 1)

    def right_side(p, t):
        div = (up(fe, p, t) - down(fe, p, t)) + (right(fn, p, t) - left(fn, p, t))
        return start[p][t] - wet[p][t] * ((0.5 * DIVERGENCE_COEF) * div)

    r = grid(right_side)
    d = grid(lambda p, t: r[p][t] * (1.0 / CHEB_CENTER))
    keeps, gains = cheb_table(ITERS)
    for index in range(ITERS):
        x = grid(lambda p, t: x[p][t] + d[p][t])
        if index < ITERS - 1:
            image = box(d)
            r = grid(
                lambda p, t: (r[p][t] - (SIGMA_SHIFT + 6.0) * d[p][t])
                + wet6[p][t] * image[p][t]
            )
            d = grid(lambda p, t: keeps[index] * d[p][t] + gains[index] * r[p][t])
    dry = dry_factor(ITERS)
    x = grid(lambda p, t: x[p][t] * (dry + (1.0 - dry) * wet[p][t]))

    for t in range(wide):
        xs[0, t] = zero
        xs[slots + 1, t] = zero
    for p in range(slots):
        for t in range(wide):
            xs[p + 1, t] = x[p][t]
    mine = [[xs[own + i, t] for t in range(wide)] for i in range(3)]
    for t in range(tiles):
        surface_out[:, lanes(t)] = mine[1][t]
        above = pltpu.roll(jnp.where(row < 1, mine[2][t], mine[1][t]), ROWS - 1, 0)
        below = pltpu.roll(jnp.where(row >= ROWS - 1, mine[0][t], mine[1][t]), 1, 0)
        slope_out[0, :, lanes(t)] = (above - below) * 0.5
        slope_out[1, :, lanes(t)] = (right(mine, 1, t) - left(mine, 1, t)) * 0.5

    for copy, side, there in near:
        @pl.when(there)
        def _(copy=copy, side=side):
            if copy is x_copy:
                whole(send_x.at[side], side_sem.at[side]).wait()
            else:
                whole(send_y, side_sem.at[2 + side]).wait()
    far(far_drain)


def finish(
    state_ref, slope_ref, surface_ref, wet_ref, active_ref,
    east_out, north_out, salt_out, surface_out, held, sems,
):
    early = (
        pltpu.make_async_copy(surface_ref, surface_out, sems.at[1]),
    ) + tuple(
        pltpu.make_async_copy(
            state_ref.at[c, 2], salt_out.at[pl.ds(c * CHUNK, CHUNK)], sems.at[4 + c]
        )
        for c in range(state_ref.shape[0])
    )
    for copy in early:
        copy.start()
    levels = held.shape[1]
    active = active_ref[...] * wet_ref[...]
    slopes = (slope_ref[0], slope_ref[1])
    for f in range(2):
        for k in range(levels):
            held[f, k] = jnp.where(
                active > k, state_ref[k // CHUNK, f, k % CHUNK] - slopes[f], 0.0
            )
        pltpu.make_async_copy(held.at[f], (east_out, north_out)[f], sems.at[2 + f]).start()
    for f in range(2):
        pltpu.make_async_copy(held.at[f], (east_out, north_out)[f], sems.at[2 + f]).wait()
    for copy in early:
        copy.wait()


def solution(mesh):
    nx, ny = mesh.shape["gx"], mesh.shape["gy"]

    def local(east, north, salt, surface, depth, wet, active):
        levels, rows, width = east.shape
        assert rows == ROWS and width % LANES == 0 and levels % CHUNK == 0
        assert ITERS + 2 <= RIM
        tiles = width // LANES
        chunks = levels // CHUNK
        n = 3 * CHUNK // 4 * tiles
        reach = min(nx - 1, -(-(ITERS + 2) // ROWS))
        slots = min(nx, 2 * reach + 1)
        f32 = jnp.float32
        vmem = pltpu.VMEM
        dma = pltpu.SemaphoreType.DMA
        block = pl.BlockSpec(memory_space=pltpu.VMEM)
        state = jax.ShapeDtypeStruct(east.shape, f32)
        hbm = pl.BlockSpec(memory_space=pltpu.HBM)
        tile = (rows, LANES)
        state3, slopes, surface_next = pl.pallas_call(
            functools.partial(kernel, nx, ny, reach, slots),
            out_shape=(
                jax.ShapeDtypeStruct((chunks, 3, CHUNK, rows, width), f32),
                jax.ShapeDtypeStruct((2,) + surface.shape, f32),
                jax.ShapeDtypeStruct(surface.shape, f32),
            ),
            in_specs=[hbm] * 7,
            out_specs=(block,) * 3,
            scratch_shapes=[
                vmem((3 * chunks, 3, CHUNK, rows, width), f32),
                vmem((3 * chunks, 3, CHUNK, rows, 2 * width), f32),
                vmem((width, 2 * width), jnp.bfloat16),
                vmem((2,) + surface.shape, jnp.int32),
                vmem((2,) + surface.shape, f32),
                vmem((n,) + tile, f32),
                vmem((3, chunks, 2 * n + 2) + tile, f32),
                vmem((2, 3, chunks, n) + tile, f32),
                vmem((3, chunks, 1) + tile, f32),
                vmem((2, 2 * tiles) + tile, f32),
                vmem((2, 1) + tile, f32),
                vmem((2, slots, 2 * tiles + 2) + tile, f32),
                vmem((slots + 2, tiles + 1) + tile, f32),
                dma((chunks,)),
                dma((2,)),
                dma((3, chunks)),
                dma((4,)),
                dma((3, slots)),
                dma((2,)),
            ],
            compiler_params=pltpu.CompilerParams(
                collective_id=0, has_side_effects=True, vmem_limit_bytes=48 * 1024 * 1024
            ),
        )(*[
            pltpu.with_memory_space_constraint(z, pltpu.HBM)
            for z in (east, north, salt, surface, depth, wet, active)
        ])
        return pl.pallas_call(
            finish,
            out_shape=(state, state, state, jax.ShapeDtypeStruct(surface.shape, f32)),
            in_specs=[block] * 5,
            out_specs=(hbm,) * 4,
            scratch_shapes=[vmem((2,) + east.shape, f32), dma((4 + chunks,))],
            compiler_params=pltpu.CompilerParams(vmem_limit_bytes=8 * 1024 * 1024),
        )(state3, slopes, surface_next, wet, active)

    return jax.shard_map(
        local,
        mesh=mesh,
        in_specs=(
            P(None, "gx", "gy"),
            P(None, "gx", "gy"),
            P(None, "gx", "gy"),
            P("gx", "gy"),
            P("gx", "gy"),
            P("gx", "gy"),
            P("gx", "gy"),
        ),
        out_specs=(P(None, "gx", "gy"), P(None, "gx", "gy"), P(None, "gx", "gy"), P("gx", "gy")),
        check_vma=False,
    )
```

```python
import functools

import jax
import jax.numpy as jnp
from jax import lax
from jax.experimental import pallas as pl
from jax.experimental.pallas import tpu as pltpu
from jax.sharding import PartitionSpec as P

ITERS = 16

TIME_STEP = 0.2
CORIOLIS = 0.3
PRESS_COEF = 0.05
VISCOSITY = 0.1
DIFFUSIVITY = 0.1
SIGMA_SHIFT = 0.25
CHEB_CENTER = 3.625
CHEB_HALF = 3.375
DIVERGENCE_COEF = 8.0

ROWS = 8
LANES = 128
CHUNK = 8
RIM = LANES // 4
MESH = pl.DeviceIdType.MESH


def cheb_table(count):
    first = CHEB_CENTER / CHEB_HALF
    ratio = 1.0 / first
    keeps = []
    gains = []
    for index in range(count):
        ratio_next = 1.0 / (2.0 * first - ratio)
        keeps.append(ratio_next * ratio)
        gains.append(2.0 * ratio_next / CHEB_HALF)
        ratio = ratio_next
    return (keeps, gains)


def dry_factor(count):
    keeps, gains = cheb_table(count)
    x, r = 1.0, -1.0
    d = r / CHEB_CENTER
    for index in range(count):
        x = x + d
        r = r - d
        d = keeps[index] * d + gains[index] * r
    return x


def kernel(
    nx, ny, reach, slots,
    east_hbm, north_hbm, salt_hbm, surface_hbm, depth_hbm, wet_hbm, active_hbm,
    state_out, slope_out, surface_out,
    held, moved, shifts, ints, floats, halo, send_x, send_y, far_c, far_e, gath, xs,
    block_count, rim_count, arrivals, blank, small_sem, halo_sem, side_sem, far_send, far_recv,
):
    gx = lax.axis_index("gx")
    gy = lax.axis_index("gy")
    width = held.shape[4]
    tiles = width // LANES
    chunks = held.shape[0] // 3
    levels = chunks * CHUNK
    groups = 3 * CHUNK // 4
    n = groups * tiles
    relative = slots < nx
    row = lax.broadcasted_iota(jnp.int32, (ROWS, LANES), 0)
    lane = lax.broadcasted_iota(jnp.int32, (ROWS, LANES), 1)
    pair = row // 2
    zero = jnp.zeros((ROWS, LANES), jnp.float32)

    def lanes(t):
        return slice(t * LANES, (t + 1) * LANES)

    def inside(x, y):
        return jnp.logical_and(
            jnp.logical_and(x >= 0, x < nx), jnp.logical_and(y >= 0, y < ny)
        )

    def whole(ref, sem):
        return pltpu.make_async_copy(ref, ref, sem)

    def load(c):
        part = pl.ds(c * CHUNK, CHUNK)
        for f, source in enumerate((east_hbm, north_hbm, salt_hbm)):
            pltpu.make_async_copy(source.at[part], held.at[c, f], halo_sem.at[1, c]).start()

    pltpu.make_async_copy(active_hbm, ints.at[0], small_sem.at[0]).start()
    pltpu.make_async_copy(wet_hbm, ints.at[1], small_sem.at[0]).start()
    load(0)

    own = reach if relative else gx
    partners = [
        (o, side)
        for o in range(-reach, reach + 1)
        for side in (-1, 0, 1)
        if (o, side) != (0, 0)
    ]
    partners.sort(key=lambda p: (-abs(p[1]), -abs(p[0])))

    def far(action):
        for o, side in partners:
            @pl.when(inside(gx + o, gy + side))
            def _(o=o, side=side):
                action(o, side)

    def counts(size):
        return (0,) if size == 1 else (1,) if size == 2 else (1, 2)

    has_x = (gx > 0).astype(jnp.int32) + (gx < nx - 1).astype(jnp.int32)
    has_y = (gy > 0).astype(jnp.int32) + (gy < ny - 1).astype(jnp.int32)

    def arrive(stage, c):
        for a in counts(nx):
            for b in counts(ny):
                @pl.when(jnp.logical_and(has_x == a, has_y == b))
                def _(a=a, b=b):
                    part = halo.at[stage, c, pl.ds(0, a * n + b)]
                    whole(part, halo_sem.at[stage, c]).wait()

    def far_arrive(kind):
        for b in counts(ny):
            @pl.when(has_y == b)
            def _(b=b):
                whole(arrivals.at[pl.ds(0, slots * (2 * tiles + b))], far_recv.at[kind]).wait()

    barrier = pltpu.get_barrier_semaphore()
    count = jnp.int32(0)
    for o, side in partners:
        there = inside(gx + o, gy + side)

        @pl.when(there)
        def _(o=o, side=side):
            pl.semaphore_signal(
                barrier, inc=1, device_id=(gx + o, gy + side), device_id_type=MESH
            )

        count = count + there.astype(jnp.int32)

    for c in range(1, chunks):
        load(c)
    pltpu.make_async_copy(surface_hbm, floats.at[0], small_sem.at[1]).start()
    pltpu.make_async_copy(depth_hbm, floats.at[1], small_sem.at[1]).start()

    def move(index):
        value = held[index].reshape(3 * CHUNK * ROWS, width)
        high = value.astype(jnp.bfloat16)
        rest = value - high.astype(jnp.float32)
        middle = rest.astype(jnp.bfloat16)
        low = (rest - middle.astype(jnp.float32)).astype(jnp.bfloat16)
        total = jnp.dot(low, shifts[...], preferred_element_type=jnp.float32)
        total = total + jnp.dot(middle, shifts[...], preferred_element_type=jnp.float32)
        total = total + jnp.dot(high, shifts[...], preferred_element_type=jnp.float32)
        moved[index] = total.reshape(3, CHUNK, ROWS, 2 * width)

    def pack(stage, c):
        rim = zero
        for f in range(3):
            for half in range(CHUNK // 4):
                group = f * (CHUNK // 4) + half
                ups = [None] * tiles
                downs = [None] * tiles
                for m in range(4):
                    kk = half * 4 + m
                    position = group * 4 + m
                    parts = [
                        held[stage * chunks + c, f, kk, :, lanes(t)] for t in range(tiles)
                    ]
                    for t in range(tiles):
                        turned = parts[t] if m == 3 else pltpu.roll(parts[t], 2 * m + 2, 0)
                        if m == 0:
                            ups[t] = turned
                            downs[t] = turned
                        else:
                            ups[t] = jnp.where(pair == m, turned, ups[t])
                            downs[t] = jnp.where(pair == (m + 1) % 4, turned, downs[t])
                    ends = jnp.where(lane < LANES // 2, parts[0], parts[-1])
                    rim = jnp.where(
                        lane // 4 == position,
                        pltpu.roll(ends, (4 * position + 2) % LANES, 1),
                        rim,
                    )
                for t in range(tiles):
                    send_x[0, stage, c, group * tiles + t] = downs[t]
                    send_x[1, stage, c, group * tiles + t] = ups[t]
        send_y[stage, c, 0] = rim

    def x_copy(stage, c, side):
        return pltpu.make_async_remote_copy(
            src_ref=send_x.at[side, stage, c],
            dst_ref=halo.at[stage, c, pl.ds((1 - side) * n, n)],
            send_sem=side_sem.at[side],
            recv_sem=halo_sem.at[stage, c],
            device_id=(gx + 2 * side - 1, gy),
            device_id_type=MESH,
        )

    def y_copy(stage, c, side):
        return pltpu.make_async_remote_copy(
            src_ref=send_y.at[stage, c],
            dst_ref=halo.at[stage, c, pl.ds(2 * n + 1 - side, 1)],
            send_sem=side_sem.at[2 + side],
            recv_sem=halo_sem.at[stage, c],
            device_id=(gx, gy + 2 * side - 1),
            device_id_type=MESH,
        )

    near = [
        (x_copy, 0, gx > 0), (x_copy, 1, gx < nx - 1),
        (y_copy, 0, gy > 0), (y_copy, 1, gy < ny - 1),
    ]

    def launch(stage, c):
        for copy, side, there in near:
            @pl.when(there)
            def _(copy=copy, side=side):
                copy(stage, c, side).start()

    def far_start(kind):
        def action(o, side):
            slot = reach - o if relative else gx
            if side == 0:
                source, target = far_c.at[kind], gath.at[kind, slot, pl.ds(0, 2 * tiles)]
            else:
                at = 2 * tiles + (1 - side) // 2
                source, target = far_e.at[kind], gath.at[kind, slot, pl.ds(at, 1)]
            pltpu.make_async_remote_copy(
                src_ref=source, dst_ref=target,
                send_sem=far_send.at[side + 1, o + reach if relative else 0],
                recv_sem=far_recv.at[kind],
                device_id=(gx + o, gy + side), device_id_type=MESH,
            ).start()

        far(action)
        pltpu.make_async_copy(
            far_c.at[kind], gath.at[kind, own, pl.ds(0, 2 * tiles)], far_recv.at[kind]
        ).start()

    def far_drain(o, side):
        whole(far_c if side == 0 else far_e, far_send.at[side + 1, o + reach]).wait()

    def fill_far(data):
        low, high = data
        first = jnp.where(lane < RIM, low[0], pltpu.roll(high[0], RIM, 1))
        second = jnp.where(
            lane < LANES - RIM, pltpu.roll(high[-1], LANES - RIM, 1), low[-1]
        )
        return jnp.where(lane < 2 * RIM, first, second)

    def put_far(kind, data):
        for f in range(2):
            for t in range(tiles):
                far_c[kind, f * tiles + t] = data[f][t]
        far_e[kind, 0] = fill_far(data)

    for side, missing in ((0, gx == 0), (1, gx == nx - 1)):
        @pl.when(missing)
        def _(side=side):
            for stage in range(3):
                @pl.loop(0, chunks)
                def _(c, stage=stage):
                    halo[stage, c, side * n:(side + 1) * n] = jnp.zeros(
                        (n, ROWS, LANES), jnp.float32
                    )

    for side, missing in ((0, gy == 0), (1, gy == ny - 1)):
        @pl.when(missing)
        def _(side=side):
            halo[:, :, 2 * n + side] = jnp.zeros((3, chunks, ROWS, LANES), jnp.float32)
            gath[:, :, 2 * tiles + side] = jnp.zeros((2, slots, ROWS, LANES), jnp.float32)

    if relative:
        blank[...] = jnp.zeros((2 * tiles, ROWS, LANES), jnp.float32)

    whole(ints, small_sem.at[0]).wait()
    active = [ints[0, :, lanes(t)] * ints[1, :, lanes(t)] for t in range(tiles)]

    def first(c):
        whole(held.at[c], halo_sem.at[1, c]).wait()
        for kk in range(CHUNK):
            for t in range(tiles):
                live = active[t] > c * CHUNK + kk
                for f in range(3):
                    held[c, f, kk, :, lanes(t)] = jnp.where(
                        live, held[c, f, kk, :, lanes(t)], 0.0
                    )
        pack(0, c)

    first(0)
    pl.semaphore_wait(barrier, count)
    launch(0, 0)

    @pl.loop(1, chunks)
    def _(c):
        first(c)
        launch(0, c)

    source = lax.broadcasted_iota(jnp.int32, (width, width), 0)
    target = lax.broadcasted_iota(jnp.int32, (width, width), 1)
    step = source - target
    one = jnp.abs(step) == 1
    sign = jnp.where(step > 0, 1.0, -1.0)
    slope = jnp.where(one, 8.0 * sign, jnp.where(jnp.abs(step) == 2, -sign, 0.0))
    shifts[:, :width] = slope.astype(jnp.bfloat16)
    shifts[:, width:] = jnp.where(one, 1.0, 0.0).astype(jnp.bfloat16)

    if relative:
        for j in range(slots):
            @pl.when(jnp.logical_not(inside(gx + j - reach, gy)))
            def _(j=j):
                for kind in range(2):
                    pltpu.make_async_copy(
                        blank, gath.at[kind, j, pl.ds(0, 2 * tiles)], far_recv.at[kind]
                    ).start()
                    for side, there in ((0, gy > 0), (1, gy < ny - 1)):
                        @pl.when(there)
                        def _(kind=kind, side=side):
                            pltpu.make_async_copy(
                                blank.at[pl.ds(0, 1)],
                                gath.at[kind, j, pl.ds(2 * tiles + side, 1)],
                                far_recv.at[kind],
                            ).start()

    whole(floats, small_sem.at[1]).wait()
    put_far(0, (
        [floats[0, :, lanes(t)] for t in range(tiles)],
        [ints[1, :, lanes(t)].astype(jnp.float32) for t in range(tiles)],
    ))

    @pl.loop(0, chunks - 1)
    def _(c):
        move(c)

    quarter = lane % 4

    def run_stage(stage, weight0, weight1):
        gain = weight1 * TIME_STEP
        keep_flow = weight1 - 4.0 * gain * VISCOSITY
        keep_salt = weight1 - 4.0 * gain * DIFFUSIVITY
        drift = -gain / 12.0
        push = drift * PRESS_COEF

        def body(c, carry, behind=stage < 2):
            press_e, press_n = list(carry[0]), list(carry[1])
            sums = [list(x) for x in carry[2:]]
            index = stage * chunks + c
            arrive(stage, c)
            if behind:
                move(index + chunks - 1)
            rims = jnp.where(quarter < 2, halo[stage, c, 2 * n], halo[stage, c, 2 * n + 1])
            r1, r2 = pltpu.roll(rims, LANES - 1, 1), pltpu.roll(rims, LANES - 2, 1)
            l1, l2 = pltpu.roll(rims, 1, 1), pltpu.roll(rims, 2, 1)
            rim_slope = jnp.where(
                quarter < 2,
                jnp.where(quarter == 0, -r2, 8.0 * r1 - r2),
                jnp.where(quarter == 2, l2 - 8.0 * l1, l2),
            )
            rim_sum = jnp.where(quarter == 1, r1, jnp.where(quarter == 2, l1, 0.0))
            for kk in range(CHUNK):
                fields = []
                for f in range(3):
                    position = f * CHUNK + kk
                    group, m = position // 4, position % 4
                    back = (-(4 * position + 2)) % LANES
                    extra_slope = pltpu.roll(rim_slope, back, 1)
                    extra_sum = pltpu.roll(rim_sum, back, 1)
                    per_tile = []
                    for t in range(tiles):
                        q = held[index, f, kk, :, lanes(t)]
                        ends = jnp.where(
                            pair == m,
                            halo[stage, c, group * tiles + t],
                            halo[stage, c, n + group * tiles + t],
                        )
                        if m != 3:
                            ends = pltpu.roll(ends, (-(2 * m + 2)) % ROWS, 0)
                        e1 = pltpu.roll(jnp.where(row < 1, ends, q), ROWS - 1, 0)
                        e2 = pltpu.roll(jnp.where(row < 2, ends, q), ROWS - 2, 0)
                        w1 = pltpu.roll(jnp.where(row >= ROWS - 1, ends, q), 1, 0)
                        w2 = pltpu.roll(jnp.where(row >= ROWS - 2, ends, q), 2, 0)
                        dy = moved[index, f, kk, :, lanes(t)]
                        sides = moved[index, f, kk, :, lanes(tiles + t)]
                        if t == 0:
                            dy = dy + jnp.where(lane < 2, extra_slope, 0.0)
                            sides = sides + jnp.where(lane < 1, extra_sum, 0.0)
                        if t == tiles - 1:
                            dy = dy + jnp.where(lane >= LANES - 2, extra_slope, 0.0)
                            sides = sides + jnp.where(lane >= LANES - 1, extra_sum, 0.0)
                        dx = 8.0 * (e1 - w1) - (e2 - w2)
                        per_tile.append((q, dx, dy, (e1 + w1) + sides))
                    fields.append(per_tile)
                for t in range(tiles):
                    live = active[t] > c * CHUNK + kk
                    (u, ux, uy, ul), (v, vx, vy, vl), (s, sx, sy, sl) = [
                        fields[f][t] for f in range(3)
                    ]
                    press_e[t] = press_e[t] + sx
                    press_n[t] = press_n[t] + sy
                    um = u * drift
                    vm = v * drift
                    news = [
                        (um * ux + vm * uy) + push * press_e[t] + (gain * CORIOLIS) * v
                        + (gain * VISCOSITY) * ul + keep_flow * u,
                        (um * vx + vm * vy) + push * press_n[t] - (gain * CORIOLIS) * u
                        + (gain * VISCOSITY) * vl + keep_flow * v,
                        (um * sx + vm * sy) + (gain * DIFFUSIVITY) * sl + keep_salt * s,
                    ]
                    for f in range(3):
                        new = news[f]
                        if weight0 is not None:
                            new = new + weight0 * held[c, f, kk, :, lanes(t)]
                        new = jnp.where(live, new, 0.0)
                        if stage < 2:
                            held[index + chunks, f, kk, :, lanes(t)] = new
                        else:
                            state_out[c, f, kk, :, lanes(t)] = new
                            if f < 2:
                                sums[f][t] = sums[f][t] + new
            if stage < 2:
                pack(stage + 1, c)
                launch(stage + 1, c)
            return (tuple(press_e), tuple(press_n)) + tuple(tuple(x) for x in sums)

        start = ((zero,) * tiles,) * (4 if stage == 2 else 2)
        if stage < 2:
            return lax.fori_loop(0, chunks, body, start)
        start = body(0, start, True)
        far_start(0)
        return lax.fori_loop(1, chunks, body, start)

    run_stage(0, None, 1.0)
    run_stage(1, 0.75, 0.25)
    carry = run_stage(2, 1.0 / 3.0, 2.0 / 3.0)

    put_far(1, [
        [floats[1, :, lanes(t)] * (carry[2 + f][t] / levels) for t in range(tiles)]
        for f in range(2)
    ])
    far_start(1)
    far_arrive(0)

    wide = tiles + 1

    def window(kind, f):
        out = []
        for p in range(slots):
            line = [gath[kind, p, f * tiles + t] for t in range(tiles)]
            below = gath[kind, p, 2 * tiles]
            above = gath[kind, p, 2 * tiles + 1]
            if f == 1:
                above = pltpu.roll(above, LANES - RIM, 1)
                below = pltpu.roll(below, RIM, 1)
            line.append(
                jnp.where(lane < RIM, above, jnp.where(lane >= LANES - RIM, below, 0.0))
            )
            out.append(line)
        return out

    def up(z, p, t):
        after = z[p + 1][t] if p + 1 < slots else zero
        return pltpu.roll(jnp.where(row < 1, after, z[p][t]), ROWS - 1, 0)

    def down(z, p, t):
        before = z[p - 1][t] if p > 0 else zero
        return pltpu.roll(jnp.where(row >= ROWS - 1, before, z[p][t]), 1, 0)

    def right(z, p, t):
        return pltpu.roll(jnp.where(lane < 1, z[p][(t + 1) % wide], z[p][t]), LANES - 1, 1)

    def left(z, p, t):
        return pltpu.roll(jnp.where(lane >= LANES - 1, z[p][(t - 1) % wide], z[p][t]), 1, 1)

    def grid(make):
        return [[make(p, t) for t in range(wide)] for p in range(slots)]

    def box(w):
        b = grid(lambda p, t: 4.0 * w[p][t] + (up(w, p, t) + down(w, p, t)))
        return grid(lambda p, t: 4.0 * b[p][t] + (right(b, p, t) + left(b, p, t)))

    x = window(0, 0)
    wet = window(0, 1)
    wet6 = grid(lambda p, t: wet[p][t] * (1.0 / 6.0))
    w = grid(lambda p, t: wet[p][t] * x[p][t])
    image = box(w)
    start = grid(lambda p, t: wet6[p][t] * image[p][t] - 6.0 * w[p][t])

    far_arrive(1)
    fe = window(1, 0)
    fn = window(1, 1)

    def right_side(p, t):
        div = (up(fe, p, t) - down(fe, p, t)) + (right(fn, p, t) - left(fn, p, t))
        return start[p][t] - wet[p][t] * ((0.5 * DIVERGENCE_COEF) * div)

    r = grid(right_side)
    d = grid(lambda p, t: r[p][t] * (1.0 / CHEB_CENTER))
    keeps, gains = cheb_table(ITERS)
    for index in range(ITERS):
        x = grid(lambda p, t: x[p][t] + d[p][t])
        if index < ITERS - 1:
            image = box(d)
            r = grid(
                lambda p, t: (r[p][t] - (SIGMA_SHIFT + 6.0) * d[p][t])
                + wet6[p][t] * image[p][t]
            )
            d = grid(lambda p, t: keeps[index] * d[p][t] + gains[index] * r[p][t])
    dry = dry_factor(ITERS)
    x = grid(lambda p, t: x[p][t] * (dry + (1.0 - dry) * wet[p][t]))

    for t in range(wide):
        xs[0, t] = zero
        xs[slots + 1, t] = zero
    for p in range(slots):
        for t in range(wide):
            xs[p + 1, t] = x[p][t]
    mine = [[xs[own + i, t] for t in range(wide)] for i in range(3)]
    for t in range(tiles):
        surface_out[:, lanes(t)] = mine[1][t]
        above = pltpu.roll(jnp.where(row < 1, mine[2][t], mine[1][t]), ROWS - 1, 0)
        below = pltpu.roll(jnp.where(row >= ROWS - 1, mine[0][t], mine[1][t]), 1, 0)
        slope_out[0, :, lanes(t)] = (above - below) * 0.5
        slope_out[1, :, lanes(t)] = (right(mine, 1, t) - left(mine, 1, t)) * 0.5

    for copy, side, there in near:
        @pl.when(there)
        def _(copy=copy, side=side):
            if copy is x_copy:
                whole(send_x.at[side], side_sem.at[side]).wait()
            else:
                whole(send_y, side_sem.at[2 + side]).wait()
    if relative:
        far(far_drain)
    else:
        if nx > 1:
            whole(block_count, far_send.at[1, 0]).wait()
        for side, there in ((-1, gy > 0), (1, gy < ny - 1)):
            @pl.when(there)
            def _(side=side):
                whole(rim_count, far_send.at[side + 1, 0]).wait()


def finish(
    state_ref, slope_ref, surface_ref, wet_ref, active_ref,
    east_out, north_out, salt_out, surface_out, held, sems,
):
    early = (
        pltpu.make_async_copy(surface_ref, surface_out, sems.at[1]),
    ) + tuple(
        pltpu.make_async_copy(
            state_ref.at[c, 2], salt_out.at[pl.ds(c * CHUNK, CHUNK)], sems.at[4 + c]
        )
        for c in range(state_ref.shape[0])
    )
    for copy in early:
        copy.start()
    levels = held.shape[1]
    active = active_ref[...] * wet_ref[...]
    slopes = (slope_ref[0], slope_ref[1])
    for f in range(2):
        for k in range(levels):
            held[f, k] = jnp.where(
                active > k, state_ref[k // CHUNK, f, k % CHUNK] - slopes[f], 0.0
            )
        pltpu.make_async_copy(held.at[f], (east_out, north_out)[f], sems.at[2 + f]).start()
    for f in range(2):
        pltpu.make_async_copy(held.at[f], (east_out, north_out)[f], sems.at[2 + f]).wait()
    for copy in early:
        copy.wait()


def solution(mesh):
    nx, ny = mesh.shape["gx"], mesh.shape["gy"]

    def local(east, north, salt, surface, depth, wet, active):
        levels, rows, width = east.shape
        assert rows == ROWS and width % LANES == 0 and levels % CHUNK == 0
        assert ITERS + 2 <= RIM
        tiles = width // LANES
        chunks = levels // CHUNK
        n = 3 * CHUNK // 4 * tiles
        reach = min(nx - 1, -(-(ITERS + 2) // ROWS))
        slots = min(nx, 2 * reach + 1)
        f32 = jnp.float32
        vmem = pltpu.VMEM
        dma = pltpu.SemaphoreType.DMA
        block = pl.BlockSpec(memory_space=pltpu.VMEM)
        state = jax.ShapeDtypeStruct(east.shape, f32)
        hbm = pl.BlockSpec(memory_space=pltpu.HBM)
        tile = (rows, LANES)
        state3, slopes, surface_next = pl.pallas_call(
            functools.partial(kernel, nx, ny, reach, slots),
            out_shape=(
                jax.ShapeDtypeStruct((chunks, 3, CHUNK, rows, width), f32),
                jax.ShapeDtypeStruct((2,) + surface.shape, f32),
                jax.ShapeDtypeStruct(surface.shape, f32),
            ),
            in_specs=[hbm] * 7,
            out_specs=(block,) * 3,
            scratch_shapes=[
                vmem((3 * chunks, 3, CHUNK, rows, width), f32),
                vmem((3 * chunks, 3, CHUNK, rows, 2 * width), f32),
                vmem((width, 2 * width), jnp.bfloat16),
                vmem((2,) + surface.shape, jnp.int32),
                vmem((2,) + surface.shape, f32),
                vmem((3, chunks, 2 * n + 2) + tile, f32),
                vmem((2, 3, chunks, n) + tile, f32),
                vmem((3, chunks, 1) + tile, f32),
                vmem((2, 2 * tiles) + tile, f32),
                vmem((2, 1) + tile, f32),
                vmem((2, slots, 2 * tiles + 2) + tile, f32),
                vmem((slots + 2, tiles + 1) + tile, f32),
                vmem((max(slots - 1, 1), 2, 2 * tiles) + tile, f32),
                vmem((slots, 2, 1) + tile, f32),
                vmem((slots * (2 * tiles + 2),) + tile, f32),
                vmem((2 * tiles,) + tile, f32),
                dma((2,)),
                dma((3, chunks)),
                dma((4,)),
                dma((3, slots if slots < nx else 1)),
                dma((2,)),
            ],
            compiler_params=pltpu.CompilerParams(
                collective_id=0, has_side_effects=True, vmem_limit_bytes=48 * 1024 * 1024
            ),
        )(*[
            pltpu.with_memory_space_constraint(z, pltpu.HBM)
            for z in (east, north, salt, surface, depth, wet, active)
        ])
        return pl.pallas_call(
            finish,
            out_shape=(state, state, state, jax.ShapeDtypeStruct(surface.shape, f32)),
            in_specs=[block] * 5,
            out_specs=(hbm,) * 4,
            scratch_shapes=[vmem((2,) + east.shape, f32), dma((4 + chunks,))],
            compiler_params=pltpu.CompilerParams(vmem_limit_bytes=8 * 1024 * 1024),
        )(state3, slopes, surface_next, wet, active)

    return jax.shard_map(
        local,
        mesh=mesh,
        in_specs=(
            P(None, "gx", "gy"),
            P(None, "gx", "gy"),
            P(None, "gx", "gy"),
            P("gx", "gy"),
            P("gx", "gy"),
            P("gx", "gy"),
            P("gx", "gy"),
        ),
        out_specs=(P(None, "gx", "gy"), P(None, "gx", "gy"), P(None, "gx", "gy"), P("gx", "gy")),
        check_vma=False,
    )
```

```python
import functools

import jax
import jax.numpy as jnp
from jax import lax
from jax.experimental import pallas as pl
from jax.experimental.pallas import tpu as pltpu
from jax.sharding import PartitionSpec as P

ITERS = 16

TIME_STEP = 0.2
CORIOLIS = 0.3
PRESS_COEF = 0.05
VISCOSITY = 0.1
DIFFUSIVITY = 0.1
SIGMA_SHIFT = 0.25
CHEB_CENTER = 3.625
CHEB_HALF = 3.375
DIVERGENCE_COEF = 8.0

ROWS = 8
LANES = 128
CHUNK = 8
RIM = LANES // 4
MESH = pl.DeviceIdType.MESH


def cheb_table(count):
    first = CHEB_CENTER / CHEB_HALF
    ratio = 1.0 / first
    keeps = []
    gains = []
    for index in range(count):
        ratio_next = 1.0 / (2.0 * first - ratio)
        keeps.append(ratio_next * ratio)
        gains.append(2.0 * ratio_next / CHEB_HALF)
        ratio = ratio_next
    return (keeps, gains)


def dry_factor(count):
    keeps, gains = cheb_table(count)
    x, r = 1.0, -1.0
    d = r / CHEB_CENTER
    for index in range(count):
        x = x + d
        r = r - d
        d = keeps[index] * d + gains[index] * r
    return x


def kernel(
    nx, ny, reach, slots,
    east_hbm, north_hbm, salt_hbm, surface_hbm, depth_hbm, wet_hbm, active_hbm,
    state_out, slope_out, surface_out,
    held, moved, shifts, ints, floats, halo, send_x, send_y, far_c, far_e, stat_e, gath, xs,
    block_count, rim_count, arrivals, blank, small_sem, halo_sem, side_sem, far_send, far_recv,
    rim_sem, relay_send, relay_recv,
):
    gx = lax.axis_index("gx")
    gy = lax.axis_index("gy")
    width = held.shape[4]
    tiles = width // LANES
    chunks = held.shape[0] // 3
    levels = chunks * CHUNK
    groups = 3 * CHUNK // 4
    n = groups * tiles
    relative = slots < nx
    row = lax.broadcasted_iota(jnp.int32, (ROWS, LANES), 0)
    lane = lax.broadcasted_iota(jnp.int32, (ROWS, LANES), 1)
    pair = row // 2
    zero = jnp.zeros((ROWS, LANES), jnp.float32)

    def lanes(t):
        return slice(t * LANES, (t + 1) * LANES)

    def inside(x, y):
        return jnp.logical_and(
            jnp.logical_and(x >= 0, x < nx), jnp.logical_and(y >= 0, y < ny)
        )

    def whole(ref, sem):
        return pltpu.make_async_copy(ref, ref, sem)

    def load(c):
        part = pl.ds(c * CHUNK, CHUNK)
        for f, source in enumerate((east_hbm, north_hbm, salt_hbm)):
            pltpu.make_async_copy(source.at[part], held.at[c, f], halo_sem.at[1, c]).start()

    pltpu.make_async_copy(active_hbm, ints.at[0], small_sem.at[0]).start()
    pltpu.make_async_copy(wet_hbm, ints.at[1], small_sem.at[0]).start()
    load(0)

    own = reach if relative else gx
    partners = [
        (o, side)
        for o in range(-reach, reach + 1)
        for side in (-1, 0, 1)
        if (o, side) != (0, 0)
    ]
    partners.sort(key=lambda p: (-abs(p[1]), -abs(p[0])))

    def far(action):
        for o, side in partners:
            @pl.when(inside(gx + o, gy + side))
            def _(o=o, side=side):
                action(o, side)

    def counts(size):
        return (0,) if size == 1 else (1,) if size == 2 else (1, 2)

    has_x = (gx > 0).astype(jnp.int32) + (gx < nx - 1).astype(jnp.int32)
    has_y = (gy > 0).astype(jnp.int32) + (gy < ny - 1).astype(jnp.int32)

    def arrive(stage, c):
        for a in counts(nx):
            for b in counts(ny):
                @pl.when(jnp.logical_and(has_x == a, has_y == b))
                def _(a=a, b=b):
                    part = halo.at[stage, c, pl.ds(0, a * n + b)]
                    whole(part, halo_sem.at[stage, c]).wait()

    def far_arrive():
        for b in counts(ny):
            @pl.when(has_y == b)
            def _(b=b):
                whole(arrivals.at[pl.ds(0, slots * (2 * tiles + b))], far_recv.at[0]).wait()

    barrier = pltpu.get_barrier_semaphore()
    count = jnp.int32(0)
    for o, side in partners:
        there = inside(gx + o, gy + side)

        @pl.when(there)
        def _(o=o, side=side):
            pl.semaphore_signal(
                barrier, inc=1, device_id=(gx + o, gy + side), device_id_type=MESH
            )

        count = count + there.astype(jnp.int32)

    for c in range(1, chunks):
        load(c)
    pltpu.make_async_copy(surface_hbm, floats.at[0], small_sem.at[1]).start()
    pltpu.make_async_copy(depth_hbm, floats.at[1], small_sem.at[1]).start()

    def move(index):
        value = held[index].reshape(3 * CHUNK * ROWS, width)
        high = value.astype(jnp.bfloat16)
        rest = value - high.astype(jnp.float32)
        middle = rest.astype(jnp.bfloat16)
        low = (rest - middle.astype(jnp.float32)).astype(jnp.bfloat16)
        total = jnp.dot(
            jnp.concatenate([low, middle, high], axis=1),
            shifts[...],
            preferred_element_type=jnp.float32,
        )
        moved[index] = total.reshape(3, CHUNK, ROWS, 2 * width)

    def pack(stage, c, half):
        for f in range(3):
            ups = [None] * tiles
            downs = [None] * tiles
            for m in range(4):
                for t in range(tiles):
                    part = held[stage * chunks + c, f, half * 4 + m, :, lanes(t)]
                    turned = part if m == 3 else pltpu.roll(part, 2 * m + 2, 0)
                    if m == 0:
                        ups[t] = turned
                        downs[t] = turned
                    else:
                        ups[t] = jnp.where(pair == m, turned, ups[t])
                        downs[t] = jnp.where(pair == (m + 1) % 4, turned, downs[t])
            for t in range(tiles):
                at = (half * 3 + f) * tiles + t
                send_x[0, stage, c, at] = downs[t]
                send_x[1, stage, c, at] = ups[t]

    def pack_rim(stage, c):
        rim = zero
        for f in range(3):
            for kk in range(CHUNK):
                position = f * CHUNK + kk
                first, last = (
                    held[stage * chunks + c, f, kk, :, lanes(t)] for t in (0, tiles - 1)
                )
                rim = jnp.where(
                    lane // 4 == position,
                    pltpu.roll(
                        jnp.where(lane < LANES // 2, first, last),
                        (4 * position + 2) % LANES, 1,
                    ),
                    rim,
                )
        send_y[stage, c, 0] = rim

    def x_copy(stage, c, side):
        return pltpu.make_async_remote_copy(
            src_ref=send_x.at[side, stage, c],
            dst_ref=halo.at[stage, c, pl.ds((1 - side) * n, n)],
            send_sem=side_sem.at[side],
            recv_sem=halo_sem.at[stage, c],
            device_id=(gx + 2 * side - 1, gy),
            device_id_type=MESH,
        )

    def y_copy(stage, c, side):
        return pltpu.make_async_remote_copy(
            src_ref=send_y.at[stage, c],
            dst_ref=halo.at[stage, c, pl.ds(2 * n + 1 - side, 1)],
            send_sem=side_sem.at[2 + side],
            recv_sem=halo_sem.at[stage, c],
            device_id=(gx, gy + 2 * side - 1),
            device_id_type=MESH,
        )

    x_sides = ((0, gx > 0), (1, gx < nx - 1))
    y_sides = ((0, gy > 0), (1, gy < ny - 1))

    def launch_x(stage, c):
        for half in range(CHUNK // 4):
            pack(stage, c, half)
        for side, there in x_sides:
            @pl.when(there)
            def _(side=side):
                x_copy(stage, c, side).start()

    def launch_y(stage, c):
        pack_rim(stage, c)
        for side, there in y_sides:
            @pl.when(there)
            def _(side=side):
                y_copy(stage, c, side).start()

    def far_start():
        def action(o, side):
            slot = reach - o if relative else gx
            if side == 0:
                source, target = far_c, gath.at[1, slot, pl.ds(0, 2 * tiles)]
            else:
                at = 2 * tiles + (1 - side) // 2
                source, target = far_e, gath.at[1, slot, pl.ds(at, 1)]
            pltpu.make_async_remote_copy(
                src_ref=source, dst_ref=target,
                send_sem=far_send.at[side + 1, o + reach if relative else 0],
                recv_sem=far_recv.at[0],
                device_id=(gx + o, gy + side), device_id_type=MESH,
            ).start()

        far(action)
        pltpu.make_async_copy(
            far_c, gath.at[1, own, pl.ds(0, 2 * tiles)], far_recv.at[0]
        ).start()

    def far_drain(o, side):
        whole(far_c if side == 0 else far_e, far_send.at[side + 1, o + reach]).wait()

    def rim_start():
        for side, there in y_sides:
            @pl.when(there)
            def _(side=side):
                pltpu.make_async_remote_copy(
                    src_ref=stat_e,
                    dst_ref=gath.at[0, own, pl.ds(2 * tiles + 1 - side, 1)],
                    send_sem=rim_sem.at[side], recv_sem=rim_sem.at[2],
                    device_id=(gx, gy + 2 * side - 1), device_id_type=MESH,
                ).start()

    def rim_arrive():
        for b in counts(ny):
            @pl.when(has_y == b)
            def _(b=b):
                whole(arrivals.at[pl.ds(0, b)], rim_sem.at[2]).wait()
        for side, there in y_sides:
            @pl.when(there)
            def _(side=side):
                whole(stat_e, rim_sem.at[side]).wait()

    def relay_steps(action, step):
        for side, there in x_sides:
            sign = 2 * side - 1
            passed = gx - sign * (step - 1)
            sends = jnp.logical_and(there, jnp.logical_and(passed >= 0, passed < nx))
            comes = jnp.logical_and(gx - sign * step >= 0, gx - sign * step < nx)
            action(side, sign, sends, comes)

    def relay(step):
        def action(side, sign, sends, comes):
            @pl.when(sends)
            def _():
                source = own - sign * (step - 1)
                target = own - sign * step if relative else source
                pltpu.make_async_remote_copy(
                    src_ref=gath.at[0, source], dst_ref=gath.at[0, target],
                    send_sem=relay_send.at[side], recv_sem=relay_recv.at[side, step - 1],
                    device_id=(gx + sign, gy), device_id_type=MESH,
                ).start()

        relay_steps(action, step)

    def relay_arrive(step):
        def action(side, sign, sends, comes):
            @pl.when(comes)
            def _():
                whole(
                    gath.at[0, own - sign * step], relay_recv.at[side, step - 1]
                ).wait()

            @pl.when(sends)
            def _():
                whole(gath.at[0, own - sign * (step - 1)], relay_send.at[side]).wait()

        relay_steps(action, step)

    def fill_far(data):
        low, high = data
        first = jnp.where(lane < RIM, low[0], pltpu.roll(high[0], RIM, 1))
        second = jnp.where(
            lane < LANES - RIM, pltpu.roll(high[-1], LANES - RIM, 1), low[-1]
        )
        return jnp.where(lane < 2 * RIM, first, second)

    def put(target, data):
        for f in range(2):
            for t in range(tiles):
                target[f * tiles + t] = data[f][t]

    for side, missing in ((0, gx == 0), (1, gx == nx - 1)):
        @pl.when(missing)
        def _(side=side):
            for stage in range(3):
                @pl.loop(0, chunks)
                def _(c, stage=stage):
                    halo[stage, c, side * n:(side + 1) * n] = jnp.zeros(
                        (n, ROWS, LANES), jnp.float32
                    )

    for side, missing in ((0, gy == 0), (1, gy == ny - 1)):
        @pl.when(missing)
        def _(side=side):
            halo[:, :, 2 * n + side] = jnp.zeros((3, chunks, ROWS, LANES), jnp.float32)
            gath[:, :, 2 * tiles + side] = jnp.zeros((2, slots, ROWS, LANES), jnp.float32)

    if relative:
        blank[...] = jnp.zeros((2 * tiles, ROWS, LANES), jnp.float32)

    whole(ints, small_sem.at[0]).wait()
    active = [ints[0, :, lanes(t)] * ints[1, :, lanes(t)] for t in range(tiles)]

    def first(c):
        whole(held.at[c], halo_sem.at[1, c]).wait()
        for kk in range(CHUNK):
            for t in range(tiles):
                live = active[t] > c * CHUNK + kk
                for f in range(3):
                    held[c, f, kk, :, lanes(t)] = jnp.where(
                        live, held[c, f, kk, :, lanes(t)], 0.0
                    )

    def first_launch(c):
        launch_y(0, c)
        launch_x(0, c)

    first(0)
    pl.semaphore_wait(barrier, count)
    first_launch(0)

    @pl.loop(1, chunks)
    def _(c):
        first(c)
        first_launch(c)

    source = lax.broadcasted_iota(jnp.int32, (width, width), 0)
    target = lax.broadcasted_iota(jnp.int32, (width, width), 1)
    step = source - target
    one = jnp.abs(step) == 1
    sign = jnp.where(step > 0, 1.0, -1.0)
    slope = jnp.where(one, 8.0 * sign, jnp.where(jnp.abs(step) == 2, -sign, 0.0))
    for i in range(3):
        part = slice(i * width, (i + 1) * width)
        shifts[part, :width] = slope.astype(jnp.bfloat16)
        shifts[part, width:] = jnp.where(one, 1.0, 0.0).astype(jnp.bfloat16)

    if relative:
        for j in range(slots):
            @pl.when(jnp.logical_not(inside(gx + j - reach, gy)))
            def _(j=j):
                gath[0, j] = jnp.zeros((2 * tiles + 2, ROWS, LANES), jnp.float32)
                pltpu.make_async_copy(
                    blank, gath.at[1, j, pl.ds(0, 2 * tiles)], far_recv.at[0]
                ).start()
                for side, there in y_sides:
                    @pl.when(there)
                    def _(side=side):
                        pltpu.make_async_copy(
                            blank.at[pl.ds(0, 1)],
                            gath.at[1, j, pl.ds(2 * tiles + side, 1)],
                            far_recv.at[0],
                        ).start()

    whole(floats, small_sem.at[1]).wait()
    stats = (
        [floats[0, :, lanes(t)] for t in range(tiles)],
        [ints[1, :, lanes(t)].astype(jnp.float32) for t in range(tiles)],
    )
    put(gath.at[0, own], stats)
    stat_e[0] = fill_far(stats)
    rim_start()

    @pl.loop(0, chunks - 1)
    def _(c):
        move(c)

    quarter = lane % 4

    def run_stage(stage, weight0, weight1):
        gain = weight1 * TIME_STEP
        keep_flow = weight1 - 4.0 * gain * VISCOSITY
        keep_salt = weight1 - 4.0 * gain * DIFFUSIVITY
        drift = -gain / 12.0
        push = drift * PRESS_COEF

        def body(c, carry, behind=stage < 2):
            press_e, press_n = list(carry[0]), list(carry[1])
            sums = [list(x) for x in carry[2:]]
            index = stage * chunks + c
            arrive(stage, c)
            if behind:
                move(index + chunks - 1)
            rims = jnp.where(quarter < 2, halo[stage, c, 2 * n], halo[stage, c, 2 * n + 1])
            r1, r2 = pltpu.roll(rims, LANES - 1, 1), pltpu.roll(rims, LANES - 2, 1)
            l1, l2 = pltpu.roll(rims, 1, 1), pltpu.roll(rims, 2, 1)
            rim_slope = jnp.where(
                quarter < 2,
                jnp.where(quarter == 0, -r2, 8.0 * r1 - r2),
                jnp.where(quarter == 2, l2 - 8.0 * l1, l2),
            )
            rim_sum = jnp.where(quarter == 1, r1, jnp.where(quarter == 2, l1, 0.0))
            for kk in range(CHUNK):
                fields = []
                for f in range(3):
                    position = f * CHUNK + kk
                    group, m = (kk // 4) * 3 + f, kk % 4
                    back = (-(4 * position + 2)) % LANES
                    extra_slope = pltpu.roll(rim_slope, back, 1)
                    extra_sum = pltpu.roll(rim_sum, back, 1)
                    per_tile = []
                    for t in range(tiles):
                        q = held[index, f, kk, :, lanes(t)]
                        ends = jnp.where(
                            pair == m,
                            halo[stage, c, group * tiles + t],
                            halo[stage, c, n + group * tiles + t],
                        )
                        if m != 3:
                            ends = pltpu.roll(ends, (-(2 * m + 2)) % ROWS, 0)
                        e1 = pltpu.roll(jnp.where(row < 1, ends, q), ROWS - 1, 0)
                        e2 = pltpu.roll(jnp.where(row < 2, ends, q), ROWS - 2, 0)
                        w1 = pltpu.roll(jnp.where(row >= ROWS - 1, ends, q), 1, 0)
                        w2 = pltpu.roll(jnp.where(row >= ROWS - 2, ends, q), 2, 0)
                        dy = moved[index, f, kk, :, lanes(t)]
                        sides = moved[index, f, kk, :, lanes(tiles + t)]
                        if t == 0:
                            dy = dy + jnp.where(lane < 2, extra_slope, 0.0)
                            sides = sides + jnp.where(lane < 1, extra_sum, 0.0)
                        if t == tiles - 1:
                            dy = dy + jnp.where(lane >= LANES - 2, extra_slope, 0.0)
                            sides = sides + jnp.where(lane >= LANES - 1, extra_sum, 0.0)
                        dx = 8.0 * (e1 - w1) - (e2 - w2)
                        per_tile.append((q, dx, dy, (e1 + w1) + sides))
                    fields.append(per_tile)
                for t in range(tiles):
                    live = active[t] > c * CHUNK + kk
                    (u, ux, uy, ul), (v, vx, vy, vl), (s, sx, sy, sl) = [
                        fields[f][t] for f in range(3)
                    ]
                    press_e[t] = press_e[t] + sx
                    press_n[t] = press_n[t] + sy
                    um = u * drift
                    vm = v * drift
                    news = [
                        (um * ux + vm * uy) + push * press_e[t] + (gain * CORIOLIS) * v
                        + (gain * VISCOSITY) * ul + keep_flow * u,
                        (um * vx + vm * vy) + push * press_n[t] - (gain * CORIOLIS) * u
                        + (gain * VISCOSITY) * vl + keep_flow * v,
                        (um * sx + vm * sy) + (gain * DIFFUSIVITY) * sl + keep_salt * s,
                    ]
                    for f in range(3):
                        new = news[f]
                        if weight0 is not None:
                            new = new + weight0 * held[c, f, kk, :, lanes(t)]
                        new = jnp.where(live, new, 0.0)
                        if stage < 2:
                            held[index + chunks, f, kk, :, lanes(t)] = new
                        else:
                            state_out[c, f, kk, :, lanes(t)] = new
                            if f < 2:
                                sums[f][t] = sums[f][t] + new
            if stage < 2:
                launch_y(stage + 1, c)
                launch_x(stage + 1, c)
            return (tuple(press_e), tuple(press_n)) + tuple(tuple(x) for x in sums)

        start = ((zero,) * tiles,) * (4 if stage == 2 else 2)
        if stage < 2:
            return lax.fori_loop(0, chunks, body, start)
        return lax.fori_loop(1, chunks, body, body(0, start, True))

    def pass_on(step):
        if step == 1:
            rim_arrive()
        elif step - 1 <= reach:
            relay_arrive(step - 1)
        if step <= reach:
            relay(step)

    run_stage(0, None, 1.0)
    pass_on(1)
    run_stage(1, 0.75, 0.25)
    pass_on(2)
    carry = run_stage(2, 1.0 / 3.0, 2.0 / 3.0)

    flows = [
        [floats[1, :, lanes(t)] * (carry[2 + f][t] / levels) for t in range(tiles)]
        for f in range(2)
    ]
    put(far_c, flows)
    far_e[0] = fill_far(flows)
    far_start()
    pass_on(3)
    pass_on(4)

    wide = tiles + 1

    def window(kind, f):
        out = []
        for p in range(slots):
            line = [gath[kind, p, f * tiles + t] for t in range(tiles)]
            below = gath[kind, p, 2 * tiles]
            above = gath[kind, p, 2 * tiles + 1]
            if f == 1:
                above = pltpu.roll(above, LANES - RIM, 1)
                below = pltpu.roll(below, RIM, 1)
            line.append(
                jnp.where(lane < RIM, above, jnp.where(lane >= LANES - RIM, below, 0.0))
            )
            out.append(line)
        return out

    def up(z, p, t):
        after = z[p + 1][t] if p + 1 < slots else zero
        return pltpu.roll(jnp.where(row < 1, after, z[p][t]), ROWS - 1, 0)

    def down(z, p, t):
        before = z[p - 1][t] if p > 0 else zero
        return pltpu.roll(jnp.where(row >= ROWS - 1, before, z[p][t]), 1, 0)

    def right(z, p, t):
        return pltpu.roll(jnp.where(lane < 1, z[p][(t + 1) % wide], z[p][t]), LANES - 1, 1)

    def left(z, p, t):
        return pltpu.roll(jnp.where(lane >= LANES - 1, z[p][(t - 1) % wide], z[p][t]), 1, 1)

    def grid(make):
        return [[make(p, t) for t in range(wide)] for p in range(slots)]

    def box(w):
        b = grid(lambda p, t: 4.0 * w[p][t] + (up(w, p, t) + down(w, p, t)))
        return grid(lambda p, t: 4.0 * b[p][t] + (right(b, p, t) + left(b, p, t)))

    x = window(0, 0)
    wet = window(0, 1)
    wet6 = grid(lambda p, t: wet[p][t] * (1.0 / 6.0))
    w = grid(lambda p, t: wet[p][t] * x[p][t])
    image = box(w)
    start = grid(lambda p, t: wet6[p][t] * image[p][t] - 6.0 * w[p][t])

    far_arrive()
    fe = window(1, 0)
    fn = window(1, 1)

    def right_side(p, t):
        div = (up(fe, p, t) - down(fe, p, t)) + (right(fn, p, t) - left(fn, p, t))
        return start[p][t] - wet[p][t] * ((0.5 * DIVERGENCE_COEF) * div)

    r = grid(right_side)
    d = grid(lambda p, t: r[p][t] * (1.0 / CHEB_CENTER))
    keeps, gains = cheb_table(ITERS)
    for index in range(ITERS):
        x = grid(lambda p, t: x[p][t] + d[p][t])
        if index < ITERS - 1:
            image = box(d)
            r = grid(
                lambda p, t: (r[p][t] - (SIGMA_SHIFT + 6.0) * d[p][t])
                + wet6[p][t] * image[p][t]
            )
            d = grid(lambda p, t: keeps[index] * d[p][t] + gains[index] * r[p][t])
    dry = dry_factor(ITERS)
    x = grid(lambda p, t: x[p][t] * (dry + (1.0 - dry) * wet[p][t]))

    for t in range(wide):
        xs[0, t] = zero
        xs[slots + 1, t] = zero
    for p in range(slots):
        for t in range(wide):
            xs[p + 1, t] = x[p][t]
    mine = [[xs[own + i, t] for t in range(wide)] for i in range(3)]
    for t in range(tiles):
        surface_out[:, lanes(t)] = mine[1][t]
        above = pltpu.roll(jnp.where(row < 1, mine[2][t], mine[1][t]), ROWS - 1, 0)
        below = pltpu.roll(jnp.where(row >= ROWS - 1, mine[0][t], mine[1][t]), 1, 0)
        slope_out[0, :, lanes(t)] = (above - below) * 0.5
        slope_out[1, :, lanes(t)] = (right(mine, 1, t) - left(mine, 1, t)) * 0.5

    for side, there in x_sides:
        @pl.when(there)
        def _(side=side):
            whole(send_x.at[side], side_sem.at[side]).wait()

    for side, there in y_sides:
        @pl.when(there)
        def _(side=side):
            whole(send_y, side_sem.at[2 + side]).wait()

    if relative:
        far(far_drain)
    else:
        if nx > 1:
            whole(block_count, far_send.at[1, 0]).wait()
        for side, there in ((-1, gy > 0), (1, gy < ny - 1)):
            @pl.when(there)
            def _(side=side):
                whole(rim_count, far_send.at[side + 1, 0]).wait()


def finish(
    state_ref, slope_ref, surface_ref, wet_ref, active_ref,
    east_out, north_out, salt_out, surface_out, held, sems,
):
    early = (
        pltpu.make_async_copy(surface_ref, surface_out, sems.at[1]),
    ) + tuple(
        pltpu.make_async_copy(
            state_ref.at[c, 2], salt_out.at[pl.ds(c * CHUNK, CHUNK)], sems.at[4 + c]
        )
        for c in range(state_ref.shape[0])
    )
    for copy in early:
        copy.start()
    levels = held.shape[1]
    active = active_ref[...] * wet_ref[...]
    slopes = (slope_ref[0], slope_ref[1])
    for f in range(2):
        for k in range(levels):
            held[f, k] = jnp.where(
                active > k, state_ref[k // CHUNK, f, k % CHUNK] - slopes[f], 0.0
            )
        pltpu.make_async_copy(held.at[f], (east_out, north_out)[f], sems.at[2 + f]).start()
    for f in range(2):
        pltpu.make_async_copy(held.at[f], (east_out, north_out)[f], sems.at[2 + f]).wait()
    for copy in early:
        copy.wait()


def solution(mesh):
    nx, ny = mesh.shape["gx"], mesh.shape["gy"]

    def local(east, north, salt, surface, depth, wet, active):
        levels, rows, width = east.shape
        assert rows == ROWS and width % LANES == 0 and levels % CHUNK == 0
        assert ITERS + 2 <= RIM and ITERS + 2 <= 3 * ROWS
        tiles = width // LANES
        chunks = levels // CHUNK
        n = 3 * CHUNK // 4 * tiles
        reach = min(nx - 1, -(-(ITERS + 2) // ROWS))
        slots = min(nx, 2 * reach + 1)
        f32 = jnp.float32
        vmem = pltpu.VMEM
        dma = pltpu.SemaphoreType.DMA
        block = pl.BlockSpec(memory_space=pltpu.VMEM)
        state = jax.ShapeDtypeStruct(east.shape, f32)
        hbm = pl.BlockSpec(memory_space=pltpu.HBM)
        tile = (rows, LANES)
        state3, slopes, surface_next = pl.pallas_call(
            functools.partial(kernel, nx, ny, reach, slots),
            out_shape=(
                jax.ShapeDtypeStruct((chunks, 3, CHUNK, rows, width), f32),
                jax.ShapeDtypeStruct((2,) + surface.shape, f32),
                jax.ShapeDtypeStruct(surface.shape, f32),
            ),
            in_specs=[hbm] * 7,
            out_specs=(block,) * 3,
            scratch_shapes=[
                vmem((3 * chunks, 3, CHUNK, rows, width), f32),
                vmem((3 * chunks, 3, CHUNK, rows, 2 * width), f32),
                vmem((3 * width, 2 * width), jnp.bfloat16),
                vmem((2,) + surface.shape, jnp.int32),
                vmem((2,) + surface.shape, f32),
                vmem((3, chunks, 2 * n + 2) + tile, f32),
                vmem((2, 3, chunks, n) + tile, f32),
                vmem((3, chunks, 1) + tile, f32),
                vmem((2 * tiles,) + tile, f32),
                vmem((1,) + tile, f32),
                vmem((1,) + tile, f32),
                vmem((2, slots, 2 * tiles + 2) + tile, f32),
                vmem((slots + 2, tiles + 1) + tile, f32),
                vmem((max(slots - 1, 1), 2 * tiles) + tile, f32),
                vmem((slots,) + tile, f32),
                vmem((slots * (2 * tiles + 2),) + tile, f32),
                vmem((2 * tiles,) + tile, f32),
                dma((2,)),
                dma((3, chunks)),
                dma((4,)),
                dma((3, slots if slots < nx else 1)),
                dma((1,)),
                dma((3,)),
                dma((2,)),
                dma((2, max(reach, 1))),
            ],
            compiler_params=pltpu.CompilerParams(
                collective_id=0, has_side_effects=True, vmem_limit_bytes=48 * 1024 * 1024
            ),
        )(*[
            pltpu.with_memory_space_constraint(z, pltpu.HBM)
            for z in (east, north, salt, surface, depth, wet, active)
        ])
        return pl.pallas_call(
            finish,
            out_shape=(state, state, state, jax.ShapeDtypeStruct(surface.shape, f32)),
            in_specs=[block] * 5,
            out_specs=(hbm,) * 4,
            scratch_shapes=[vmem((2,) + east.shape, f32), dma((4 + chunks,))],
            compiler_params=pltpu.CompilerParams(vmem_limit_bytes=8 * 1024 * 1024),
        )(state3, slopes, surface_next, wet, active)

    return jax.shard_map(
        local,
        mesh=mesh,
        in_specs=(
            P(None, "gx", "gy"),
            P(None, "gx", "gy"),
            P(None, "gx", "gy"),
            P("gx", "gy"),
            P("gx", "gy"),
            P("gx", "gy"),
            P("gx", "gy"),
        ),
        out_specs=(P(None, "gx", "gy"), P(None, "gx", "gy"), P(None, "gx", "gy"), P("gx", "gy")),
        check_vma=False,
    )
```

```python
import functools

import jax
import jax.numpy as jnp
from jax import lax
from jax.experimental import pallas as pl
from jax.experimental.pallas import tpu as pltpu
from jax.sharding import PartitionSpec as P

ITERS = 16

TIME_STEP = 0.2
CORIOLIS = 0.3
PRESS_COEF = 0.05
VISCOSITY = 0.1
DIFFUSIVITY = 0.1
SIGMA_SHIFT = 0.25
CHEB_CENTER = 3.625
CHEB_HALF = 3.375
DIVERGENCE_COEF = 8.0

ROWS = 8
LANES = 128
CHUNK = 8
RIM = LANES // 4
MESH = pl.DeviceIdType.MESH


def cheb_table(count):
    first = CHEB_CENTER / CHEB_HALF
    ratio = 1.0 / first
    keeps = []
    gains = []
    for index in range(count):
        ratio_next = 1.0 / (2.0 * first - ratio)
        keeps.append(ratio_next * ratio)
        gains.append(2.0 * ratio_next / CHEB_HALF)
        ratio = ratio_next
    return (keeps, gains)


def dry_factor(count):
    keeps, gains = cheb_table(count)
    x, r = 1.0, -1.0
    d = r / CHEB_CENTER
    for index in range(count):
        x = x + d
        r = r - d
        d = keeps[index] * d + gains[index] * r
    return x


def kernel(
    nx, ny, reach, slots,
    east_hbm, north_hbm, salt_hbm, surface_hbm, depth_hbm, wet_hbm, active_hbm,
    state_out, slope_out, surface_out,
    held, moved, shifts, ints, floats, halo, send_x, send_y, far_c, far_e, stat_e, gath, xs,
    block_count, rim_count, arrivals, blank, small_sem, halo_sem, side_sem, far_send, far_recv,
    rim_sem, relay_send, relay_recv,
):
    gx = lax.axis_index("gx")
    gy = lax.axis_index("gy")
    width = held.shape[4]
    tiles = width // LANES
    chunks = held.shape[0] // 3
    levels = chunks * CHUNK
    groups = 3 * CHUNK // 4
    n = groups * tiles
    relative = slots < nx
    row = lax.broadcasted_iota(jnp.int32, (ROWS, LANES), 0)
    lane = lax.broadcasted_iota(jnp.int32, (ROWS, LANES), 1)
    pair = row // 2
    zero = jnp.zeros((ROWS, LANES), jnp.float32)

    def lanes(t):
        return slice(t * LANES, (t + 1) * LANES)

    def inside(x, y):
        return jnp.logical_and(
            jnp.logical_and(x >= 0, x < nx), jnp.logical_and(y >= 0, y < ny)
        )

    def whole(ref, sem):
        return pltpu.make_async_copy(ref, ref, sem)

    def load(c):
        part = pl.ds(c * CHUNK, CHUNK)
        for f, source in enumerate((east_hbm, north_hbm, salt_hbm)):
            pltpu.make_async_copy(source.at[part], held.at[c, f], halo_sem.at[1, c]).start()

    pltpu.make_async_copy(active_hbm, ints.at[0], small_sem.at[0]).start()
    pltpu.make_async_copy(wet_hbm, ints.at[1], small_sem.at[0]).start()
    load(0)

    own = reach if relative else gx
    partners = [
        (o, side)
        for o in range(-reach, reach + 1)
        for side in (-1, 0, 1)
        if (o, side) != (0, 0)
    ]
    partners.sort(key=lambda p: (-abs(p[1]), -abs(p[0])))

    def far(action):
        for o, side in partners:
            @pl.when(inside(gx + o, gy + side))
            def _(o=o, side=side):
                action(o, side)

    def counts(size):
        return (0,) if size == 1 else (1,) if size == 2 else (1, 2)

    has_x = (gx > 0).astype(jnp.int32) + (gx < nx - 1).astype(jnp.int32)
    has_y = (gy > 0).astype(jnp.int32) + (gy < ny - 1).astype(jnp.int32)

    def arrive(stage, c):
        for a in counts(nx):
            for b in counts(ny):
                @pl.when(jnp.logical_and(has_x == a, has_y == b))
                def _(a=a, b=b):
                    part = halo.at[stage, c, pl.ds(0, a * n + b)]
                    whole(part, halo_sem.at[stage, c]).wait()

    def far_arrive():
        for b in counts(ny):
            @pl.when(has_y == b)
            def _(b=b):
                whole(arrivals.at[pl.ds(0, slots * (2 * tiles + b))], far_recv.at[0]).wait()

    barrier = pltpu.get_barrier_semaphore()
    count = jnp.int32(0)
    for o, side in ((-1, 0), (1, 0), (0, -1), (0, 1)):
        there = inside(gx + o, gy + side)

        @pl.when(there)
        def _(o=o, side=side):
            pl.semaphore_signal(
                barrier, inc=1, device_id=(gx + o, gy + side), device_id_type=MESH
            )

        count = count + there.astype(jnp.int32)

    for c in range(1, chunks):
        load(c)
    pltpu.make_async_copy(surface_hbm, floats.at[0], small_sem.at[1]).start()
    pltpu.make_async_copy(depth_hbm, floats.at[1], small_sem.at[1]).start()

    def move(index):
        value = held[index].reshape(3 * CHUNK * ROWS, width)
        high = value.astype(jnp.bfloat16)
        rest = value - high.astype(jnp.float32)
        middle = rest.astype(jnp.bfloat16)
        low = (rest - middle.astype(jnp.float32)).astype(jnp.bfloat16)
        total = jnp.dot(
            jnp.concatenate([low, middle, high], axis=1),
            shifts[...],
            preferred_element_type=jnp.float32,
        )
        moved[index] = total.reshape(3, CHUNK, ROWS, 2 * width)

    def pack(stage, c, half):
        for f in range(3):
            ups = [None] * tiles
            downs = [None] * tiles
            for m in range(4):
                for t in range(tiles):
                    part = held[stage * chunks + c, f, half * 4 + m, :, lanes(t)]
                    turned = part if m == 3 else pltpu.roll(part, 2 * m + 2, 0)
                    if m == 0:
                        ups[t] = turned
                        downs[t] = turned
                    else:
                        ups[t] = jnp.where(pair == m, turned, ups[t])
                        downs[t] = jnp.where(pair == (m + 1) % 4, turned, downs[t])
            for t in range(tiles):
                at = (half * 3 + f) * tiles + t
                send_x[0, stage, c, at] = downs[t]
                send_x[1, stage, c, at] = ups[t]

    def pack_rim(stage, c):
        rim = zero
        for f in range(3):
            for kk in range(CHUNK):
                position = f * CHUNK + kk
                first, last = (
                    held[stage * chunks + c, f, kk, :, lanes(t)] for t in (0, tiles - 1)
                )
                rim = jnp.where(
                    lane // 4 == position,
                    pltpu.roll(
                        jnp.where(lane < LANES // 2, first, last),
                        (4 * position + 2) % LANES, 1,
                    ),
                    rim,
                )
        send_y[stage, c, 0] = rim

    def x_copy(stage, c, side):
        return pltpu.make_async_remote_copy(
            src_ref=send_x.at[side, stage, c],
            dst_ref=halo.at[stage, c, pl.ds((1 - side) * n, n)],
            send_sem=side_sem.at[side],
            recv_sem=halo_sem.at[stage, c],
            device_id=(gx + 2 * side - 1, gy),
            device_id_type=MESH,
        )

    def y_copy(stage, c, side):
        return pltpu.make_async_remote_copy(
            src_ref=send_y.at[stage, c],
            dst_ref=halo.at[stage, c, pl.ds(2 * n + 1 - side, 1)],
            send_sem=side_sem.at[2 + side],
            recv_sem=halo_sem.at[stage, c],
            device_id=(gx, gy + 2 * side - 1),
            device_id_type=MESH,
        )

    x_sides = ((0, gx > 0), (1, gx < nx - 1))
    y_sides = ((0, gy > 0), (1, gy < ny - 1))

    def launch_x(stage, c):
        for half in range(CHUNK // 4):
            pack(stage, c, half)
        for side, there in x_sides:
            @pl.when(there)
            def _(side=side):
                x_copy(stage, c, side).start()

    def launch_y(stage, c):
        pack_rim(stage, c)
        for side, there in y_sides:
            @pl.when(there)
            def _(side=side):
                y_copy(stage, c, side).start()

    def far_start():
        def action(o, side):
            slot = reach - o if relative else gx
            if side == 0:
                source, target = far_c, gath.at[1, slot, pl.ds(0, 2 * tiles)]
            else:
                at = 2 * tiles + (1 - side) // 2
                source, target = far_e, gath.at[1, slot, pl.ds(at, 1)]
            pltpu.make_async_remote_copy(
                src_ref=source, dst_ref=target,
                send_sem=far_send.at[side + 1, o + reach if relative else 0],
                recv_sem=far_recv.at[0],
                device_id=(gx + o, gy + side), device_id_type=MESH,
            ).start()

        far(action)
        pltpu.make_async_copy(
            far_c, gath.at[1, own, pl.ds(0, 2 * tiles)], far_recv.at[0]
        ).start()

    def far_drain(o, side):
        whole(far_c if side == 0 else far_e, far_send.at[side + 1, o + reach]).wait()

    def rim_start():
        for side, there in y_sides:
            @pl.when(there)
            def _(side=side):
                pltpu.make_async_remote_copy(
                    src_ref=stat_e,
                    dst_ref=gath.at[0, own, pl.ds(2 * tiles + 1 - side, 1)],
                    send_sem=rim_sem.at[side], recv_sem=rim_sem.at[2],
                    device_id=(gx, gy + 2 * side - 1), device_id_type=MESH,
                ).start()

    def rim_arrive():
        for b in counts(ny):
            @pl.when(has_y == b)
            def _(b=b):
                whole(arrivals.at[pl.ds(0, b)], rim_sem.at[2]).wait()
        for side, there in y_sides:
            @pl.when(there)
            def _(side=side):
                whole(stat_e, rim_sem.at[side]).wait()

    def relay_steps(action, step):
        for side, there in x_sides:
            sign = 2 * side - 1
            passed = gx - sign * (step - 1)
            sends = jnp.logical_and(there, jnp.logical_and(passed >= 0, passed < nx))
            comes = jnp.logical_and(gx - sign * step >= 0, gx - sign * step < nx)
            action(side, sign, sends, comes)

    def relay(step):
        def action(side, sign, sends, comes):
            @pl.when(sends)
            def _():
                source = own - sign * (step - 1)
                target = own - sign * step if relative else source
                pltpu.make_async_remote_copy(
                    src_ref=gath.at[0, source], dst_ref=gath.at[0, target],
                    send_sem=relay_send.at[side], recv_sem=relay_recv.at[side, step - 1],
                    device_id=(gx + sign, gy), device_id_type=MESH,
                ).start()

        relay_steps(action, step)

    def relay_arrive(step):
        def action(side, sign, sends, comes):
            @pl.when(comes)
            def _():
                whole(
                    gath.at[0, own - sign * step], relay_recv.at[side, step - 1]
                ).wait()

            @pl.when(sends)
            def _():
                whole(gath.at[0, own - sign * (step - 1)], relay_send.at[side]).wait()

        relay_steps(action, step)

    def fill_far(data):
        low, high = data
        first = jnp.where(lane < RIM, low[0], pltpu.roll(high[0], RIM, 1))
        second = jnp.where(
            lane < LANES - RIM, pltpu.roll(high[-1], LANES - RIM, 1), low[-1]
        )
        return jnp.where(lane < 2 * RIM, first, second)

    def put(target, data):
        for f in range(2):
            for t in range(tiles):
                target[f * tiles + t] = data[f][t]

    for side, missing in ((0, gx == 0), (1, gx == nx - 1)):
        @pl.when(missing)
        def _(side=side):
            for stage in range(3):
                @pl.loop(0, chunks)
                def _(c, stage=stage):
                    halo[stage, c, side * n:(side + 1) * n] = jnp.zeros(
                        (n, ROWS, LANES), jnp.float32
                    )

    for side, missing in ((0, gy == 0), (1, gy == ny - 1)):
        @pl.when(missing)
        def _(side=side):
            halo[:, :, 2 * n + side] = jnp.zeros((3, chunks, ROWS, LANES), jnp.float32)
            gath[:, :, 2 * tiles + side] = jnp.zeros((2, slots, ROWS, LANES), jnp.float32)

    if relative:
        blank[...] = jnp.zeros((2 * tiles, ROWS, LANES), jnp.float32)

    whole(ints, small_sem.at[0]).wait()
    active = [ints[0, :, lanes(t)] * ints[1, :, lanes(t)] for t in range(tiles)]

    def first(c):
        whole(held.at[c], halo_sem.at[1, c]).wait()
        for kk in range(CHUNK):
            for t in range(tiles):
                live = active[t] > c * CHUNK + kk
                for f in range(3):
                    held[c, f, kk, :, lanes(t)] = jnp.where(
                        live, held[c, f, kk, :, lanes(t)], 0.0
                    )

    def first_launch(c):
        launch_y(0, c)
        launch_x(0, c)

    first(0)
    pl.semaphore_wait(barrier, count)
    first_launch(0)

    @pl.loop(1, chunks)
    def _(c):
        first(c)
        first_launch(c)

    source = lax.broadcasted_iota(jnp.int32, (width, width), 0)
    target = lax.broadcasted_iota(jnp.int32, (width, width), 1)
    step = source - target
    one = jnp.abs(step) == 1
    sign = jnp.where(step > 0, 1.0, -1.0)
    slope = jnp.where(one, 8.0 * sign, jnp.where(jnp.abs(step) == 2, -sign, 0.0))
    for i in range(3):
        part = slice(i * width, (i + 1) * width)
        shifts[part, :width] = slope.astype(jnp.bfloat16)
        shifts[part, width:] = jnp.where(one, 1.0, 0.0).astype(jnp.bfloat16)

    if relative:
        for j in range(slots):
            @pl.when(jnp.logical_not(inside(gx + j - reach, gy)))
            def _(j=j):
                gath[0, j] = jnp.zeros((2 * tiles + 2, ROWS, LANES), jnp.float32)
                pltpu.make_async_copy(
                    blank, gath.at[1, j, pl.ds(0, 2 * tiles)], far_recv.at[0]
                ).start()
                for side, there in y_sides:
                    @pl.when(there)
                    def _(side=side):
                        pltpu.make_async_copy(
                            blank.at[pl.ds(0, 1)],
                            gath.at[1, j, pl.ds(2 * tiles + side, 1)],
                            far_recv.at[0],
                        ).start()

    whole(floats, small_sem.at[1]).wait()
    stats = (
        [floats[0, :, lanes(t)] for t in range(tiles)],
        [ints[1, :, lanes(t)].astype(jnp.float32) for t in range(tiles)],
    )
    put(gath.at[0, own], stats)
    stat_e[0] = fill_far(stats)
    rim_start()

    @pl.loop(0, chunks - 1)
    def _(c):
        move(c)

    quarter = lane % 4

    def run_stage(stage, weight0, weight1):
        gain = weight1 * TIME_STEP
        keep_flow = weight1 - 4.0 * gain * VISCOSITY
        keep_salt = weight1 - 4.0 * gain * DIFFUSIVITY
        drift = -gain / 12.0
        push = drift * PRESS_COEF

        def body(c, carry, behind=stage < 2):
            press_e, press_n = list(carry[0]), list(carry[1])
            sums = [list(x) for x in carry[2:]]
            index = stage * chunks + c
            arrive(stage, c)
            if behind:
                move(index + chunks - 1)
            rims = jnp.where(quarter < 2, halo[stage, c, 2 * n], halo[stage, c, 2 * n + 1])
            r1, r2 = pltpu.roll(rims, LANES - 1, 1), pltpu.roll(rims, LANES - 2, 1)
            l1, l2 = pltpu.roll(rims, 1, 1), pltpu.roll(rims, 2, 1)
            rim_slope = jnp.where(
                quarter < 2,
                jnp.where(quarter == 0, -r2, 8.0 * r1 - r2),
                jnp.where(quarter == 2, l2 - 8.0 * l1, l2),
            )
            rim_sum = jnp.where(quarter == 1, r1, jnp.where(quarter == 2, l1, 0.0))
            for kk in range(CHUNK):
                fields = []
                for f in range(3):
                    position = f * CHUNK + kk
                    group, m = (kk // 4) * 3 + f, kk % 4
                    back = (-(4 * position + 2)) % LANES
                    extra_slope = pltpu.roll(rim_slope, back, 1)
                    extra_sum = pltpu.roll(rim_sum, back, 1)
                    per_tile = []
                    for t in range(tiles):
                        q = held[index, f, kk, :, lanes(t)]
                        ends = jnp.where(
                            pair == m,
                            halo[stage, c, group * tiles + t],
                            halo[stage, c, n + group * tiles + t],
                        )
                        if m != 3:
                            ends = pltpu.roll(ends, (-(2 * m + 2)) % ROWS, 0)
                        e1 = pltpu.roll(jnp.where(row < 1, ends, q), ROWS - 1, 0)
                        e2 = pltpu.roll(jnp.where(row < 2, ends, q), ROWS - 2, 0)
                        w1 = pltpu.roll(jnp.where(row >= ROWS - 1, ends, q), 1, 0)
                        w2 = pltpu.roll(jnp.where(row >= ROWS - 2, ends, q), 2, 0)
                        dy = moved[index, f, kk, :, lanes(t)]
                        sides = moved[index, f, kk, :, lanes(tiles + t)]
                        if t == 0:
                            dy = dy + jnp.where(lane < 2, extra_slope, 0.0)
                            sides = sides + jnp.where(lane < 1, extra_sum, 0.0)
                        if t == tiles - 1:
                            dy = dy + jnp.where(lane >= LANES - 2, extra_slope, 0.0)
                            sides = sides + jnp.where(lane >= LANES - 1, extra_sum, 0.0)
                        dx = 8.0 * (e1 - w1) - (e2 - w2)
                        per_tile.append((q, dx, dy, (e1 + w1) + sides))
                    fields.append(per_tile)
                for t in range(tiles):
                    live = active[t] > c * CHUNK + kk
                    (u, ux, uy, ul), (v, vx, vy, vl), (s, sx, sy, sl) = [
                        fields[f][t] for f in range(3)
                    ]
                    press_e[t] = press_e[t] + sx
                    press_n[t] = press_n[t] + sy
                    um = u * drift
                    vm = v * drift
                    news = [
                        (um * ux + vm * uy) + push * press_e[t] + (gain * CORIOLIS) * v
                        + (gain * VISCOSITY) * ul + keep_flow * u,
                        (um * vx + vm * vy) + push * press_n[t] - (gain * CORIOLIS) * u
                        + (gain * VISCOSITY) * vl + keep_flow * v,
                        (um * sx + vm * sy) + (gain * DIFFUSIVITY) * sl + keep_salt * s,
                    ]
                    for f in range(3):
                        new = news[f]
                        if weight0 is not None:
                            new = new + weight0 * held[c, f, kk, :, lanes(t)]
                        new = jnp.where(live, new, 0.0)
                        if stage < 2:
                            held[index + chunks, f, kk, :, lanes(t)] = new
                        else:
                            state_out[c, f, kk, :, lanes(t)] = new
                            if f < 2:
                                sums[f][t] = sums[f][t] + new
            if stage < 2:
                launch_y(stage + 1, c)
                launch_x(stage + 1, c)
            return (tuple(press_e), tuple(press_n)) + tuple(tuple(x) for x in sums)

        start = ((zero,) * tiles,) * (4 if stage == 2 else 2)
        if stage < 2:
            return lax.fori_loop(0, chunks, body, start)
        return lax.fori_loop(1, chunks, body, body(0, start, True))

    def pass_on(step):
        if step == 1:
            rim_arrive()
        elif step - 1 <= reach:
            relay_arrive(step - 1)
        if step <= reach:
            relay(step)

    run_stage(0, None, 1.0)
    pass_on(1)
    run_stage(1, 0.75, 0.25)
    pass_on(2)
    carry = run_stage(2, 1.0 / 3.0, 2.0 / 3.0)

    flows = [
        [floats[1, :, lanes(t)] * (carry[2 + f][t] / levels) for t in range(tiles)]
        for f in range(2)
    ]
    put(far_c, flows)
    far_e[0] = fill_far(flows)
    far_start()
    pass_on(3)
    pass_on(4)

    wide = tiles + 1

    def window(kind, f):
        out = []
        for p in range(slots):
            line = [gath[kind, p, f * tiles + t] for t in range(tiles)]
            below = gath[kind, p, 2 * tiles]
            above = gath[kind, p, 2 * tiles + 1]
            if f == 1:
                above = pltpu.roll(above, LANES - RIM, 1)
                below = pltpu.roll(below, RIM, 1)
            line.append(
                jnp.where(lane < RIM, above, jnp.where(lane >= LANES - RIM, below, 0.0))
            )
            out.append(line)
        return out

    def up(z, p, t):
        after = z[p + 1][t] if p + 1 < slots else zero
        return pltpu.roll(jnp.where(row < 1, after, z[p][t]), ROWS - 1, 0)

    def down(z, p, t):
        before = z[p - 1][t] if p > 0 else zero
        return pltpu.roll(jnp.where(row >= ROWS - 1, before, z[p][t]), 1, 0)

    def right(z, p, t):
        return pltpu.roll(jnp.where(lane < 1, z[p][(t + 1) % wide], z[p][t]), LANES - 1, 1)

    def left(z, p, t):
        return pltpu.roll(jnp.where(lane >= LANES - 1, z[p][(t - 1) % wide], z[p][t]), 1, 1)

    def grid(make):
        return [[make(p, t) for t in range(wide)] for p in range(slots)]

    def box(w):
        b = grid(lambda p, t: 4.0 * w[p][t] + (up(w, p, t) + down(w, p, t)))
        return grid(lambda p, t: 4.0 * b[p][t] + (right(b, p, t) + left(b, p, t)))

    x = window(0, 0)
    wet = window(0, 1)
    wet6 = grid(lambda p, t: wet[p][t] * (1.0 / 6.0))
    w = grid(lambda p, t: wet[p][t] * x[p][t])
    image = box(w)
    start = grid(lambda p, t: wet6[p][t] * image[p][t] - 6.0 * w[p][t])

    far_arrive()
    fe = window(1, 0)
    fn = window(1, 1)

    def right_side(p, t):
        div = (up(fe, p, t) - down(fe, p, t)) + (right(fn, p, t) - left(fn, p, t))
        return start[p][t] - wet[p][t] * ((0.5 * DIVERGENCE_COEF) * div)

    r = grid(right_side)
    d = grid(lambda p, t: r[p][t] * (1.0 / CHEB_CENTER))
    keeps, gains = cheb_table(ITERS)
    for index in range(ITERS):
        x = grid(lambda p, t: x[p][t] + d[p][t])
        if index < ITERS - 1:
            image = box(d)
            r = grid(
                lambda p, t: (r[p][t] - (SIGMA_SHIFT + 6.0) * d[p][t])
                + wet6[p][t] * image[p][t]
            )
            d = grid(lambda p, t: keeps[index] * d[p][t] + gains[index] * r[p][t])
    dry = dry_factor(ITERS)
    x = grid(lambda p, t: x[p][t] * (dry + (1.0 - dry) * wet[p][t]))

    for t in range(wide):
        xs[0, t] = zero
        xs[slots + 1, t] = zero
    for p in range(slots):
        for t in range(wide):
            xs[p + 1, t] = x[p][t]
    mine = [[xs[own + i, t] for t in range(wide)] for i in range(3)]
    for t in range(tiles):
        surface_out[:, lanes(t)] = mine[1][t]
        above = pltpu.roll(jnp.where(row < 1, mine[2][t], mine[1][t]), ROWS - 1, 0)
        below = pltpu.roll(jnp.where(row >= ROWS - 1, mine[0][t], mine[1][t]), 1, 0)
        slope_out[0, :, lanes(t)] = (above - below) * 0.5
        slope_out[1, :, lanes(t)] = (right(mine, 1, t) - left(mine, 1, t)) * 0.5

    for side, there in x_sides:
        @pl.when(there)
        def _(side=side):
            whole(send_x.at[side], side_sem.at[side]).wait()

    for side, there in y_sides:
        @pl.when(there)
        def _(side=side):
            whole(send_y, side_sem.at[2 + side]).wait()

    if relative:
        far(far_drain)
    else:
        if nx > 1:
            whole(block_count, far_send.at[1, 0]).wait()
        for side, there in ((-1, gy > 0), (1, gy < ny - 1)):
            @pl.when(there)
            def _(side=side):
                whole(rim_count, far_send.at[side + 1, 0]).wait()


def finish(
    state_ref, slope_ref, surface_ref, wet_ref, active_ref,
    east_out, north_out, salt_out, surface_out, held, sems,
):
    early = (
        pltpu.make_async_copy(surface_ref, surface_out, sems.at[1]),
    ) + tuple(
        pltpu.make_async_copy(
            state_ref.at[c, 2], salt_out.at[pl.ds(c * CHUNK, CHUNK)], sems.at[4 + c]
        )
        for c in range(state_ref.shape[0])
    )
    for copy in early:
        copy.start()
    levels = held.shape[1]
    active = active_ref[...] * wet_ref[...]
    slopes = (slope_ref[0], slope_ref[1])
    for f in range(2):
        for k in range(levels):
            held[f, k] = jnp.where(
                active > k, state_ref[k // CHUNK, f, k % CHUNK] - slopes[f], 0.0
            )
        pltpu.make_async_copy(held.at[f], (east_out, north_out)[f], sems.at[2 + f]).start()
    for f in range(2):
        pltpu.make_async_copy(held.at[f], (east_out, north_out)[f], sems.at[2 + f]).wait()
    for copy in early:
        copy.wait()


def solution(mesh):
    nx, ny = mesh.shape["gx"], mesh.shape["gy"]

    def local(east, north, salt, surface, depth, wet, active):
        levels, rows, width = east.shape
        assert rows == ROWS and width % LANES == 0 and levels % CHUNK == 0
        assert ITERS + 2 <= RIM and ITERS + 2 <= 3 * ROWS
        tiles = width // LANES
        chunks = levels // CHUNK
        n = 3 * CHUNK // 4 * tiles
        reach = min(nx - 1, -(-(ITERS + 2) // ROWS))
        slots = min(nx, 2 * reach + 1)
        f32 = jnp.float32
        vmem = pltpu.VMEM
        dma = pltpu.SemaphoreType.DMA
        block = pl.BlockSpec(memory_space=pltpu.VMEM)
        state = jax.ShapeDtypeStruct(east.shape, f32)
        hbm = pl.BlockSpec(memory_space=pltpu.HBM)
        tile = (rows, LANES)
        state3, slopes, surface_next = pl.pallas_call(
            functools.partial(kernel, nx, ny, reach, slots),
            out_shape=(
                jax.ShapeDtypeStruct((chunks, 3, CHUNK, rows, width), f32),
                jax.ShapeDtypeStruct((2,) + surface.shape, f32),
                jax.ShapeDtypeStruct(surface.shape, f32),
            ),
            in_specs=[hbm] * 7,
            out_specs=(block,) * 3,
            scratch_shapes=[
                vmem((3 * chunks, 3, CHUNK, rows, width), f32),
                vmem((3 * chunks, 3, CHUNK, rows, 2 * width), f32),
                vmem((3 * width, 2 * width), jnp.bfloat16),
                vmem((2,) + surface.shape, jnp.int32),
                vmem((2,) + surface.shape, f32),
                vmem((3, chunks, 2 * n + 2) + tile, f32),
                vmem((2, 3, chunks, n) + tile, f32),
                vmem((3, chunks, 1) + tile, f32),
                vmem((2 * tiles,) + tile, f32),
                vmem((1,) + tile, f32),
                vmem((1,) + tile, f32),
                vmem((2, slots, 2 * tiles + 2) + tile, f32),
                vmem((slots + 2, tiles + 1) + tile, f32),
                vmem((max(slots - 1, 1), 2 * tiles) + tile, f32),
                vmem((slots,) + tile, f32),
                vmem((slots * (2 * tiles + 2),) + tile, f32),
                vmem((2 * tiles,) + tile, f32),
                dma((2,)),
                dma((3, chunks)),
                dma((4,)),
                dma((3, slots if slots < nx else 1)),
                dma((1,)),
                dma((3,)),
                dma((2,)),
                dma((2, max(reach, 1))),
            ],
            compiler_params=pltpu.CompilerParams(
                collective_id=0, has_side_effects=True, vmem_limit_bytes=48 * 1024 * 1024
            ),
        )(*[
            pltpu.with_memory_space_constraint(z, pltpu.HBM)
            for z in (east, north, salt, surface, depth, wet, active)
        ])
        return pl.pallas_call(
            finish,
            out_shape=(state, state, state, jax.ShapeDtypeStruct(surface.shape, f32)),
            in_specs=[block] * 5,
            out_specs=(hbm,) * 4,
            scratch_shapes=[vmem((2,) + east.shape, f32), dma((4 + chunks,))],
            compiler_params=pltpu.CompilerParams(vmem_limit_bytes=8 * 1024 * 1024),
        )(state3, slopes, surface_next, wet, active)

    return jax.shard_map(
        local,
        mesh=mesh,
        in_specs=(
            P(None, "gx", "gy"),
            P(None, "gx", "gy"),
            P(None, "gx", "gy"),
            P("gx", "gy"),
            P("gx", "gy"),
            P("gx", "gy"),
            P("gx", "gy"),
        ),
        out_specs=(P(None, "gx", "gy"), P(None, "gx", "gy"), P(None, "gx", "gy"), P("gx", "gy")),
        check_vma=False,
    )
```

```python
import functools

import jax
import jax.numpy as jnp
from jax import lax
from jax.experimental import pallas as pl
from jax.experimental.pallas import tpu as pltpu
from jax.sharding import PartitionSpec as P

ITERS = 16

TIME_STEP = 0.2
CORIOLIS = 0.3
PRESS_COEF = 0.05
VISCOSITY = 0.1
DIFFUSIVITY = 0.1
SIGMA_SHIFT = 0.25
CHEB_CENTER = 3.625
CHEB_HALF = 3.375
DIVERGENCE_COEF = 8.0

ROWS = 8
LANES = 128
CHUNK = 8
RIM = LANES // 4
MESH = pl.DeviceIdType.MESH


def cheb_table(count):
    first = CHEB_CENTER / CHEB_HALF
    ratio = 1.0 / first
    keeps = []
    gains = []
    for index in range(count):
        ratio_next = 1.0 / (2.0 * first - ratio)
        keeps.append(ratio_next * ratio)
        gains.append(2.0 * ratio_next / CHEB_HALF)
        ratio = ratio_next
    return (keeps, gains)


def dry_factor(count):
    keeps, gains = cheb_table(count)
    x, r = 1.0, -1.0
    d = r / CHEB_CENTER
    for index in range(count):
        x = x + d
        r = r - d
        d = keeps[index] * d + gains[index] * r
    return x


def kernel(
    nx, ny, reach, slots,
    east_hbm, north_hbm, salt_hbm, surface_hbm, depth_hbm, wet_hbm, active_hbm,
    state_out, slope_out, surface_out,
    held, moved, shifts, ints, floats, halo, send_x, send_y, far_c, far_e, stat_e, gath, xs,
    block_count, rim_count, arrivals, blank, small_sem, halo_sem, side_sem, far_send, far_recv,
    rim_sem, relay_send, relay_recv,
):
    gx = lax.axis_index("gx")
    gy = lax.axis_index("gy")
    width = held.shape[4]
    tiles = width // LANES
    chunks = held.shape[0] // 3
    levels = chunks * CHUNK
    groups = 3 * CHUNK // 4
    n = groups * tiles
    relative = slots < nx
    row = lax.broadcasted_iota(jnp.int32, (ROWS, LANES), 0)
    lane = lax.broadcasted_iota(jnp.int32, (ROWS, LANES), 1)
    pair = row // 2
    zero = jnp.zeros((ROWS, LANES), jnp.float32)

    def lanes(t):
        return slice(t * LANES, (t + 1) * LANES)

    def inside(x, y):
        return jnp.logical_and(
            jnp.logical_and(x >= 0, x < nx), jnp.logical_and(y >= 0, y < ny)
        )

    def whole(ref, sem):
        return pltpu.make_async_copy(ref, ref, sem)

    def load(c):
        part = pl.ds(c * CHUNK, CHUNK)
        for f, source in enumerate((east_hbm, north_hbm, salt_hbm)):
            pltpu.make_async_copy(source.at[part], held.at[c, f], halo_sem.at[1, c]).start()

    own = reach if relative else gx
    partners = [
        (o, side)
        for o in range(-reach, reach + 1)
        for side in (-1, 0, 1)
        if (o, side) != (0, 0)
    ]
    partners.sort(key=lambda p: (-abs(p[1]), -abs(p[0])))

    def far(action):
        for o, side in partners:
            @pl.when(inside(gx + o, gy + side))
            def _(o=o, side=side):
                action(o, side)

    def counts(size):
        return (0,) if size == 1 else (1,) if size == 2 else (1, 2)

    has_x = (gx > 0).astype(jnp.int32) + (gx < nx - 1).astype(jnp.int32)
    has_y = (gy > 0).astype(jnp.int32) + (gy < ny - 1).astype(jnp.int32)

    def arrive(stage, c):
        for a in counts(nx):
            for b in counts(ny):
                @pl.when(jnp.logical_and(has_x == a, has_y == b))
                def _(a=a, b=b):
                    part = halo.at[stage, c, pl.ds(0, a * n + b)]
                    whole(part, halo_sem.at[stage % 2, c]).wait()

    def far_arrive():
        for b in counts(ny):
            @pl.when(has_y == b)
            def _(b=b):
                whole(arrivals.at[pl.ds(0, slots * (2 * tiles + b))], far_recv.at[0]).wait()

    barrier = pltpu.get_barrier_semaphore()
    count = jnp.int32(0)
    for o, side in ((-1, 0), (1, 0), (0, -1), (0, 1)):
        there = inside(gx + o, gy + side)

        @pl.when(there)
        def _(o=o, side=side):
            pl.semaphore_signal(
                barrier, inc=1, device_id=(gx + o, gy + side), device_id_type=MESH
            )

        count = count + there.astype(jnp.int32)

    pltpu.make_async_copy(active_hbm, ints.at[0], small_sem.at[0]).start()
    pltpu.make_async_copy(wet_hbm, ints.at[1], small_sem.at[0]).start()
    load(0)

    source = lax.broadcasted_iota(jnp.int32, (width, width), 0)
    target = lax.broadcasted_iota(jnp.int32, (width, width), 1)
    step = source - target
    one = jnp.abs(step) == 1
    sign = jnp.where(step > 0, 1.0, -1.0)
    slope = jnp.where(one, 8.0 * sign, jnp.where(jnp.abs(step) == 2, -sign, 0.0))
    for i in range(3):
        part = slice(i * width, (i + 1) * width)
        shifts[part, :width] = slope.astype(jnp.bfloat16)
        shifts[part, width:] = jnp.where(one, 1.0, 0.0).astype(jnp.bfloat16)

    def move(index):
        value = held[index].reshape(3 * CHUNK * ROWS, width)
        high = value.astype(jnp.bfloat16)
        rest = value - high.astype(jnp.float32)
        middle = rest.astype(jnp.bfloat16)
        low = (rest - middle.astype(jnp.float32)).astype(jnp.bfloat16)
        total = jnp.dot(
            jnp.concatenate([low, middle, high], axis=1),
            shifts[...],
            preferred_element_type=jnp.float32,
        )
        moved[index] = total.reshape(3, CHUNK, ROWS, 2 * width)

    def pack(stage, c, half):
        for f in range(3):
            ups = [None] * tiles
            downs = [None] * tiles
            for m in range(4):
                for t in range(tiles):
                    part = held[stage * chunks + c, f, half * 4 + m, :, lanes(t)]
                    turned = part if m == 3 else pltpu.roll(part, 2 * m + 2, 0)
                    if m == 0:
                        ups[t] = turned
                        downs[t] = turned
                    else:
                        ups[t] = jnp.where(pair == m, turned, ups[t])
                        downs[t] = jnp.where(pair == (m + 1) % 4, turned, downs[t])
            for t in range(tiles):
                at = (half * 3 + f) * tiles + t
                send_x[0, stage, c, at] = downs[t]
                send_x[1, stage, c, at] = ups[t]

    def pack_rim(stage, c):
        rim = zero
        for f in range(3):
            for kk in range(CHUNK):
                position = f * CHUNK + kk
                first, last = (
                    held[stage * chunks + c, f, kk, :, lanes(t)] for t in (0, tiles - 1)
                )
                rim = jnp.where(
                    lane // 4 == position,
                    pltpu.roll(
                        jnp.where(lane < LANES // 2, first, last),
                        (4 * position + 2) % LANES, 1,
                    ),
                    rim,
                )
        send_y[stage, c, 0] = rim

    def x_copy(stage, c, side):
        return pltpu.make_async_remote_copy(
            src_ref=send_x.at[side, stage, c],
            dst_ref=halo.at[stage, c, pl.ds((1 - side) * n, n)],
            send_sem=side_sem.at[side],
            recv_sem=halo_sem.at[stage % 2, c],
            device_id=(gx + 2 * side - 1, gy),
            device_id_type=MESH,
        )

    def y_copy(stage, c, side):
        return pltpu.make_async_remote_copy(
            src_ref=send_y.at[stage, c],
            dst_ref=halo.at[stage, c, pl.ds(2 * n + 1 - side, 1)],
            send_sem=side_sem.at[2 + side],
            recv_sem=halo_sem.at[stage % 2, c],
            device_id=(gx, gy + 2 * side - 1),
            device_id_type=MESH,
        )

    x_sides = ((0, gx > 0), (1, gx < nx - 1))
    y_sides = ((0, gy > 0), (1, gy < ny - 1))

    def launch(stage, c):
        for half in range(CHUNK // 4):
            pack(stage, c, half)
        pack_rim(stage, c)
        for side, there in y_sides:
            @pl.when(there)
            def _(side=side):
                y_copy(stage, c, side).start()
        for side, there in x_sides:
            @pl.when(there)
            def _(side=side):
                x_copy(stage, c, side).start()

    def far_start():
        def action(o, side):
            slot = reach - o if relative else gx
            if side == 0:
                source, target = far_c, gath.at[1, slot, pl.ds(0, 2 * tiles)]
            else:
                at = 2 * tiles + (1 - side) // 2
                source, target = far_e, gath.at[1, slot, pl.ds(at, 1)]
            pltpu.make_async_remote_copy(
                src_ref=source, dst_ref=target,
                send_sem=far_send.at[side + 1, o + reach if relative else 0],
                recv_sem=far_recv.at[0],
                device_id=(gx + o, gy + side), device_id_type=MESH,
            ).start()

        far(action)
        pltpu.make_async_copy(
            far_c, gath.at[1, own, pl.ds(0, 2 * tiles)], far_recv.at[0]
        ).start()

    def far_drain(o, side):
        whole(far_c if side == 0 else far_e, far_send.at[side + 1, o + reach]).wait()

    def rim_start():
        for side, there in y_sides:
            @pl.when(there)
            def _(side=side):
                pltpu.make_async_remote_copy(
                    src_ref=stat_e,
                    dst_ref=gath.at[0, own, pl.ds(2 * tiles + 1 - side, 1)],
                    send_sem=rim_sem.at[side], recv_sem=rim_sem.at[2],
                    device_id=(gx, gy + 2 * side - 1), device_id_type=MESH,
                ).start()

    def rim_arrive():
        for b in counts(ny):
            @pl.when(has_y == b)
            def _(b=b):
                whole(arrivals.at[pl.ds(0, b)], rim_sem.at[2]).wait()
        for side, there in y_sides:
            @pl.when(there)
            def _(side=side):
                whole(stat_e, rim_sem.at[side]).wait()

    def relay_steps(action, step):
        for side, there in x_sides:
            sign = 2 * side - 1
            passed = gx - sign * (step - 1)
            sends = jnp.logical_and(there, jnp.logical_and(passed >= 0, passed < nx))
            comes = jnp.logical_and(gx - sign * step >= 0, gx - sign * step < nx)
            action(side, sign, sends, comes)

    def relay(step):
        def action(side, sign, sends, comes):
            @pl.when(sends)
            def _():
                source = own - sign * (step - 1)
                target = own - sign * step if relative else source
                pltpu.make_async_remote_copy(
                    src_ref=gath.at[0, source], dst_ref=gath.at[0, target],
                    send_sem=relay_send.at[side], recv_sem=relay_recv.at[side, step - 1],
                    device_id=(gx + sign, gy), device_id_type=MESH,
                ).start()

        relay_steps(action, step)

    def relay_arrive(step):
        def action(side, sign, sends, comes):
            @pl.when(comes)
            def _():
                whole(
                    gath.at[0, own - sign * step], relay_recv.at[side, step - 1]
                ).wait()

            @pl.when(sends)
            def _():
                whole(gath.at[0, own - sign * (step - 1)], relay_send.at[side]).wait()

        relay_steps(action, step)

    def fill_far(data):
        low, high = data
        first = jnp.where(lane < RIM, low[0], pltpu.roll(high[0], RIM, 1))
        second = jnp.where(
            lane < LANES - RIM, pltpu.roll(high[-1], LANES - RIM, 1), low[-1]
        )
        return jnp.where(lane < 2 * RIM, first, second)

    def put(target, data):
        for f in range(2):
            for t in range(tiles):
                target[f * tiles + t] = data[f][t]

    for side, missing in ((0, gx == 0), (1, gx == nx - 1)):
        @pl.when(missing)
        def _(side=side):
            for stage in range(3):
                @pl.loop(0, chunks)
                def _(c, stage=stage):
                    halo[stage, c, side * n:(side + 1) * n] = jnp.zeros(
                        (n, ROWS, LANES), jnp.float32
                    )

    for side, missing in ((0, gy == 0), (1, gy == ny - 1)):
        @pl.when(missing)
        def _(side=side):
            halo[:, :, 2 * n + side] = jnp.zeros((3, chunks, ROWS, LANES), jnp.float32)
            gath[:, :, 2 * tiles + side] = jnp.zeros((2, slots, ROWS, LANES), jnp.float32)

    if relative:
        blank[...] = jnp.zeros((2 * tiles, ROWS, LANES), jnp.float32)

    whole(ints, small_sem.at[0]).wait()
    active = [ints[0, :, lanes(t)] * ints[1, :, lanes(t)] for t in range(tiles)]

    def first(c):
        whole(held.at[c], halo_sem.at[1, c]).wait()
        for kk in range(CHUNK):
            for t in range(tiles):
                live = active[t] > c * CHUNK + kk
                for f in range(3):
                    held[c, f, kk, :, lanes(t)] = jnp.where(
                        live, held[c, f, kk, :, lanes(t)], 0.0
                    )

    first(0)
    for c in range(1, chunks):
        load(c)
    pltpu.make_async_copy(surface_hbm, floats.at[0], small_sem.at[1]).start()
    pltpu.make_async_copy(depth_hbm, floats.at[1], small_sem.at[1]).start()
    pl.semaphore_wait(barrier, count)
    launch(0, 0)

    @pl.loop(1, chunks)
    def _(c):
        first(c)
        launch(0, c)

    if relative:
        for j in range(slots):
            @pl.when(jnp.logical_not(inside(gx + j - reach, gy)))
            def _(j=j):
                gath[0, j] = jnp.zeros((2 * tiles + 2, ROWS, LANES), jnp.float32)
                pltpu.make_async_copy(
                    blank, gath.at[1, j, pl.ds(0, 2 * tiles)], far_recv.at[0]
                ).start()
                for side, there in y_sides:
                    @pl.when(there)
                    def _(side=side):
                        pltpu.make_async_copy(
                            blank.at[pl.ds(0, 1)],
                            gath.at[1, j, pl.ds(2 * tiles + side, 1)],
                            far_recv.at[0],
                        ).start()

    whole(floats, small_sem.at[1]).wait()
    stats = (
        [floats[0, :, lanes(t)] for t in range(tiles)],
        [ints[1, :, lanes(t)].astype(jnp.float32) for t in range(tiles)],
    )
    put(gath.at[0, own], stats)
    stat_e[0] = fill_far(stats)
    rim_start()

    @pl.loop(0, chunks - 1)
    def _(c):
        move(c)

    quarter = lane % 4

    def run_stage(stage, weight0, weight1):
        gain = weight1 * TIME_STEP
        keep_flow = weight1 - 4.0 * gain * VISCOSITY
        keep_salt = weight1 - 4.0 * gain * DIFFUSIVITY
        drift = -gain / 12.0
        push = drift * PRESS_COEF

        def body(c, carry, behind=stage < 2):
            press_e, press_n = list(carry[0]), list(carry[1])
            sums = [list(x) for x in carry[2:]]
            index = stage * chunks + c
            arrive(stage, c)
            if behind:
                move(index + chunks - 1)
            rims = jnp.where(quarter < 2, halo[stage, c, 2 * n], halo[stage, c, 2 * n + 1])
            r1, r2 = pltpu.roll(rims, LANES - 1, 1), pltpu.roll(rims, LANES - 2, 1)
            l1, l2 = pltpu.roll(rims, 1, 1), pltpu.roll(rims, 2, 1)
            rim_slope = jnp.where(
                quarter < 2,
                jnp.where(quarter == 0, -r2, 8.0 * r1 - r2),
                jnp.where(quarter == 2, l2 - 8.0 * l1, l2),
            )
            rim_sum = jnp.where(quarter == 1, r1, jnp.where(quarter == 2, l1, 0.0))
            for kk in range(CHUNK):
                fields = []
                for f in range(3):
                    position = f * CHUNK + kk
                    group, m = (kk // 4) * 3 + f, kk % 4
                    back = (-(4 * position + 2)) % LANES
                    extra_slope = pltpu.roll(rim_slope, back, 1)
                    extra_sum = pltpu.roll(rim_sum, back, 1)
                    per_tile = []
                    for t in range(tiles):
                        q = held[index, f, kk, :, lanes(t)]
                        ends = jnp.where(
                            pair == m,
                            halo[stage, c, group * tiles + t],
                            halo[stage, c, n + group * tiles + t],
                        )
                        if m != 3:
                            ends = pltpu.roll(ends, (-(2 * m + 2)) % ROWS, 0)
                        e1 = pltpu.roll(jnp.where(row < 1, ends, q), ROWS - 1, 0)
                        e2 = pltpu.roll(jnp.where(row < 2, ends, q), ROWS - 2, 0)
                        w1 = pltpu.roll(jnp.where(row >= ROWS - 1, ends, q), 1, 0)
                        w2 = pltpu.roll(jnp.where(row >= ROWS - 2, ends, q), 2, 0)
                        dy = moved[index, f, kk, :, lanes(t)]
                        sides = moved[index, f, kk, :, lanes(tiles + t)]
                        if t == 0:
                            dy = dy + jnp.where(lane < 2, extra_slope, 0.0)
                            sides = sides + jnp.where(lane < 1, extra_sum, 0.0)
                        if t == tiles - 1:
                            dy = dy + jnp.where(lane >= LANES - 2, extra_slope, 0.0)
                            sides = sides + jnp.where(lane >= LANES - 1, extra_sum, 0.0)
                        dx = 8.0 * (e1 - w1) - (e2 - w2)
                        per_tile.append((q, dx, dy, (e1 + w1) + sides))
                    fields.append(per_tile)
                for t in range(tiles):
                    live = active[t] > c * CHUNK + kk
                    (u, ux, uy, ul), (v, vx, vy, vl), (s, sx, sy, sl) = [
                        fields[f][t] for f in range(3)
                    ]
                    press_e[t] = press_e[t] + sx
                    press_n[t] = press_n[t] + sy
                    um = u * drift
                    vm = v * drift
                    news = [
                        (um * ux + vm * uy) + push * press_e[t] + (gain * CORIOLIS) * v
                        + (gain * VISCOSITY) * ul + keep_flow * u,
                        (um * vx + vm * vy) + push * press_n[t] - (gain * CORIOLIS) * u
                        + (gain * VISCOSITY) * vl + keep_flow * v,
                        (um * sx + vm * sy) + (gain * DIFFUSIVITY) * sl + keep_salt * s,
                    ]
                    for f in range(3):
                        new = news[f]
                        if weight0 is not None:
                            new = new + weight0 * held[c, f, kk, :, lanes(t)]
                        new = jnp.where(live, new, 0.0)
                        if stage < 2:
                            held[index + chunks, f, kk, :, lanes(t)] = new
                        else:
                            state_out[c, f, kk, :, lanes(t)] = new
                            if f < 2:
                                sums[f][t] = sums[f][t] + new
            if stage < 2:
                launch(stage + 1, c)
            return (tuple(press_e), tuple(press_n)) + tuple(tuple(x) for x in sums)

        start = ((zero,) * tiles,) * (4 if stage == 2 else 2)
        if stage < 2:
            return lax.fori_loop(0, chunks, body, start)
        return lax.fori_loop(1, chunks, body, body(0, start, True))

    def pass_on(step):
        if step == 1:
            rim_arrive()
        elif step - 1 <= reach:
            relay_arrive(step - 1)
        if step <= reach:
            relay(step)

    run_stage(0, None, 1.0)
    pass_on(1)
    run_stage(1, 0.75, 0.25)
    pass_on(2)
    carry = run_stage(2, 1.0 / 3.0, 2.0 / 3.0)

    flows = [
        [floats[1, :, lanes(t)] * (carry[2 + f][t] / levels) for t in range(tiles)]
        for f in range(2)
    ]
    put(far_c, flows)
    far_e[0] = fill_far(flows[::-1])
    far_start()
    pass_on(3)
    pass_on(4)

    wide = tiles + 1

    def window(kind, f):
        out = []
        for p in range(slots):
            line = [gath[kind, p, f * tiles + t] for t in range(tiles)]
            below = gath[kind, p, 2 * tiles]
            above = gath[kind, p, 2 * tiles + 1]
            if f != kind:
                above = pltpu.roll(above, LANES - RIM, 1)
                below = pltpu.roll(below, RIM, 1)
            line.append(
                jnp.where(lane < RIM, above, jnp.where(lane >= LANES - RIM, below, 0.0))
            )
            out.append(line)
        return out

    def up(z, p, t):
        after = z[p + 1][t] if p + 1 < slots else zero
        return pltpu.roll(jnp.where(row < 1, after, z[p][t]), ROWS - 1, 0)

    def down(z, p, t):
        before = z[p - 1][t] if p > 0 else zero
        return pltpu.roll(jnp.where(row >= ROWS - 1, before, z[p][t]), 1, 0)

    def right(z, p, t):
        return pltpu.roll(jnp.where(lane < 1, z[p][(t + 1) % wide], z[p][t]), LANES - 1, 1)

    def left(z, p, t):
        return pltpu.roll(jnp.where(lane >= LANES - 1, z[p][(t - 1) % wide], z[p][t]), 1, 1)

    def grid(make):
        return [[make(p, t) for t in range(wide)] for p in range(slots)]

    def box(w):
        b = grid(lambda p, t: 4.0 * w[p][t] + (up(w, p, t) + down(w, p, t)))
        return grid(lambda p, t: 4.0 * b[p][t] + (right(b, p, t) + left(b, p, t)))

    x = window(0, 0)
    wet = window(0, 1)
    wet6 = grid(lambda p, t: wet[p][t] * (1.0 / 6.0))
    w = grid(lambda p, t: wet[p][t] * x[p][t])
    image = box(w)
    start = grid(lambda p, t: wet6[p][t] * image[p][t] - 6.0 * w[p][t])

    far_arrive()
    fe = window(1, 0)
    fn = window(1, 1)

    def right_side(p, t):
        div = (up(fe, p, t) - down(fe, p, t)) + (right(fn, p, t) - left(fn, p, t))
        return start[p][t] - wet[p][t] * ((0.5 * DIVERGENCE_COEF) * div)

    r = grid(right_side)
    d = grid(lambda p, t: r[p][t] * (1.0 / CHEB_CENTER))
    keeps, gains = cheb_table(ITERS)
    for index in range(ITERS):
        x = grid(lambda p, t: x[p][t] + d[p][t])
        if index < ITERS - 1:
            image = box(d)
            r = grid(
                lambda p, t: (r[p][t] - (SIGMA_SHIFT + 6.0) * d[p][t])
                + wet6[p][t] * image[p][t]
            )
            d = grid(lambda p, t: keeps[index] * d[p][t] + gains[index] * r[p][t])
    dry = dry_factor(ITERS)
    x = grid(lambda p, t: x[p][t] * (dry + (1.0 - dry) * wet[p][t]))

    for t in range(wide):
        xs[0, t] = zero
        xs[slots + 1, t] = zero
    for p in range(slots):
        for t in range(wide):
            xs[p + 1, t] = x[p][t]
    mine = [[xs[own + i, t] for t in range(wide)] for i in range(3)]
    for t in range(tiles):
        surface_out[:, lanes(t)] = mine[1][t]
        above = pltpu.roll(jnp.where(row < 1, mine[2][t], mine[1][t]), ROWS - 1, 0)
        below = pltpu.roll(jnp.where(row >= ROWS - 1, mine[0][t], mine[1][t]), 1, 0)
        slope_out[0, :, lanes(t)] = (above - below) * 0.5
        slope_out[1, :, lanes(t)] = (right(mine, 1, t) - left(mine, 1, t)) * 0.5

    for side, there in x_sides:
        @pl.when(there)
        def _(side=side):
            whole(send_x.at[side], side_sem.at[side]).wait()

    for side, there in y_sides:
        @pl.when(there)
        def _(side=side):
            whole(send_y, side_sem.at[2 + side]).wait()

    if relative:
        far(far_drain)
    else:
        if nx > 1:
            whole(block_count, far_send.at[1, 0]).wait()
        for side, there in ((-1, gy > 0), (1, gy < ny - 1)):
            @pl.when(there)
            def _(side=side):
                whole(rim_count, far_send.at[side + 1, 0]).wait()


def finish(
    state_ref, slope_ref, surface_ref, wet_ref, active_ref,
    east_out, north_out, salt_out, surface_out, held, sems,
):
    early = (
        pltpu.make_async_copy(surface_ref, surface_out, sems.at[1]),
    ) + tuple(
        pltpu.make_async_copy(
            state_ref.at[c, 2], salt_out.at[pl.ds(c * CHUNK, CHUNK)], sems.at[4 + c]
        )
        for c in range(state_ref.shape[0])
    )
    for copy in early:
        copy.start()
    levels = held.shape[1]
    active = active_ref[...] * wet_ref[...]
    slopes = (slope_ref[0], slope_ref[1])
    for f in range(2):
        for k in range(levels):
            held[f, k] = jnp.where(
                active > k, state_ref[k // CHUNK, f, k % CHUNK] - slopes[f], 0.0
            )
        pltpu.make_async_copy(held.at[f], (east_out, north_out)[f], sems.at[2 + f]).start()
    for f in range(2):
        pltpu.make_async_copy(held.at[f], (east_out, north_out)[f], sems.at[2 + f]).wait()
    for copy in early:
        copy.wait()


def solution(mesh):
    nx, ny = mesh.shape["gx"], mesh.shape["gy"]

    def local(east, north, salt, surface, depth, wet, active):
        levels, rows, width = east.shape
        assert rows == ROWS and width % LANES == 0 and levels % CHUNK == 0
        assert ITERS + 2 <= RIM and ITERS + 2 <= 3 * ROWS
        tiles = width // LANES
        chunks = levels // CHUNK
        n = 3 * CHUNK // 4 * tiles
        reach = min(nx - 1, -(-(ITERS + 2) // ROWS))
        slots = min(nx, 2 * reach + 1)
        f32 = jnp.float32
        vmem = pltpu.VMEM
        dma = pltpu.SemaphoreType.DMA
        block = pl.BlockSpec(memory_space=pltpu.VMEM)
        state = jax.ShapeDtypeStruct(east.shape, f32)
        hbm = pl.BlockSpec(memory_space=pltpu.HBM)
        tile = (rows, LANES)
        state3, slopes, surface_next = pl.pallas_call(
            functools.partial(kernel, nx, ny, reach, slots),
            out_shape=(
                jax.ShapeDtypeStruct((chunks, 3, CHUNK, rows, width), f32),
                jax.ShapeDtypeStruct((2,) + surface.shape, f32),
                jax.ShapeDtypeStruct(surface.shape, f32),
            ),
            in_specs=[hbm] * 7,
            out_specs=(block,) * 3,
            scratch_shapes=[
                vmem((3 * chunks, 3, CHUNK, rows, width), f32),
                vmem((3 * chunks, 3, CHUNK, rows, 2 * width), f32),
                vmem((3 * width, 2 * width), jnp.bfloat16),
                vmem((2,) + surface.shape, jnp.int32),
                vmem((2,) + surface.shape, f32),
                vmem((3, chunks, 2 * n + 2) + tile, f32),
                vmem((2, 3, chunks, n) + tile, f32),
                vmem((3, chunks, 1) + tile, f32),
                vmem((2 * tiles,) + tile, f32),
                vmem((1,) + tile, f32),
                vmem((1,) + tile, f32),
                vmem((2, slots, 2 * tiles + 2) + tile, f32),
                vmem((slots + 2, tiles + 1) + tile, f32),
                vmem((max(slots - 1, 1), 2 * tiles) + tile, f32),
                vmem((slots,) + tile, f32),
                vmem((slots * (2 * tiles + 2),) + tile, f32),
                vmem((2 * tiles,) + tile, f32),
                dma((2,)),
                dma((2, chunks)),
                dma((4,)),
                dma((3, slots if slots < nx else 1)),
                dma((1,)),
                dma((3,)),
                dma((2,)),
                dma((2, max(reach, 1))),
            ],
            compiler_params=pltpu.CompilerParams(
                collective_id=0, has_side_effects=True, vmem_limit_bytes=48 * 1024 * 1024
            ),
        )(*[
            pltpu.with_memory_space_constraint(z, pltpu.HBM)
            for z in (east, north, salt, surface, depth, wet, active)
        ])
        return pl.pallas_call(
            finish,
            out_shape=(state, state, state, jax.ShapeDtypeStruct(surface.shape, f32)),
            in_specs=[block] * 5,
            out_specs=(hbm,) * 4,
            scratch_shapes=[vmem((2,) + east.shape, f32), dma((4 + chunks,))],
            compiler_params=pltpu.CompilerParams(vmem_limit_bytes=8 * 1024 * 1024),
        )(state3, slopes, surface_next, wet, active)

    return jax.shard_map(
        local,
        mesh=mesh,
        in_specs=(
            P(None, "gx", "gy"),
            P(None, "gx", "gy"),
            P(None, "gx", "gy"),
            P("gx", "gy"),
            P("gx", "gy"),
            P("gx", "gy"),
            P("gx", "gy"),
        ),
        out_specs=(P(None, "gx", "gy"), P(None, "gx", "gy"), P(None, "gx", "gy"), P("gx", "gy")),
        check_vma=False,
    )
```

```python
import functools

import jax
import jax.numpy as jnp
from jax import lax
from jax.experimental import pallas as pl
from jax.experimental.pallas import tpu as pltpu
from jax.sharding import PartitionSpec as P

ITERS = 16

TIME_STEP = 0.2
CORIOLIS = 0.3
PRESS_COEF = 0.05
VISCOSITY = 0.1
DIFFUSIVITY = 0.1
SIGMA_SHIFT = 0.25
CHEB_CENTER = 3.625
CHEB_HALF = 3.375
DIVERGENCE_COEF = 8.0

ROWS = 8
LANES = 128
CHUNK = 8
RIM = LANES // 4
MESH = pl.DeviceIdType.MESH


def cheb_table(count):
    first = CHEB_CENTER / CHEB_HALF
    ratio = 1.0 / first
    keeps = []
    gains = []
    for index in range(count):
        ratio_next = 1.0 / (2.0 * first - ratio)
        keeps.append(ratio_next * ratio)
        gains.append(2.0 * ratio_next / CHEB_HALF)
        ratio = ratio_next
    return (keeps, gains)


def dry_factor(count):
    keeps, gains = cheb_table(count)
    x, r = 1.0, -1.0
    d = r / CHEB_CENTER
    for index in range(count):
        x = x + d
        r = r - d
        d = keeps[index] * d + gains[index] * r
    return x


def kernel(
    nx, ny, reach, slots,
    east_hbm, north_hbm, salt_hbm, surface_hbm, depth_hbm, wet_hbm, active_hbm,
    state_out, slope_out, surface_out,
    held, moved, shifts, ints, floats, halo, send_x, send_y, far_c, far_e, stat_e, gath, xs,
    block_count, rim_count, y_count, arrivals, blank, halo_sem, side_sem, far_send, far_recv,
    rim_sem, relay_send, relay_recv,
):
    gx = lax.axis_index("gx")
    gy = lax.axis_index("gy")
    width = held.shape[4]
    tiles = width // LANES
    chunks = held.shape[0] // 3
    levels = chunks * CHUNK
    groups = 3 * CHUNK // 4
    n = groups * tiles
    relative = slots < nx
    row = lax.broadcasted_iota(jnp.int32, (ROWS, LANES), 0)
    lane = lax.broadcasted_iota(jnp.int32, (ROWS, LANES), 1)
    pair = row // 2
    zero = jnp.zeros((ROWS, LANES), jnp.float32)

    def lanes(t):
        return slice(t * LANES, (t + 1) * LANES)

    def inside(x, y):
        return jnp.logical_and(
            jnp.logical_and(x >= 0, x < nx), jnp.logical_and(y >= 0, y < ny)
        )

    def whole(ref, sem):
        return pltpu.make_async_copy(ref, ref, sem)

    def load(c):
        part = pl.ds(c * CHUNK, CHUNK)
        for f, source in enumerate((east_hbm, north_hbm, salt_hbm)):
            pltpu.make_async_copy(source.at[part], held.at[c, f], halo_sem.at[1, c]).start()

    own = reach if relative else gx
    partners = [
        (o, side)
        for o in range(-reach, reach + 1)
        for side in (-1, 0, 1)
        if (o, side) != (0, 0)
    ]
    partners.sort(key=lambda p: (-abs(p[1]), p[0] != 0, -abs(p[0])))

    def far(action):
        for o, side in partners:
            @pl.when(inside(gx + o, gy + side))
            def _(o=o, side=side):
                action(o, side)

    def counts(size):
        return (0,) if size == 1 else (1,) if size == 2 else (1, 2)

    has_x = (gx > 0).astype(jnp.int32) + (gx < nx - 1).astype(jnp.int32)
    has_y = (gy > 0).astype(jnp.int32) + (gy < ny - 1).astype(jnp.int32)

    def arrive(stage, c):
        for a in counts(nx):
            for b in counts(ny):
                @pl.when(jnp.logical_and(has_x == a, has_y == b))
                def _(a=a, b=b):
                    part = halo.at[stage, c, pl.ds(0, a * n + b)]
                    whole(part, halo_sem.at[stage % 2, c]).wait()

    def far_arrive():
        for b in counts(ny):
            @pl.when(has_y == b)
            def _(b=b):
                whole(arrivals.at[pl.ds(0, slots * (2 * tiles + b))], far_recv.at[0]).wait()

    barrier = pltpu.get_barrier_semaphore()
    count = jnp.int32(0)
    for o, side in ((-1, 0), (1, 0), (0, -1), (0, 1)):
        there = inside(gx + o, gy + side)

        @pl.when(there)
        def _(o=o, side=side):
            pl.semaphore_signal(
                barrier, inc=1, device_id=(gx + o, gy + side), device_id_type=MESH
            )

        count = count + there.astype(jnp.int32)

    pltpu.make_async_copy(active_hbm, ints.at[0], relay_recv.at[0, 0]).start()
    pltpu.make_async_copy(wet_hbm, ints.at[1], relay_recv.at[0, 0]).start()
    load(0)

    source = lax.broadcasted_iota(jnp.int32, (width, width), 0)
    target = lax.broadcasted_iota(jnp.int32, (width, width), 1)
    step = source - target
    one = jnp.abs(step) == 1
    sign = jnp.where(step > 0, 1.0, -1.0)
    slope = jnp.where(one, 8.0 * sign, jnp.where(jnp.abs(step) == 2, -sign, 0.0))
    for i in range(3):
        part = slice(i * width, (i + 1) * width)
        shifts[part, :width] = slope.astype(jnp.bfloat16)
        shifts[part, width:] = jnp.where(one, 1.0, 0.0).astype(jnp.bfloat16)

    def move(index):
        value = held[index].reshape(3 * CHUNK * ROWS, width)
        high = value.astype(jnp.bfloat16)
        rest = value - high.astype(jnp.float32)
        middle = rest.astype(jnp.bfloat16)
        low = (rest - middle.astype(jnp.float32)).astype(jnp.bfloat16)
        total = jnp.dot(
            jnp.concatenate([low, middle, high], axis=1),
            shifts[...],
            preferred_element_type=jnp.float32,
        )
        moved[index] = total.reshape(3, CHUNK, ROWS, 2 * width)

    def pack(stage, c, half):
        for f in range(3):
            ups = [None] * tiles
            downs = [None] * tiles
            for m in range(4):
                for t in range(tiles):
                    part = held[stage * chunks + c, f, half * 4 + m, :, lanes(t)]
                    turned = part if m == 3 else pltpu.roll(part, 2 * m + 2, 0)
                    if m == 0:
                        ups[t] = turned
                        downs[t] = turned
                    else:
                        ups[t] = jnp.where(pair == m, turned, ups[t])
                        downs[t] = jnp.where(pair == (m + 1) % 4, turned, downs[t])
            for t in range(tiles):
                at = (half * 3 + f) * tiles + t
                send_x[0, stage, c, at] = downs[t]
                send_x[1, stage, c, at] = ups[t]

    def pack_rim(stage, c):
        rim = zero
        for f in range(3):
            for kk in range(CHUNK):
                position = f * CHUNK + kk
                first, last = (
                    held[stage * chunks + c, f, kk, :, lanes(t)] for t in (0, tiles - 1)
                )
                rim = jnp.where(
                    lane // 4 == position,
                    pltpu.roll(
                        jnp.where(lane < LANES // 2, first, last),
                        (4 * position + 2) % LANES, 1,
                    ),
                    rim,
                )
        return rim

    def x_copy(stage, c, side):
        return pltpu.make_async_remote_copy(
            src_ref=send_x.at[side, stage, c],
            dst_ref=halo.at[stage, c, pl.ds((1 - side) * n, n)],
            send_sem=side_sem.at[0],
            recv_sem=halo_sem.at[stage % 2, c],
            device_id=(gx + 2 * side - 1, gy),
            device_id_type=MESH,
        )

    def y_copy(stage, c, side):
        return pltpu.make_async_remote_copy(
            src_ref=send_y.at[stage, c],
            dst_ref=halo.at[stage, c, pl.ds(2 * n + 1 - side, 1)],
            send_sem=side_sem.at[1],
            recv_sem=halo_sem.at[stage % 2, c],
            device_id=(gx, gy + 2 * side - 1),
            device_id_type=MESH,
        )

    x_sides = ((0, gx > 0), (1, gx < nx - 1))
    y_sides = ((0, gy > 0), (1, gy < ny - 1))

    def launch(stage, c):
        for half in range(CHUNK // 4):
            pack(stage, c, half)
        rim = pack_rim(stage, c)
        for side, there in x_sides:
            @pl.when(there)
            def _(side=side):
                x_copy(stage, c, side).start()
        send_y[stage, c, 0] = rim
        for side, there in y_sides:
            @pl.when(there)
            def _(side=side):
                y_copy(stage, c, side).start()

    def far_start():
        def action(o, side):
            slot = reach - o if relative else gx
            if side == 0:
                source, target = far_c, gath.at[1, slot, pl.ds(0, 2 * tiles)]
            else:
                at = 2 * tiles + (1 - side) // 2
                source, target = far_e, gath.at[1, slot, pl.ds(at, 1)]
            pltpu.make_async_remote_copy(
                src_ref=source, dst_ref=target,
                send_sem=far_send.at[side + 1, o + reach if relative else 0],
                recv_sem=far_recv.at[0],
                device_id=(gx + o, gy + side), device_id_type=MESH,
            ).start()

        far(action)
        pltpu.make_async_copy(
            far_c, gath.at[1, own, pl.ds(0, 2 * tiles)], far_recv.at[0]
        ).start()

    def far_drain(o, side):
        whole(far_c if side == 0 else far_e, far_send.at[side + 1, o + reach]).wait()

    def rim_start():
        for side, there in y_sides:
            @pl.when(there)
            def _(side=side):
                pltpu.make_async_remote_copy(
                    src_ref=stat_e,
                    dst_ref=gath.at[0, own, pl.ds(2 * tiles + 1 - side, 1)],
                    send_sem=relay_send.at[side], recv_sem=rim_sem.at[0],
                    device_id=(gx, gy + 2 * side - 1), device_id_type=MESH,
                ).start()

    def rim_arrive():
        for b in counts(ny):
            @pl.when(has_y == b)
            def _(b=b):
                whole(arrivals.at[pl.ds(0, b)], rim_sem.at[0]).wait()
        for side, there in y_sides:
            @pl.when(there)
            def _(side=side):
                whole(stat_e, relay_send.at[side]).wait()

    def relay_steps(action, step):
        for side, there in x_sides:
            sign = 2 * side - 1
            passed = gx - sign * (step - 1)
            sends = jnp.logical_and(there, jnp.logical_and(passed >= 0, passed < nx))
            comes = jnp.logical_and(gx - sign * step >= 0, gx - sign * step < nx)
            action(side, sign, sends, comes)

    def relay(step):
        def action(side, sign, sends, comes):
            @pl.when(sends)
            def _():
                source = own - sign * (step - 1)
                target = own - sign * step if relative else source
                pltpu.make_async_remote_copy(
                    src_ref=gath.at[0, source], dst_ref=gath.at[0, target],
                    send_sem=relay_send.at[side], recv_sem=relay_recv.at[side, step - 1],
                    device_id=(gx + sign, gy), device_id_type=MESH,
                ).start()

        relay_steps(action, step)

    def relay_arrive(step):
        def action(side, sign, sends, comes):
            @pl.when(comes)
            def _():
                whole(
                    gath.at[0, own - sign * step], relay_recv.at[side, step - 1]
                ).wait()

            @pl.when(sends)
            def _():
                whole(gath.at[0, own - sign * (step - 1)], relay_send.at[side]).wait()

        relay_steps(action, step)

    def fill_far(data):
        low, high = data
        first = jnp.where(lane < RIM, low[0], pltpu.roll(high[0], RIM, 1))
        second = jnp.where(
            lane < LANES - RIM, pltpu.roll(high[-1], LANES - RIM, 1), low[-1]
        )
        return jnp.where(lane < 2 * RIM, first, second)

    def put(target, data):
        for f in range(2):
            for t in range(tiles):
                target[f * tiles + t] = data[f][t]

    for side, missing in ((0, gx == 0), (1, gx == nx - 1)):
        @pl.when(missing)
        def _(side=side):
            for stage in range(3):
                @pl.loop(0, chunks)
                def _(c, stage=stage):
                    halo[stage, c, side * n:(side + 1) * n] = jnp.zeros(
                        (n, ROWS, LANES), jnp.float32
                    )

    for side, missing in ((0, gy == 0), (1, gy == ny - 1)):
        @pl.when(missing)
        def _(side=side):
            halo[:, :, 2 * n + side] = jnp.zeros((3, chunks, ROWS, LANES), jnp.float32)
            gath[:, :, 2 * tiles + side] = jnp.zeros((2, slots, ROWS, LANES), jnp.float32)

    if relative:
        blank[...] = jnp.zeros((2 * tiles, ROWS, LANES), jnp.float32)

    whole(ints, relay_recv.at[0, 0]).wait()
    active = [ints[0, :, lanes(t)] * ints[1, :, lanes(t)] for t in range(tiles)]

    def first(c):
        whole(held.at[c], halo_sem.at[1, c]).wait()
        for kk in range(CHUNK):
            for t in range(tiles):
                live = active[t] > c * CHUNK + kk
                for f in range(3):
                    held[c, f, kk, :, lanes(t)] = jnp.where(
                        live, held[c, f, kk, :, lanes(t)], 0.0
                    )

    first(0)
    for c in range(1, chunks):
        load(c)
    pltpu.make_async_copy(surface_hbm, floats.at[0], relay_recv.at[0, 1]).start()
    pltpu.make_async_copy(depth_hbm, floats.at[1], relay_recv.at[0, 1]).start()
    pl.semaphore_wait(barrier, count)
    launch(0, 0)

    @pl.loop(1, chunks)
    def _(c):
        first(c)
        launch(0, c)

    if relative:
        for j in range(slots):
            @pl.when(jnp.logical_not(inside(gx + j - reach, gy)))
            def _(j=j):
                gath[0, j] = jnp.zeros((2 * tiles + 2, ROWS, LANES), jnp.float32)
                pltpu.make_async_copy(
                    blank, gath.at[1, j, pl.ds(0, 2 * tiles)], far_recv.at[0]
                ).start()
                for side, there in y_sides:
                    @pl.when(there)
                    def _(side=side):
                        pltpu.make_async_copy(
                            blank.at[pl.ds(0, 1)],
                            gath.at[1, j, pl.ds(2 * tiles + side, 1)],
                            far_recv.at[0],
                        ).start()

    whole(floats, relay_recv.at[0, 1]).wait()
    stats = (
        [floats[0, :, lanes(t)] for t in range(tiles)],
        [ints[1, :, lanes(t)].astype(jnp.float32) for t in range(tiles)],
    )
    put(gath.at[0, own], stats)
    stat_e[0] = fill_far(stats)
    rim_start()

    @pl.loop(0, chunks - 1)
    def _(c):
        move(c)

    quarter = lane % 4

    def run_stage(stage, weight0, weight1):
        gain = weight1 * TIME_STEP
        keep_flow = weight1 - 4.0 * gain * VISCOSITY
        keep_salt = weight1 - 4.0 * gain * DIFFUSIVITY
        drift = -gain / 12.0
        push = drift * PRESS_COEF

        def body(c, carry, behind=stage < 2):
            press_e, press_n = list(carry[0]), list(carry[1])
            sums = [list(x) for x in carry[2:]]
            index = stage * chunks + c
            arrive(stage, c)
            if behind:
                move(index + chunks - 1)
            rims = jnp.where(quarter < 2, halo[stage, c, 2 * n], halo[stage, c, 2 * n + 1])
            r1, r2 = pltpu.roll(rims, LANES - 1, 1), pltpu.roll(rims, LANES - 2, 1)
            l1, l2 = pltpu.roll(rims, 1, 1), pltpu.roll(rims, 2, 1)
            rim_slope = jnp.where(
                quarter < 2,
                jnp.where(quarter == 0, -r2, 8.0 * r1 - r2),
                jnp.where(quarter == 2, l2 - 8.0 * l1, l2),
            )
            rim_sum = jnp.where(quarter == 1, r1, jnp.where(quarter == 2, l1, 0.0))
            for kk in range(CHUNK):
                fields = []
                for f in range(3):
                    position = f * CHUNK + kk
                    group, m = (kk // 4) * 3 + f, kk % 4
                    back = (-(4 * position + 2)) % LANES
                    extra_slope = pltpu.roll(rim_slope, back, 1)
                    extra_sum = pltpu.roll(rim_sum, back, 1)
                    per_tile = []
                    for t in range(tiles):
                        q = held[index, f, kk, :, lanes(t)]
                        ends = jnp.where(
                            pair == m,
                            halo[stage, c, group * tiles + t],
                            halo[stage, c, n + group * tiles + t],
                        )
                        if m != 3:
                            ends = pltpu.roll(ends, (-(2 * m + 2)) % ROWS, 0)
                        e1 = pltpu.roll(jnp.where(row < 1, ends, q), ROWS - 1, 0)
                        e2 = pltpu.roll(jnp.where(row < 2, ends, q), ROWS - 2, 0)
                        w1 = pltpu.roll(jnp.where(row >= ROWS - 1, ends, q), 1, 0)
                        w2 = pltpu.roll(jnp.where(row >= ROWS - 2, ends, q), 2, 0)
                        dy = moved[index, f, kk, :, lanes(t)]
                        sides = moved[index, f, kk, :, lanes(tiles + t)]
                        if t == 0:
                            dy = dy + jnp.where(lane < 2, extra_slope, 0.0)
                            sides = sides + jnp.where(lane < 1, extra_sum, 0.0)
                        if t == tiles - 1:
                            dy = dy + jnp.where(lane >= LANES - 2, extra_slope, 0.0)
                            sides = sides + jnp.where(lane >= LANES - 1, extra_sum, 0.0)
                        dx = 8.0 * (e1 - w1) - (e2 - w2)
                        per_tile.append((q, dx, dy, (e1 + w1) + sides))
                    fields.append(per_tile)
                for t in range(tiles):
                    live = active[t] > c * CHUNK + kk
                    (u, ux, uy, ul), (v, vx, vy, vl), (s, sx, sy, sl) = [
                        fields[f][t] for f in range(3)
                    ]
                    press_e[t] = press_e[t] + sx
                    press_n[t] = press_n[t] + sy
                    um = u * drift
                    vm = v * drift
                    news = [
                        (um * ux + vm * uy) + push * press_e[t] + (gain * CORIOLIS) * v
                        + (gain * VISCOSITY) * ul + keep_flow * u,
                        (um * vx + vm * vy) + push * press_n[t] - (gain * CORIOLIS) * u
                        + (gain * VISCOSITY) * vl + keep_flow * v,
                        (um * sx + vm * sy) + (gain * DIFFUSIVITY) * sl + keep_salt * s,
                    ]
                    for f in range(3):
                        new = news[f]
                        if weight0 is not None:
                            new = new + weight0 * held[c, f, kk, :, lanes(t)]
                        new = jnp.where(live, new, 0.0)
                        if stage < 2:
                            held[index + chunks, f, kk, :, lanes(t)] = new
                        else:
                            state_out[c, f, kk, :, lanes(t)] = new
                            if f < 2:
                                sums[f][t] = sums[f][t] + new
            if stage < 2:
                launch(stage + 1, c)
            return (tuple(press_e), tuple(press_n)) + tuple(tuple(x) for x in sums)

        start = ((zero,) * tiles,) * (4 if stage == 2 else 2)
        if stage < 2:
            return lax.fori_loop(0, chunks, body, start)
        return lax.fori_loop(1, chunks, body, body(0, start, True))

    def pass_on(step):
        if step == 1:
            rim_arrive()
        elif step - 1 <= reach:
            relay_arrive(step - 1)
        if step <= reach:
            relay(step)

    run_stage(0, None, 1.0)
    pass_on(1)
    run_stage(1, 0.75, 0.25)
    pass_on(2)
    carry = run_stage(2, 1.0 / 3.0, 2.0 / 3.0)

    flows = [
        [floats[1, :, lanes(t)] * (carry[2 + f][t] / levels) for t in range(tiles)]
        for f in range(2)
    ]
    put(far_c, flows)
    far_e[0] = fill_far(flows[::-1])
    far_start()
    pass_on(3)
    pass_on(4)

    wide = tiles + 1

    def window(kind, f):
        out = []
        for p in range(slots):
            line = [gath[kind, p, f * tiles + t] for t in range(tiles)]
            below = gath[kind, p, 2 * tiles]
            above = gath[kind, p, 2 * tiles + 1]
            if f != kind:
                above = pltpu.roll(above, LANES - RIM, 1)
                below = pltpu.roll(below, RIM, 1)
            line.append(
                jnp.where(lane < RIM, above, jnp.where(lane >= LANES - RIM, below, 0.0))
            )
            out.append(line)
        return out

    def up(z, p, t):
        after = z[p + 1][t] if p + 1 < slots else zero
        return pltpu.roll(jnp.where(row < 1, after, z[p][t]), ROWS - 1, 0)

    def down(z, p, t):
        before = z[p - 1][t] if p > 0 else zero
        return pltpu.roll(jnp.where(row >= ROWS - 1, before, z[p][t]), 1, 0)

    def right(z, p, t):
        return pltpu.roll(jnp.where(lane < 1, z[p][(t + 1) % wide], z[p][t]), LANES - 1, 1)

    def left(z, p, t):
        return pltpu.roll(jnp.where(lane >= LANES - 1, z[p][(t - 1) % wide], z[p][t]), 1, 1)

    def grid(make):
        return [[make(p, t) for t in range(wide)] for p in range(slots)]

    def box(w):
        b = grid(lambda p, t: 4.0 * w[p][t] + (up(w, p, t) + down(w, p, t)))
        return grid(lambda p, t: 4.0 * b[p][t] + (right(b, p, t) + left(b, p, t)))

    x = window(0, 0)
    wet = window(0, 1)
    wet6 = grid(lambda p, t: wet[p][t] * (1.0 / 6.0))
    w = grid(lambda p, t: wet[p][t] * x[p][t])
    image = box(w)
    start = grid(lambda p, t: wet6[p][t] * image[p][t] - 6.0 * w[p][t])

    far_arrive()
    fe = window(1, 0)
    fn = window(1, 1)

    def right_side(p, t):
        div = (up(fe, p, t) - down(fe, p, t)) + (right(fn, p, t) - left(fn, p, t))
        return start[p][t] - wet[p][t] * ((0.5 * DIVERGENCE_COEF) * div)

    r = grid(right_side)
    d = grid(lambda p, t: r[p][t] * (1.0 / CHEB_CENTER))
    keeps, gains = cheb_table(ITERS)
    for index in range(ITERS):
        x = grid(lambda p, t: x[p][t] + d[p][t])
        if index < ITERS - 1:
            image = box(d)
            r = grid(
                lambda p, t: (r[p][t] - (SIGMA_SHIFT + 6.0) * d[p][t])
                + wet6[p][t] * image[p][t]
            )
            d = grid(lambda p, t: keeps[index] * d[p][t] + gains[index] * r[p][t])
    dry = dry_factor(ITERS)
    x = grid(lambda p, t: x[p][t] * (dry + (1.0 - dry) * wet[p][t]))

    for t in range(wide):
        xs[0, t] = zero
        xs[slots + 1, t] = zero
    for p in range(slots):
        for t in range(wide):
            xs[p + 1, t] = x[p][t]
    mine = [[xs[own + i, t] for t in range(wide)] for i in range(3)]
    for t in range(tiles):
        surface_out[:, lanes(t)] = mine[1][t]
        above = pltpu.roll(jnp.where(row < 1, mine[2][t], mine[1][t]), ROWS - 1, 0)
        below = pltpu.roll(jnp.where(row >= ROWS - 1, mine[0][t], mine[1][t]), 1, 0)
        slope_out[0, :, lanes(t)] = (above - below) * 0.5
        slope_out[1, :, lanes(t)] = (right(mine, 1, t) - left(mine, 1, t)) * 0.5

    for a in counts(nx):
        @pl.when(jnp.logical_and(has_x == a, has_x > 0))
        def _(a=a):
            whole(send_x.at[pl.ds(0, max(a, 1))], side_sem.at[0]).wait()

    for b in counts(ny):
        @pl.when(jnp.logical_and(has_y == b, has_y > 0))
        def _(b=b):
            whole(y_count.at[pl.ds(0, max(b, 1))], side_sem.at[1]).wait()

    if relative:
        far(far_drain)
    else:
        if nx > 1:
            whole(block_count, far_send.at[1, 0]).wait()
        for side, there in ((-1, gy > 0), (1, gy < ny - 1)):
            @pl.when(there)
            def _(side=side):
                whole(rim_count, far_send.at[side + 1, 0]).wait()


def finish(
    state_ref, slope_ref, surface_ref, wet_ref, active_ref,
    east_out, north_out, salt_out, surface_out, held, sems,
):
    early = (
        pltpu.make_async_copy(surface_ref, surface_out, sems.at[1]),
    ) + tuple(
        pltpu.make_async_copy(
            state_ref.at[c, 2], salt_out.at[pl.ds(c * CHUNK, CHUNK)], sems.at[4 + c]
        )
        for c in range(state_ref.shape[0])
    )
    for copy in early:
        copy.start()
    levels = held.shape[1]
    active = active_ref[...] * wet_ref[...]
    slopes = (slope_ref[0], slope_ref[1])
    for f in range(2):
        for k in range(levels):
            held[f, k] = jnp.where(
                active > k, state_ref[k // CHUNK, f, k % CHUNK] - slopes[f], 0.0
            )
        pltpu.make_async_copy(held.at[f], (east_out, north_out)[f], sems.at[2 + f]).start()
    for f in range(2):
        pltpu.make_async_copy(held.at[f], (east_out, north_out)[f], sems.at[2 + f]).wait()
    for copy in early:
        copy.wait()


def solution(mesh):
    nx, ny = mesh.shape["gx"], mesh.shape["gy"]

    def local(east, north, salt, surface, depth, wet, active):
        levels, rows, width = east.shape
        assert rows == ROWS and width % LANES == 0 and levels % CHUNK == 0
        assert ITERS + 2 <= RIM and ITERS + 2 <= 3 * ROWS
        tiles = width // LANES
        chunks = levels // CHUNK
        n = 3 * CHUNK // 4 * tiles
        reach = min(nx - 1, -(-(ITERS + 2) // ROWS))
        slots = min(nx, 2 * reach + 1)
        f32 = jnp.float32
        vmem = pltpu.VMEM
        dma = pltpu.SemaphoreType.DMA
        block = pl.BlockSpec(memory_space=pltpu.VMEM)
        state = jax.ShapeDtypeStruct(east.shape, f32)
        hbm = pl.BlockSpec(memory_space=pltpu.HBM)
        tile = (rows, LANES)
        state3, slopes, surface_next = pl.pallas_call(
            functools.partial(kernel, nx, ny, reach, slots),
            out_shape=(
                jax.ShapeDtypeStruct((chunks, 3, CHUNK, rows, width), f32),
                jax.ShapeDtypeStruct((2,) + surface.shape, f32),
                jax.ShapeDtypeStruct(surface.shape, f32),
            ),
            in_specs=[hbm] * 7,
            out_specs=(block,) * 3,
            scratch_shapes=[
                vmem((3 * chunks, 3, CHUNK, rows, width), f32),
                vmem((3 * chunks, 3, CHUNK, rows, 2 * width), f32),
                vmem((3 * width, 2 * width), jnp.bfloat16),
                vmem((2,) + surface.shape, jnp.int32),
                vmem((2,) + surface.shape, f32),
                vmem((3, chunks, 2 * n + 2) + tile, f32),
                vmem((2, 3, chunks, n) + tile, f32),
                vmem((3, chunks, 1) + tile, f32),
                vmem((2 * tiles,) + tile, f32),
                vmem((1,) + tile, f32),
                vmem((1,) + tile, f32),
                vmem((2, slots, 2 * tiles + 2) + tile, f32),
                vmem((slots + 2, tiles + 1) + tile, f32),
                vmem((max(slots - 1, 1), 2 * tiles) + tile, f32),
                vmem((slots,) + tile, f32),
                vmem((2, 3, chunks, 1) + tile, f32),
                vmem((slots * (2 * tiles + 2),) + tile, f32),
                vmem((2 * tiles,) + tile, f32),
                dma((2, chunks)),
                dma((2,)),
                dma((3, slots if slots < nx else 1)),
                dma((1,)),
                dma((1,)),
                dma((2,)),
                dma((2, max(reach, 2))),
            ],
            compiler_params=pltpu.CompilerParams(
                collective_id=0, has_side_effects=True, vmem_limit_bytes=48 * 1024 * 1024
            ),
        )(*[
            pltpu.with_memory_space_constraint(z, pltpu.HBM)
            for z in (east, north, salt, surface, depth, wet, active)
        ])
        return pl.pallas_call(
            finish,
            out_shape=(state, state, state, jax.ShapeDtypeStruct(surface.shape, f32)),
            in_specs=[block] * 5,
            out_specs=(hbm,) * 4,
            scratch_shapes=[vmem((2,) + east.shape, f32), dma((4 + chunks,))],
            compiler_params=pltpu.CompilerParams(vmem_limit_bytes=8 * 1024 * 1024),
        )(state3, slopes, surface_next, wet, active)

    return jax.shard_map(
        local,
        mesh=mesh,
        in_specs=(
            P(None, "gx", "gy"),
            P(None, "gx", "gy"),
            P(None, "gx", "gy"),
            P("gx", "gy"),
            P("gx", "gy"),
            P("gx", "gy"),
            P("gx", "gy"),
        ),
        out_specs=(P(None, "gx", "gy"), P(None, "gx", "gy"), P(None, "gx", "gy"), P("gx", "gy")),
        check_vma=False,
    )
```

```python
import functools

import jax
import jax.numpy as jnp
from jax import lax
from jax.experimental import pallas as pl
from jax.experimental.pallas import tpu as pltpu
from jax.sharding import PartitionSpec as P

ITERS = 16

TIME_STEP = 0.2
CORIOLIS = 0.3
PRESS_COEF = 0.05
VISCOSITY = 0.1
DIFFUSIVITY = 0.1
SIGMA_SHIFT = 0.25
CHEB_CENTER = 3.625
CHEB_HALF = 3.375
DIVERGENCE_COEF = 8.0

ROWS = 8
LANES = 128
CHUNK = 8
RIM = LANES // 4
MESH = pl.DeviceIdType.MESH


def cheb_table(count):
    first = CHEB_CENTER / CHEB_HALF
    ratio = 1.0 / first
    keeps = []
    gains = []
    for index in range(count):
        ratio_next = 1.0 / (2.0 * first - ratio)
        keeps.append(ratio_next * ratio)
        gains.append(2.0 * ratio_next / CHEB_HALF)
        ratio = ratio_next
    return (keeps, gains)


def dry_factor(count):
    keeps, gains = cheb_table(count)
    x, r = 1.0, -1.0
    d = r / CHEB_CENTER
    for index in range(count):
        x = x + d
        r = r - d
        d = keeps[index] * d + gains[index] * r
    return x


def kernel(
    nx, ny, reach, slots,
    east_hbm, north_hbm, salt_hbm, surface_hbm, depth_hbm, wet_hbm, active_hbm,
    state_out, slope_out, surface_out,
    held, moved, shifts, ints, floats, halo, send_x, send_y, far_c, far_e, stat_e, gath, xs,
    y_count, arrivals, blank, halo_sem, side_sem, far_send, far_recv,
    rim_sem, relay_send, relay_recv,
):
    gx = lax.axis_index("gx")
    gy = lax.axis_index("gy")
    width = held.shape[4]
    tiles = width // LANES
    chunks = held.shape[0] // 3
    levels = chunks * CHUNK
    groups = 3 * CHUNK // 4
    n = groups * tiles
    relative = slots < nx
    row = lax.broadcasted_iota(jnp.int32, (ROWS, LANES), 0)
    lane = lax.broadcasted_iota(jnp.int32, (ROWS, LANES), 1)
    pair = row // 2
    zero = jnp.zeros((ROWS, LANES), jnp.float32)

    def lanes(t):
        return slice(t * LANES, (t + 1) * LANES)

    def inside(x, y):
        return jnp.logical_and(
            jnp.logical_and(x >= 0, x < nx), jnp.logical_and(y >= 0, y < ny)
        )

    def whole(ref, sem):
        return pltpu.make_async_copy(ref, ref, sem)

    def load(c):
        part = pl.ds(c * CHUNK, CHUNK)
        for f, source in enumerate((east_hbm, north_hbm, salt_hbm)):
            pltpu.make_async_copy(source.at[part], held.at[c, f], halo_sem.at[1, c]).start()

    own = reach if relative else gx
    partners = [
        (o, side)
        for o in range(-reach, reach + 1)
        for side in (-1, 0, 1)
        if (o, side) != (0, 0)
    ]
    partners.sort(key=lambda p: (-abs(p[1]), p[0] != 0, -abs(p[0])))

    def far(action):
        for o, side in partners:
            @pl.when(inside(gx + o, gy + side))
            def _(o=o, side=side):
                action(o, side)

    def counts(size):
        return (0,) if size == 1 else (1,) if size == 2 else (1, 2)

    has_x = (gx > 0).astype(jnp.int32) + (gx < nx - 1).astype(jnp.int32)
    has_y = (gy > 0).astype(jnp.int32) + (gy < ny - 1).astype(jnp.int32)

    def arrive(stage, c):
        for a in counts(nx):
            for b in counts(ny):
                @pl.when(jnp.logical_and(has_x == a, has_y == b))
                def _(a=a, b=b):
                    part = halo.at[stage, c, pl.ds(0, a * n + b)]
                    whole(part, halo_sem.at[stage % 2, c]).wait()

    def far_arrive():
        for b in counts(ny):
            @pl.when(has_y == b)
            def _(b=b):
                whole(arrivals.at[pl.ds(0, slots * (2 * tiles + b))], far_recv.at[0]).wait()

    barrier = pltpu.get_barrier_semaphore()
    count = jnp.int32(0)
    for o, side in ((-1, 0), (1, 0), (0, -1), (0, 1)):
        there = inside(gx + o, gy + side)

        @pl.when(there)
        def _(o=o, side=side):
            pl.semaphore_signal(
                barrier, inc=1, device_id=(gx + o, gy + side), device_id_type=MESH
            )

        count = count + there.astype(jnp.int32)

    pltpu.make_async_copy(active_hbm, ints.at[0], relay_recv.at[0, 0]).start()
    pltpu.make_async_copy(wet_hbm, ints.at[1], relay_recv.at[0, 0]).start()
    load(0)

    source = lax.broadcasted_iota(jnp.int32, (width, width), 0)
    target = lax.broadcasted_iota(jnp.int32, (width, width), 1)
    step = source - target
    one = jnp.abs(step) == 1
    sign = jnp.where(step > 0, 1.0, -1.0)
    slope = jnp.where(one, 8.0 * sign, jnp.where(jnp.abs(step) == 2, -sign, 0.0))
    for i in range(3):
        part = slice(i * width, (i + 1) * width)
        shifts[part, :width] = slope.astype(jnp.bfloat16)
        shifts[part, width:] = jnp.where(one, 1.0, 0.0).astype(jnp.bfloat16)

    def move(index):
        value = held[index].reshape(3 * CHUNK * ROWS, width)
        high = value.astype(jnp.bfloat16)
        rest = value - high.astype(jnp.float32)
        middle = rest.astype(jnp.bfloat16)
        low = (rest - middle.astype(jnp.float32)).astype(jnp.bfloat16)
        total = jnp.dot(
            jnp.concatenate([low, middle, high], axis=1),
            shifts[...],
            preferred_element_type=jnp.float32,
        )
        moved[index] = total.reshape(3, CHUNK, ROWS, 2 * width)

    def pack(stage, c, half):
        for f in range(3):
            ups = [None] * tiles
            downs = [None] * tiles
            for m in range(4):
                for t in range(tiles):
                    part = held[stage * chunks + c, f, half * 4 + m, :, lanes(t)]
                    turned = part if m == 3 else pltpu.roll(part, 2 * m + 2, 0)
                    if m == 0:
                        ups[t] = turned
                        downs[t] = turned
                    else:
                        ups[t] = jnp.where(pair == m, turned, ups[t])
                        downs[t] = jnp.where(pair == (m + 1) % 4, turned, downs[t])
            for t in range(tiles):
                at = (half * 3 + f) * tiles + t
                send_x[0, stage, c, at] = downs[t]
                send_x[1, stage, c, at] = ups[t]

    def pack_rim(stage, c):
        rim = zero
        for f in range(3):
            for kk in range(CHUNK):
                position = f * CHUNK + kk
                first, last = (
                    held[stage * chunks + c, f, kk, :, lanes(t)] for t in (0, tiles - 1)
                )
                rim = jnp.where(
                    lane // 4 == position,
                    pltpu.roll(
                        jnp.where(lane < LANES // 2, first, last),
                        (4 * position + 2) % LANES, 1,
                    ),
                    rim,
                )
        return rim

    def x_copy(stage, c, side):
        return pltpu.make_async_remote_copy(
            src_ref=send_x.at[side, stage, c],
            dst_ref=halo.at[stage, c, pl.ds((1 - side) * n, n)],
            send_sem=side_sem.at[0],
            recv_sem=halo_sem.at[stage % 2, c],
            device_id=(gx + 2 * side - 1, gy),
            device_id_type=MESH,
        )

    def y_copy(stage, c, side):
        return pltpu.make_async_remote_copy(
            src_ref=send_y.at[stage, c],
            dst_ref=halo.at[stage, c, pl.ds(2 * n + 1 - side, 1)],
            send_sem=side_sem.at[1],
            recv_sem=halo_sem.at[stage % 2, c],
            device_id=(gx, gy + 2 * side - 1),
            device_id_type=MESH,
        )

    x_sides = ((0, gx > 0), (1, gx < nx - 1))
    y_sides = ((0, gy > 0), (1, gy < ny - 1))

    def launch(stage, c):
        for half in range(CHUNK // 4):
            pack(stage, c, half)
        rim = pack_rim(stage, c)
        for side, there in x_sides:
            @pl.when(there)
            def _(side=side):
                x_copy(stage, c, side).start()
        send_y[stage, c, 0] = rim
        for side, there in y_sides:
            @pl.when(there)
            def _(side=side):
                y_copy(stage, c, side).start()

    def far_start():
        def action(o, side):
            slot = reach - o if relative else gx
            if side == 0:
                source, target = far_c, gath.at[1, slot, pl.ds(0, 2 * tiles)]
            else:
                at = 2 * tiles + (1 - side) // 2
                source, target = far_e, gath.at[1, slot, pl.ds(at, 1)]
            pltpu.make_async_remote_copy(
                src_ref=source, dst_ref=target,
                send_sem=far_send.at[side + 1, o + reach] if relative else far_send.at[0, 0],
                recv_sem=far_recv.at[0],
                device_id=(gx + o, gy + side), device_id_type=MESH,
            ).start()

        far(action)
        pltpu.make_async_copy(
            far_c, gath.at[1, own, pl.ds(0, 2 * tiles)], far_recv.at[0]
        ).start()

    def far_drain(o, side):
        whole(far_c if side == 0 else far_e, far_send.at[side + 1, o + reach]).wait()

    def rim_start():
        for side, there in y_sides:
            @pl.when(there)
            def _(side=side):
                pltpu.make_async_remote_copy(
                    src_ref=stat_e,
                    dst_ref=gath.at[0, own, pl.ds(2 * tiles + 1 - side, 1)],
                    send_sem=relay_send.at[side], recv_sem=rim_sem.at[0],
                    device_id=(gx, gy + 2 * side - 1), device_id_type=MESH,
                ).start()

    def rim_arrive():
        for b in counts(ny):
            @pl.when(has_y == b)
            def _(b=b):
                whole(arrivals.at[pl.ds(0, b)], rim_sem.at[0]).wait()
        for side, there in y_sides:
            @pl.when(there)
            def _(side=side):
                whole(stat_e, relay_send.at[side]).wait()

    def relay_steps(action, step):
        for side, there in x_sides:
            sign = 2 * side - 1
            passed = gx - sign * (step - 1)
            sends = jnp.logical_and(there, jnp.logical_and(passed >= 0, passed < nx))
            comes = jnp.logical_and(gx - sign * step >= 0, gx - sign * step < nx)
            action(side, sign, sends, comes)

    def relay(step):
        def action(side, sign, sends, comes):
            @pl.when(sends)
            def _():
                source = own - sign * (step - 1)
                target = own - sign * step if relative else source
                pltpu.make_async_remote_copy(
                    src_ref=gath.at[0, source], dst_ref=gath.at[0, target],
                    send_sem=relay_send.at[side], recv_sem=relay_recv.at[side, step - 1],
                    device_id=(gx + sign, gy), device_id_type=MESH,
                ).start()

        relay_steps(action, step)

    def relay_arrive(step):
        def action(side, sign, sends, comes):
            @pl.when(comes)
            def _():
                whole(
                    gath.at[0, own - sign * step], relay_recv.at[side, step - 1]
                ).wait()

            @pl.when(sends)
            def _():
                whole(gath.at[0, own - sign * (step - 1)], relay_send.at[side]).wait()

        relay_steps(action, step)

    def fill_far(data):
        low, high = data
        first = jnp.where(lane < RIM, low[0], pltpu.roll(high[0], RIM, 1))
        second = jnp.where(
            lane < LANES - RIM, pltpu.roll(high[-1], LANES - RIM, 1), low[-1]
        )
        return jnp.where(lane < 2 * RIM, first, second)

    def put(target, data):
        for f in range(2):
            for t in range(tiles):
                target[f * tiles + t] = data[f][t]

    for side, missing in ((0, gx == 0), (1, gx == nx - 1)):
        @pl.when(missing)
        def _(side=side):
            for stage in range(3):
                @pl.loop(0, chunks)
                def _(c, stage=stage):
                    halo[stage, c, side * n:(side + 1) * n] = jnp.zeros(
                        (n, ROWS, LANES), jnp.float32
                    )

    for side, missing in ((0, gy == 0), (1, gy == ny - 1)):
        @pl.when(missing)
        def _(side=side):
            halo[:, :, 2 * n + side] = jnp.zeros((3, chunks, ROWS, LANES), jnp.float32)
            gath[:, :, 2 * tiles + side] = jnp.zeros((2, slots, ROWS, LANES), jnp.float32)

    if relative:
        blank[...] = jnp.zeros((2 * tiles, ROWS, LANES), jnp.float32)

    whole(ints, relay_recv.at[0, 0]).wait()
    active = [ints[0, :, lanes(t)] * ints[1, :, lanes(t)] for t in range(tiles)]

    def first(c):
        whole(held.at[c], halo_sem.at[1, c]).wait()
        for kk in range(CHUNK):
            for t in range(tiles):
                live = active[t] > c * CHUNK + kk
                for f in range(3):
                    held[c, f, kk, :, lanes(t)] = jnp.where(
                        live, held[c, f, kk, :, lanes(t)], 0.0
                    )

    first(0)
    for c in range(1, chunks):
        load(c)
    pltpu.make_async_copy(surface_hbm, floats.at[0], relay_recv.at[0, 1]).start()
    pltpu.make_async_copy(depth_hbm, floats.at[1], relay_recv.at[0, 1]).start()
    pl.semaphore_wait(barrier, count)
    launch(0, 0)

    @pl.loop(1, chunks)
    def _(c):
        first(c)
        launch(0, c)

    if relative:
        for j in range(slots):
            @pl.when(jnp.logical_not(inside(gx + j - reach, gy)))
            def _(j=j):
                gath[0, j] = jnp.zeros((2 * tiles + 2, ROWS, LANES), jnp.float32)
                pltpu.make_async_copy(
                    blank, gath.at[1, j, pl.ds(0, 2 * tiles)], far_recv.at[0]
                ).start()
                for side, there in y_sides:
                    @pl.when(there)
                    def _(side=side):
                        pltpu.make_async_copy(
                            blank.at[pl.ds(0, 1)],
                            gath.at[1, j, pl.ds(2 * tiles + side, 1)],
                            far_recv.at[0],
                        ).start()

    whole(floats, relay_recv.at[0, 1]).wait()
    stats = (
        [floats[0, :, lanes(t)] for t in range(tiles)],
        [ints[1, :, lanes(t)].astype(jnp.float32) for t in range(tiles)],
    )
    put(gath.at[0, own], stats)
    stat_e[0] = fill_far(stats)
    rim_start()

    @pl.loop(0, chunks - 1)
    def _(c):
        move(c)

    quarter = lane % 4

    def run_stage(stage, weight0, weight1):
        gain = weight1 * TIME_STEP
        keep_flow = weight1 - 4.0 * gain * VISCOSITY
        keep_salt = weight1 - 4.0 * gain * DIFFUSIVITY
        drift = -gain / 12.0
        push = drift * PRESS_COEF

        def body(c, carry, behind=stage < 2):
            press_e, press_n = list(carry[0]), list(carry[1])
            sums = [list(x) for x in carry[2:]]
            index = stage * chunks + c
            arrive(stage, c)
            if behind:
                move(index + chunks - 1)
            rims = jnp.where(quarter < 2, halo[stage, c, 2 * n], halo[stage, c, 2 * n + 1])
            r1, r2 = pltpu.roll(rims, LANES - 1, 1), pltpu.roll(rims, LANES - 2, 1)
            l1, l2 = pltpu.roll(rims, 1, 1), pltpu.roll(rims, 2, 1)
            rim_slope = jnp.where(
                quarter < 2,
                jnp.where(quarter == 0, -r2, 8.0 * r1 - r2),
                jnp.where(quarter == 2, l2 - 8.0 * l1, l2),
            )
            rim_sum = jnp.where(quarter == 1, r1, jnp.where(quarter == 2, l1, 0.0))
            for kk in range(CHUNK):
                fields = []
                for f in range(3):
                    position = f * CHUNK + kk
                    group, m = (kk // 4) * 3 + f, kk % 4
                    back = (-(4 * position + 2)) % LANES
                    extra_slope = pltpu.roll(rim_slope, back, 1)
                    extra_sum = pltpu.roll(rim_sum, back, 1)
                    per_tile = []
                    for t in range(tiles):
                        q = held[index, f, kk, :, lanes(t)]
                        ends = jnp.where(
                            pair == m,
                            halo[stage, c, group * tiles + t],
                            halo[stage, c, n + group * tiles + t],
                        )
                        if m != 3:
                            ends = pltpu.roll(ends, (-(2 * m + 2)) % ROWS, 0)
                        e1 = pltpu.roll(jnp.where(row < 1, ends, q), ROWS - 1, 0)
                        e2 = pltpu.roll(jnp.where(row < 2, ends, q), ROWS - 2, 0)
                        w1 = pltpu.roll(jnp.where(row >= ROWS - 1, ends, q), 1, 0)
                        w2 = pltpu.roll(jnp.where(row >= ROWS - 2, ends, q), 2, 0)
                        dy = moved[index, f, kk, :, lanes(t)]
                        sides = moved[index, f, kk, :, lanes(tiles + t)]
                        if t == 0:
                            dy = dy + jnp.where(lane < 2, extra_slope, 0.0)
                            sides = sides + jnp.where(lane < 1, extra_sum, 0.0)
                        if t == tiles - 1:
                            dy = dy + jnp.where(lane >= LANES - 2, extra_slope, 0.0)
                            sides = sides + jnp.where(lane >= LANES - 1, extra_sum, 0.0)
                        dx = 8.0 * (e1 - w1) - (e2 - w2)
                        per_tile.append((q, dx, dy, (e1 + w1) + sides))
                    fields.append(per_tile)
                for t in range(tiles):
                    live = active[t] > c * CHUNK + kk
                    (u, ux, uy, ul), (v, vx, vy, vl), (s, sx, sy, sl) = [
                        fields[f][t] for f in range(3)
                    ]
                    press_e[t] = press_e[t] + sx
                    press_n[t] = press_n[t] + sy
                    um = u * drift
                    vm = v * drift
                    news = [
                        (um * ux + vm * uy) + push * press_e[t] + (gain * CORIOLIS) * v
                        + (gain * VISCOSITY) * ul + keep_flow * u,
                        (um * vx + vm * vy) + push * press_n[t] - (gain * CORIOLIS) * u
                        + (gain * VISCOSITY) * vl + keep_flow * v,
                        (um * sx + vm * sy) + (gain * DIFFUSIVITY) * sl + keep_salt * s,
                    ]
                    for f in range(3):
                        new = news[f]
                        if weight0 is not None:
                            new = new + weight0 * held[c, f, kk, :, lanes(t)]
                        new = jnp.where(live, new, 0.0)
                        if stage < 2:
                            held[index + chunks, f, kk, :, lanes(t)] = new
                        else:
                            state_out[c, f, kk, :, lanes(t)] = new
                            if f < 2:
                                sums[f][t] = sums[f][t] + new
            if stage < 2:
                launch(stage + 1, c)
            return (tuple(press_e), tuple(press_n)) + tuple(tuple(x) for x in sums)

        start = ((zero,) * tiles,) * (4 if stage == 2 else 2)
        if stage < 2:
            return lax.fori_loop(0, chunks, body, start)
        return lax.fori_loop(1, chunks, body, body(0, start, True))

    def pass_on(step):
        if step == 1:
            rim_arrive()
        elif step - 1 <= reach:
            relay_arrive(step - 1)
        if step <= reach:
            relay(step)

    run_stage(0, None, 1.0)
    pass_on(1)
    run_stage(1, 0.75, 0.25)
    pass_on(2)
    carry = run_stage(2, 1.0 / 3.0, 2.0 / 3.0)

    flows = [
        [floats[1, :, lanes(t)] * (carry[2 + f][t] / levels) for t in range(tiles)]
        for f in range(2)
    ]
    put(far_c, flows)
    far_e[0] = fill_far(flows[::-1])
    far_start()
    pass_on(3)
    pass_on(4)

    wide = tiles + 1

    def window(kind, f):
        out = []
        for p in range(slots):
            line = [gath[kind, p, f * tiles + t] for t in range(tiles)]
            below = gath[kind, p, 2 * tiles]
            above = gath[kind, p, 2 * tiles + 1]
            if f != kind:
                above = pltpu.roll(above, LANES - RIM, 1)
                below = pltpu.roll(below, RIM, 1)
            line.append(
                jnp.where(lane < RIM, above, jnp.where(lane >= LANES - RIM, below, 0.0))
            )
            out.append(line)
        return out

    def up(z, p, t):
        after = z[p + 1][t] if p + 1 < slots else zero
        return pltpu.roll(jnp.where(row < 1, after, z[p][t]), ROWS - 1, 0)

    def down(z, p, t):
        before = z[p - 1][t] if p > 0 else zero
        return pltpu.roll(jnp.where(row >= ROWS - 1, before, z[p][t]), 1, 0)

    def right(z, p, t):
        return pltpu.roll(jnp.where(lane < 1, z[p][(t + 1) % wide], z[p][t]), LANES - 1, 1)

    def left(z, p, t):
        return pltpu.roll(jnp.where(lane >= LANES - 1, z[p][(t - 1) % wide], z[p][t]), 1, 1)

    def grid(make):
        return [[make(p, t) for t in range(wide)] for p in range(slots)]

    def box(w):
        b = grid(lambda p, t: 4.0 * w[p][t] + (up(w, p, t) + down(w, p, t)))
        return grid(lambda p, t: 4.0 * b[p][t] + (right(b, p, t) + left(b, p, t)))

    x = window(0, 0)
    wet = window(0, 1)
    wet6 = grid(lambda p, t: wet[p][t] * (1.0 / 6.0))
    w = grid(lambda p, t: wet[p][t] * x[p][t])
    image = box(w)
    start = grid(lambda p, t: wet6[p][t] * image[p][t] - 6.0 * w[p][t])

    far_arrive()
    fe = window(1, 0)
    fn = window(1, 1)

    def right_side(p, t):
        div = (up(fe, p, t) - down(fe, p, t)) + (right(fn, p, t) - left(fn, p, t))
        return start[p][t] - wet[p][t] * ((0.5 * DIVERGENCE_COEF) * div)

    r = grid(right_side)
    d = grid(lambda p, t: r[p][t] * (1.0 / CHEB_CENTER))
    keeps, gains = cheb_table(ITERS)
    for index in range(ITERS):
        x = grid(lambda p, t: x[p][t] + d[p][t])
        if index < ITERS - 1:
            image = box(d)
            r = grid(
                lambda p, t: (r[p][t] - (SIGMA_SHIFT + 6.0) * d[p][t])
                + wet6[p][t] * image[p][t]
            )
            d = grid(lambda p, t: keeps[index] * d[p][t] + gains[index] * r[p][t])
    dry = dry_factor(ITERS)
    x = grid(lambda p, t: x[p][t] * (dry + (1.0 - dry) * wet[p][t]))

    for t in range(wide):
        xs[0, t] = zero
        xs[slots + 1, t] = zero
    for p in range(slots):
        for t in range(wide):
            xs[p + 1, t] = x[p][t]
    mine = [[xs[own + i, t] for t in range(wide)] for i in range(3)]
    for t in range(tiles):
        surface_out[:, lanes(t)] = mine[1][t]
        above = pltpu.roll(jnp.where(row < 1, mine[2][t], mine[1][t]), ROWS - 1, 0)
        below = pltpu.roll(jnp.where(row >= ROWS - 1, mine[0][t], mine[1][t]), 1, 0)
        slope_out[0, :, lanes(t)] = (above - below) * 0.5
        slope_out[1, :, lanes(t)] = (right(mine, 1, t) - left(mine, 1, t)) * 0.5

    for a in counts(nx):
        @pl.when(jnp.logical_and(has_x == a, has_x > 0))
        def _(a=a):
            whole(send_x.at[pl.ds(0, max(a, 1))], side_sem.at[0]).wait()

    for b in counts(ny):
        @pl.when(jnp.logical_and(has_y == b, has_y > 0))
        def _(b=b):
            whole(y_count.at[pl.ds(0, max(b, 1))], side_sem.at[1]).wait()

    if relative:
        far(far_drain)
    else:
        for b in counts(ny):
            @pl.when(has_y == b)
            def _(b=b):
                sent = (slots - 1) * 2 * tiles + b * slots
                whole(arrivals.at[pl.ds(0, sent)], far_send.at[0, 0]).wait()


def finish(
    state_ref, slope_ref, surface_ref, wet_ref, active_ref,
    east_out, north_out, salt_out, surface_out, held, sems,
):
    surface_copy = pltpu.make_async_copy(surface_ref, surface_out, sems.at[1])
    surface_copy.start()
    for c in range(state_ref.shape[0]):
        pltpu.make_async_copy(
            state_ref.at[c, 2], salt_out.at[pl.ds(c * CHUNK, CHUNK)], sems.at[0]
        ).start()
    levels = held.shape[1]
    active = active_ref[...] * wet_ref[...]
    slopes = (slope_ref[0], slope_ref[1])
    for f in range(2):
        for k in range(levels):
            held[f, k] = jnp.where(
                active > k, state_ref[k // CHUNK, f, k % CHUNK] - slopes[f], 0.0
            )
        pltpu.make_async_copy(held.at[f], (east_out, north_out)[f], sems.at[0]).start()
    pltpu.make_async_copy(held, held, sems.at[0]).wait()
    surface_copy.wait()


def solution(mesh):
    nx, ny = mesh.shape["gx"], mesh.shape["gy"]

    def local(east, north, salt, surface, depth, wet, active):
        levels, rows, width = east.shape
        assert rows == ROWS and width % LANES == 0 and levels % CHUNK == 0
        assert ITERS + 2 <= RIM and ITERS + 2 <= 3 * ROWS
        tiles = width // LANES
        chunks = levels // CHUNK
        n = 3 * CHUNK // 4 * tiles
        reach = min(nx - 1, -(-(ITERS + 2) // ROWS))
        slots = min(nx, 2 * reach + 1)
        f32 = jnp.float32
        vmem = pltpu.VMEM
        dma = pltpu.SemaphoreType.DMA
        block = pl.BlockSpec(memory_space=pltpu.VMEM)
        state = jax.ShapeDtypeStruct(east.shape, f32)
        hbm = pl.BlockSpec(memory_space=pltpu.HBM)
        tile = (rows, LANES)
        state3, slopes, surface_next = pl.pallas_call(
            functools.partial(kernel, nx, ny, reach, slots),
            out_shape=(
                jax.ShapeDtypeStruct((chunks, 3, CHUNK, rows, width), f32),
                jax.ShapeDtypeStruct((2,) + surface.shape, f32),
                jax.ShapeDtypeStruct(surface.shape, f32),
            ),
            in_specs=[hbm] * 7,
            out_specs=(block,) * 3,
            scratch_shapes=[
                vmem((3 * chunks, 3, CHUNK, rows, width), f32),
                vmem((3 * chunks, 3, CHUNK, rows, 2 * width), f32),
                vmem((3 * width, 2 * width), jnp.bfloat16),
                vmem((2,) + surface.shape, jnp.int32),
                vmem((2,) + surface.shape, f32),
                vmem((3, chunks, 2 * n + 2) + tile, f32),
                vmem((2, 3, chunks, n) + tile, f32),
                vmem((3, chunks, 1) + tile, f32),
                vmem((2 * tiles,) + tile, f32),
                vmem((1,) + tile, f32),
                vmem((1,) + tile, f32),
                vmem((2, slots, 2 * tiles + 2) + tile, f32),
                vmem((slots + 2, tiles + 1) + tile, f32),
                vmem((2, 3, chunks, 1) + tile, f32),
                vmem((slots * (2 * tiles + 2),) + tile, f32),
                vmem((2 * tiles,) + tile, f32),
                dma((2, chunks)),
                dma((2,)),
                dma((3, slots) if slots < nx else (1, 1)),
                dma((1,)),
                dma((1,)),
                dma((2,)),
                dma((2, max(reach, 2))),
            ],
            compiler_params=pltpu.CompilerParams(
                collective_id=0, has_side_effects=True, vmem_limit_bytes=48 * 1024 * 1024
            ),
        )(*[
            pltpu.with_memory_space_constraint(z, pltpu.HBM)
            for z in (east, north, salt, surface, depth, wet, active)
        ])
        return pl.pallas_call(
            finish,
            out_shape=(state, state, state, jax.ShapeDtypeStruct(surface.shape, f32)),
            in_specs=[block] * 5,
            out_specs=(hbm,) * 4,
            scratch_shapes=[vmem((3,) + east.shape, f32), dma((2,))],
            compiler_params=pltpu.CompilerParams(vmem_limit_bytes=8 * 1024 * 1024),
        )(state3, slopes, surface_next, wet, active)

    return jax.shard_map(
        local,
        mesh=mesh,
        in_specs=(
            P(None, "gx", "gy"),
            P(None, "gx", "gy"),
            P(None, "gx", "gy"),
            P("gx", "gy"),
            P("gx", "gy"),
            P("gx", "gy"),
            P("gx", "gy"),
        ),
        out_specs=(P(None, "gx", "gy"), P(None, "gx", "gy"), P(None, "gx", "gy"), P("gx", "gy")),
        check_vma=False,
    )
```
